8 devices in a mesh: frag: 1 (over z), dev2: 2 (over y), dev: 4 (over x, core).
Axes of the slice: x: 2, y: 2, z: 1, core: 2. Of those that a mesh axis runs over, the one named last changes fastest.
Arguments:
- ao_ints: bfloat16 [128, 128, 128, 128], P(('frag', 'dev'), 'dev2')
- c_occ: bfloat16 [128, 4], P('frag')
- c_virt: bfloat16 [128, 112], P('frag')
Outputs:
- output: float32 [4, 112, 448], P('frag', None, ('dev2', 'dev'))
All inputs are finite; a program needn't handle non-finite values.
Results may differ from the reference program's by a relative error of at most 0.001.
Values are sent between devices in bfloat16 or wider.
A program may use at most 1 GiB of HBM per device.

```python
import jax
import jax.numpy as jnp
from jax import lax

NBF = 128
OCC = 4
VIRT = 112


def setup_inputs(seed: int = 0, part: int = 0) -> dict:
    base_key = jax.random.fold_in(jax.random.key(seed), part)
    key_ao, key_occ, key_virt = jax.random.split(base_key, 3)
    row_keys = jax.random.split(key_ao, NBF)
    ao_ints = lax.map(
        lambda row_key: jax.random.normal(row_key, (NBF, NBF, NBF), jnp.float32).astype(jnp.bfloat16),
        row_keys)
    c_occ = jax.random.normal(key_occ, (NBF, OCC), jnp.float32) * NBF ** -0.5
    c_virt = jax.random.normal(key_virt, (NBF, VIRT), jnp.float32) * NBF ** -0.5
    return {"ao_ints": ao_ints, "c_occ": c_occ.astype(jnp.bfloat16), "c_virt": c_virt.astype(jnp.bfloat16)}


def reference(ao_ints, c_occ, c_virt):
    occ_f32 = c_occ.astype(jnp.float32)
    virt_f32 = c_virt.astype(jnp.float32)

    def half_row(ao_row):
        t_one = jnp.einsum("qrs,rj->qsj", ao_row.astype(jnp.float32), occ_f32).astype(jnp.bfloat16)
        return jnp.einsum("qsj,sb->qjb", t_one.astype(jnp.float32), virt_f32).astype(jnp.bfloat16)

    half_ints = lax.map(half_row, ao_ints).astype(jnp.float32)
    e_part = jnp.einsum("pi,pqjb->iqjb", occ_f32, half_ints)
    mo_ints = jnp.einsum("iqjb,qa->iajb", e_part, virt_f32)
    return mo_ints.reshape(OCC, VIRT, OCC * VIRT)
```

```python
import functools

import jax
import jax.numpy as jnp
from jax import lax
from jax.experimental import pallas as pl
from jax.experimental.pallas import tpu as pltpu
from jax.sharding import PartitionSpec as P

MESH = pl.DeviceIdType.MESH
F32 = jnp.float32
BF16 = jnp.bfloat16

ROWS_P = 32
ROWS_Q = 64
NBF = 128
OCC = 4
VIRT = 112
HALF = VIRT // 2
TILE_Q = 4
STEPS = ROWS_Q // TILE_Q
SLOTS = 8
DEVS = 8
COLS = 4


def iota(shape, dim):
    return lax.broadcasted_iota(jnp.int32, shape, dim)


def one_hot(cond):
    return jnp.where(cond, 1.0, 0.0).astype(BF16)


def dot(a, b):
    return jnp.dot(a, b, preferred_element_type=F32)


def dot_nt(a, b):
    return lax.dot_general(a, b, (((1,), (1,)), ((), ())), preferred_element_type=F32)


def dot_tn(a, b):
    return lax.dot_general(a, b, (((0,), (0,)), ((), ())), preferred_element_type=F32)


def kernel(a_hbm, co_hbm, cv_hbm, out_ref, abuf, co_ref, cv_ref, lhs1, cv2, w2, cvx, t1, sendbuf, recv,
           a_sem, c_sem, send_sem, recv_sem):
    row, col = lax.axis_index("dev2"), lax.axis_index("dev")
    me = row * COLS + col

    def fetch(step, slot):
        return pltpu.make_async_copy(a_hbm.at[:, pl.ds(step * TILE_Q, TILE_Q)], abuf.at[slot], a_sem.at[slot])

    co_copy = pltpu.make_async_copy(co_hbm, co_ref, c_sem.at[0])
    cv_copy = pltpu.make_async_copy(cv_hbm, cv_ref, c_sem.at[1])
    co_copy.start()
    cv_copy.start()
    for s in range(SLOTS):
        fetch(s, s).start()

    def peer(k):
        to = lax.rem(me + k, DEVS)
        return to, {"dev2": to // COLS, "dev": lax.rem(to, COLS)}

    barrier = pltpu.get_barrier_semaphore()
    for k in range(1, DEVS):
        pl.semaphore_signal(barrier, inc=1, device_id=peer(k)[1], device_id_type=MESH)

    co_copy.wait()
    cv_copy.wait()
    co, cv = co_ref[...], cv_ref[...]

    r16, c4 = iota((16, OCC), 0), iota((16, OCC), 1)
    co_t = dot_nt(one_hot(r16 % OCC == c4), co)
    r16 = iota((16, NBF), 0)
    lhs1[...] = jnp.concatenate(
        [jnp.where(r16 // OCC == k, co_t, 0.0) for k in range(2)], axis=1).astype(BF16)

    co_i = dot_nt(one_hot(iota((32, OCC), 0) % OCC == iota((32, OCC), 1)), co).astype(BF16)
    r, c = iota((NBF, 256), 0), iota((NBF, 256), 1)
    spread = dot(co_i, one_hot(r == col * ROWS_P + (c % NBF) // OCC))
    r, c = iota((32, 256), 0), iota((32, 256), 1)
    w2[...] = jnp.where(((r // OCC) % 2 == c // NBF) & (r // 8 == c % OCC), spread, 0.0).astype(BF16)

    b, c = iota((VIRT, 256), 0), iota((VIRT, 256), 1)
    halves = dot(cv, one_hot((b == (c // NBF) * HALF + c % 64) & (c % 64 < HALF)))
    c = iota((NBF, 256), 1)
    for par in range(2):
        cv2[par * NBF:(par + 1) * NBF, :] = jnp.where((c // 64) % 2 == par, halves, 0.0).astype(BF16)

    q, c = iota((NBF, 512), 0), iota((NBF, 512), 1)
    rows = dot_tn(cv, one_hot(q == ((c % 256) // OCC) * 2 + c // 256))
    c = iota((VIRT, 512), 1)
    for i in range(OCC):
        cvx[i * VIRT:(i + 1) * VIRT, :] = jnp.where(c % OCC == i, rows, 0.0).astype(BF16)

    pl.semaphore_wait(barrier, DEVS - 1)

    def step_body(step, carry):
        slot = lax.rem(step, SLOTS)
        fetch(step, slot).wait()
        left = lhs1[...]
        for qp in range(2):
            for pp in range(0, 16, 2):
                parts = []
                for p0 in (2 * pp, 2 * pp + 2):
                    rhs = jnp.concatenate(
                        [abuf[slot, p0:p0 + 2, 2 * qp + par].reshape(256, NBF) for par in range(2)], axis=1)
                    parts.append(dot(left, rhs)[:8])
                at = qp * 128 + pp * 8
                t1[at:at + 16, :] = jnp.concatenate(parts, axis=0).astype(BF16)
        half = dot(t1[...], cv2[...]).astype(BF16)
        e_part = dot(w2[...], half)
        for j in range(OCC):
            for h in range(2):
                sendbuf[step, 2 * j + h] = e_part[8 * j:8 * j + 8, h * NBF:(h + 1) * NBF]
        recv[step, me] = sendbuf[step, me]
        for k in range(1, DEVS):
            to, where = peer(k)
            pltpu.make_async_remote_copy(
                src_ref=sendbuf.at[step, to], dst_ref=recv.at[step, me],
                send_sem=send_sem, recv_sem=recv_sem.at[step],
                device_id=where, device_id_type=MESH).start()

        @pl.when(step + SLOTS < STEPS)
        def _():
            fetch(step + SLOTS, slot).start()

        return carry

    lax.fori_loop(0, STEPS, step_body, 0)

    def arrived(step, carry):
        view = recv.at[step, pl.ds(0, DEVS - 1)]
        pltpu.make_async_copy(view, view, recv_sem.at[step]).wait()
        return carry

    lax.fori_loop(0, STEPS, arrived, 0)
    sums = []
    for r in range(2):
        part = recv[:, COLS * r] + recv[:, COLS * r + 1]
        part += recv[:, COLS * r + 2] + recv[:, COLS * r + 3]
        sums.append(part.reshape(STEPS * 8, NBF))
    even = jnp.concatenate(sums, axis=0)
    both = jnp.concatenate([even, pltpu.roll(even, 64, 1)], axis=0)
    high = both.astype(BF16)
    rest = both - high.astype(F32)
    mid = rest.astype(BF16)
    low = (rest - mid.astype(F32)).astype(BF16)
    left = cvx[...]
    total = dot(left, high) + dot(left, mid) + dot(left, low)
    for i in range(OCC):
        out_ref[i] = total[i * VIRT:(i + 1) * VIRT, :HALF]

    sent = sendbuf.at[:, pl.ds(0, DEVS - 1)]
    pltpu.make_async_copy(sent, sent, send_sem).wait()


def solution(mesh):
    def local_block(ao_blk, c_occ, c_virt):
        hbm = pl.BlockSpec(memory_space=pltpu.HBM)
        return pl.pallas_call(
            kernel,
            out_shape=jax.ShapeDtypeStruct((OCC, VIRT, HALF), F32),
            in_specs=[hbm] * 3,
            out_specs=pl.BlockSpec(memory_space=pltpu.VMEM),
            scratch_shapes=[
                pltpu.VMEM((SLOTS, ROWS_P, TILE_Q, NBF, NBF), BF16),
                pltpu.VMEM((NBF, OCC), BF16),
                pltpu.VMEM((NBF, VIRT), BF16),
                pltpu.VMEM((16, 256), BF16),
                pltpu.VMEM((256, 256), BF16),
                pltpu.VMEM((32, 256), BF16),
                pltpu.VMEM((OCC * VIRT, 512), BF16),
                pltpu.VMEM((256, 256), BF16),
                pltpu.VMEM((STEPS, DEVS, 8, NBF), F32),
                pltpu.VMEM((STEPS, DEVS, 8, NBF), F32),
                pltpu.SemaphoreType.DMA((SLOTS,)),
                pltpu.SemaphoreType.DMA((2,)),
                pltpu.SemaphoreType.DMA,
                pltpu.SemaphoreType.DMA((STEPS,)),
            ],
            compiler_params=pltpu.CompilerParams(
                collective_id=0, has_side_effects=True, vmem_limit_bytes=48 * 1024 * 1024),
        )(ao_blk, c_occ, c_virt)

    return jax.shard_map(
        local_block, mesh=mesh,
        in_specs=(P(("frag", "dev"), "dev2", None, None), P("frag", None), P("frag", None)),
        out_specs=P("frag", None, ("dev2", "dev")),
        check_vma=False)
```

```python
import functools

import jax
import jax.numpy as jnp
from jax import lax
from jax.experimental import pallas as pl
from jax.experimental.pallas import tpu as pltpu
from jax.sharding import PartitionSpec as P

MESH = pl.DeviceIdType.MESH
F32 = jnp.float32
BF16 = jnp.bfloat16

ROWS_P = 32
ROWS_Q = 64
NBF = 128
OCC = 4
VIRT = 112
HALF = VIRT // 2
TILE_Q = 4
STEPS = ROWS_Q // TILE_Q
SLOTS = 8
DEVS = 8
COLS = 4


def iota(shape, dim):
    return lax.broadcasted_iota(jnp.int32, shape, dim)


def one_hot(cond):
    return jnp.where(cond, 1.0, 0.0).astype(BF16)


def dot(a, b):
    return jnp.dot(a, b, preferred_element_type=F32)


def dot_nt(a, b):
    return lax.dot_general(a, b, (((1,), (1,)), ((), ())), preferred_element_type=F32)


def dot_tn(a, b):
    return lax.dot_general(a, b, (((0,), (0,)), ((), ())), preferred_element_type=F32)


def kernel(a_hbm, co_hbm, cv_hbm, recv, cvx, abuf, co_ref, cv_ref, lhs1, cv2, w2, t1, sendbuf,
           a_sem, c_sem, send_sem, recv_sem):
    row, col = lax.axis_index("dev2"), lax.axis_index("dev")
    me = row * COLS + col

    def fetch(step, slot):
        return pltpu.make_async_copy(a_hbm.at[:, pl.ds(step * TILE_Q, TILE_Q)], abuf.at[slot], a_sem.at[slot])

    co_copy = pltpu.make_async_copy(co_hbm, co_ref, c_sem.at[0])
    cv_copy = pltpu.make_async_copy(cv_hbm, cv_ref, c_sem.at[1])
    co_copy.start()
    cv_copy.start()
    for s in range(SLOTS):
        fetch(s, s).start()

    def peer(k):
        to = lax.rem(me + k, DEVS)
        return to, {"dev2": to // COLS, "dev": lax.rem(to, COLS)}

    barrier = pltpu.get_barrier_semaphore()
    for k in range(1, DEVS):
        pl.semaphore_signal(barrier, inc=1, device_id=peer(k)[1], device_id_type=MESH)

    co_copy.wait()
    cv_copy.wait()
    co, cv = co_ref[...], cv_ref[...]

    co_t = dot(one_hot(iota((16, OCC), 0) % OCC == iota((16, OCC), 1)), co)
    r16 = iota((16, NBF), 0)
    lhs1[...] = jnp.concatenate(
        [jnp.where(r16 // OCC == k, co_t, 0.0) for k in range(2)], axis=1).astype(BF16)

    co_i = dot(one_hot(iota((32, OCC), 0) % OCC == iota((32, OCC), 1)), co).astype(BF16)
    r, c = iota((NBF, 256), 0), iota((NBF, 256), 1)
    spread = dot(co_i, one_hot(r == col * ROWS_P + (c % NBF) // OCC))
    r, c = iota((32, 256), 0), iota((32, 256), 1)
    w2[...] = jnp.where(((r // OCC) % 2 == c // NBF) & (r // 8 == c % OCC), spread, 0.0).astype(BF16)

    b, c = iota((VIRT, 256), 0), iota((VIRT, 256), 1)
    halves = dot_tn(cv, one_hot((b == (c // NBF) * HALF + c % 64) & (c % 64 < HALF)))
    c = iota((NBF, 256), 1)
    for par in range(2):
        cv2[par * NBF:(par + 1) * NBF, :] = jnp.where((c // 64) % 2 == par, halves, 0.0).astype(BF16)

    wide = jnp.concatenate([cv, jnp.zeros((NBF - VIRT, NBF), BF16)], axis=0)
    r, q = iota((512, NBF), 0), iota((512, NBF), 1)
    rows = dot_nt(one_hot(q == ((r % 256) // OCC) * 2 + r // 256), wide)
    for i in range(OCC):
        cvx[:, i * NBF:(i + 1) * NBF] = jnp.where(r % OCC == i, rows, 0.0).astype(BF16)

    pl.semaphore_wait(barrier, DEVS - 1)

    def step_body(step, carry):
        slot = lax.rem(step, SLOTS)
        fetch(step, slot).wait()
        left = lhs1[...]
        for qp in range(2):
            for pp in range(0, 16, 2):
                parts = []
                for p0 in (2 * pp, 2 * pp + 2):
                    rhs = jnp.concatenate(
                        [abuf[slot, p0:p0 + 2, 2 * qp + par].reshape(256, NBF) for par in range(2)], axis=1)
                    parts.append(dot(left, rhs)[:8])
                at = qp * 128 + pp * 8
                t1[at:at + 16, :] = jnp.concatenate(parts, axis=0).astype(BF16)
        half = dot(t1[...], cv2[...]).astype(BF16)
        e_part = dot(w2[...], half)
        for j in range(OCC):
            for h in range(2):
                sendbuf[step, 2 * j + h] = e_part[8 * j:8 * j + 8, h * NBF:(h + 1) * NBF]
        recv[step, me] = sendbuf[step, me]
        for k in range(1, DEVS):
            to, where = peer(k)
            pltpu.make_async_remote_copy(
                src_ref=sendbuf.at[step, to], dst_ref=recv.at[step, me],
                send_sem=send_sem, recv_sem=recv_sem.at[step],
                device_id=where, device_id_type=MESH).start()

        @pl.when(step + SLOTS < STEPS)
        def _():
            fetch(step + SLOTS, slot).start()

        return carry

    lax.fori_loop(0, STEPS, step_body, 0)

    def arrived(step, carry):
        view = recv.at[step, pl.ds(0, DEVS - 1)]
        pltpu.make_async_copy(view, view, recv_sem.at[step]).wait()
        return carry

    lax.fori_loop(0, STEPS, arrived, 0)
    sent = sendbuf.at[:, pl.ds(0, DEVS - 1)]
    pltpu.make_async_copy(sent, sent, send_sem).wait()


def finish(recv, cvx, out_ref):
    sums = []
    for r in range(2):
        part = recv[:, COLS * r] + recv[:, COLS * r + 1]
        part += recv[:, COLS * r + 2] + recv[:, COLS * r + 3]
        sums.append(part.reshape(STEPS * 8, NBF).T)
    half = jnp.concatenate(sums, axis=1)
    both = jnp.concatenate([half[:64], half[64:]], axis=1)
    high = both.astype(BF16)
    rest = both - high.astype(F32)
    mid = rest.astype(BF16)
    low = (rest - mid.astype(F32)).astype(BF16)
    right = cvx[...]
    total = dot(high, right) + dot(mid, right) + dot(low, right)
    for i in range(OCC):
        out_ref[i] = total[:HALF, i * NBF:i * NBF + VIRT]


def solution(mesh):
    def local_block(ao_blk, c_occ, c_virt):
        hbm = pl.BlockSpec(memory_space=pltpu.HBM)
        vmem = pl.BlockSpec(memory_space=pltpu.VMEM)
        recv, cvx = pl.pallas_call(
            kernel,
            out_shape=[
                jax.ShapeDtypeStruct((STEPS, DEVS, 8, NBF), F32),
                jax.ShapeDtypeStruct((512, 512), BF16),
            ],
            in_specs=[hbm] * 3,
            out_specs=[vmem] * 2,
            scratch_shapes=[
                pltpu.VMEM((SLOTS, ROWS_P, TILE_Q, NBF, NBF), BF16),
                pltpu.VMEM((OCC, NBF), BF16),
                pltpu.VMEM((VIRT, NBF), BF16),
                pltpu.VMEM((16, 256), BF16),
                pltpu.VMEM((256, 256), BF16),
                pltpu.VMEM((32, 256), BF16),
                pltpu.VMEM((256, 256), BF16),
                pltpu.VMEM((STEPS, DEVS, 8, NBF), F32),
                pltpu.SemaphoreType.DMA((SLOTS,)),
                pltpu.SemaphoreType.DMA((2,)),
                pltpu.SemaphoreType.DMA,
                pltpu.SemaphoreType.DMA((STEPS,)),
            ],
            compiler_params=pltpu.CompilerParams(
                collective_id=0, has_side_effects=True, vmem_limit_bytes=48 * 1024 * 1024),
        )(ao_blk, pltpu.with_memory_space_constraint(c_occ.T, pltpu.HBM),
          pltpu.with_memory_space_constraint(c_virt.T, pltpu.HBM))
        out = pl.pallas_call(
            finish,
            out_shape=jax.ShapeDtypeStruct((OCC, HALF, VIRT), F32),
            in_specs=[vmem] * 2,
            out_specs=vmem,
            compiler_params=pltpu.CompilerParams(vmem_limit_bytes=8 * 1024 * 1024),
        )(recv, cvx)
        return jnp.swapaxes(out, 1, 2)

    return jax.shard_map(
        local_block, mesh=mesh,
        in_specs=(P(("frag", "dev"), "dev2", None, None), P("frag", None), P("frag", None)),
        out_specs=P("frag", None, ("dev2", "dev")),
        check_vma=False)
```

```python
import functools

import jax
import jax.numpy as jnp
from jax import lax
from jax.experimental import pallas as pl
from jax.experimental.pallas import tpu as pltpu
from jax.sharding import PartitionSpec as P

MESH = pl.DeviceIdType.MESH
F32 = jnp.float32
BF16 = jnp.bfloat16

ROWS_P = 32
ROWS_Q = 64
NBF = 128
OCC = 4
VIRT = 112
HALF = VIRT // 2
TILE_Q = 4
STEPS = ROWS_Q // TILE_Q
SLOTS = 8
DEVS = 8
COLS = 4


def iota(shape, dim):
    return lax.broadcasted_iota(jnp.int32, shape, dim)


def one_hot(cond):
    return jnp.where(cond, 1.0, 0.0).astype(BF16)


def dot(a, b):
    return jnp.dot(a, b, preferred_element_type=F32)


def dot_nt(a, b):
    return lax.dot_general(a, b, (((1,), (1,)), ((), ())), preferred_element_type=F32)


def dot_tn(a, b):
    return lax.dot_general(a, b, (((0,), (0,)), ((), ())), preferred_element_type=F32)


def kernel(a_hbm, co_hbm, cv_hbm, recv, cvx, abuf, co_ref, cv_ref, lhs1, cv2, w2, t1, sendbuf,
           a_sem, c_sem, send_sem, recv_sem):
    row, col = lax.axis_index("dev2"), lax.axis_index("dev")
    me = row * COLS + col

    def fetch(step, slot):
        return pltpu.make_async_copy(a_hbm.at[:, pl.ds(step * TILE_Q, TILE_Q)], abuf.at[slot], a_sem.at[slot])

    co_copy = pltpu.make_async_copy(co_hbm, co_ref, c_sem.at[0])
    cv_copy = pltpu.make_async_copy(cv_hbm, cv_ref, c_sem.at[1])
    co_copy.start()
    cv_copy.start()
    for s in range(SLOTS):
        fetch(s, s).start(priority=1)

    def peer(k):
        to = lax.rem(me + k, DEVS)
        return to, {"dev2": to // COLS, "dev": lax.rem(to, COLS)}

    barrier = pltpu.get_barrier_semaphore()
    for k in range(1, DEVS):
        pl.semaphore_signal(barrier, inc=1, device_id=peer(k)[1], device_id_type=MESH)

    co_copy.wait()
    cv_copy.wait()
    co, cv = co_ref[...], cv_ref[...]

    co_t = dot(one_hot(iota((16, OCC), 0) % OCC == iota((16, OCC), 1)), co)
    r16 = iota((16, NBF), 0)
    lhs1[...] = jnp.concatenate(
        [jnp.where(r16 // OCC == k, co_t, 0.0) for k in range(2)], axis=1).astype(BF16)

    co_i = dot(one_hot(iota((32, OCC), 0) % OCC == iota((32, OCC), 1)), co).astype(BF16)
    r, c = iota((NBF, 256), 0), iota((NBF, 256), 1)
    spread = dot(co_i, one_hot(r == col * ROWS_P + (c % NBF) // OCC))
    r, c = iota((32, 256), 0), iota((32, 256), 1)
    w2[...] = jnp.where(((r // OCC) % 2 == c // NBF) & (r // 8 == c % OCC), spread, 0.0).astype(BF16)

    b, c = iota((VIRT, 256), 0), iota((VIRT, 256), 1)
    halves = dot_tn(cv, one_hot((b == (c // NBF) * HALF + c % 64) & (c % 64 < HALF)))
    c = iota((NBF, 256), 1)
    for par in range(2):
        cv2[par * NBF:(par + 1) * NBF, :] = jnp.where((c // 64) % 2 == par, halves, 0.0).astype(BF16)

    wide = jnp.concatenate([cv, jnp.zeros((NBF - VIRT, NBF), BF16)], axis=0)
    r, q = iota((512, NBF), 0), iota((512, NBF), 1)
    rows = dot_nt(one_hot(q == ((r % 256) // OCC) * 2 + r // 256), wide)
    for i in range(OCC):
        cvx[:, i * NBF:(i + 1) * NBF] = jnp.where(r % OCC == i, rows, 0.0).astype(BF16)

    pl.semaphore_wait(barrier, DEVS - 1)

    def step_body(step, carry):
        slot = lax.rem(step, SLOTS)
        fetch(step, slot).wait()
        left = lhs1[...]
        for qp in range(2):
            for pp in range(0, 16, 2):
                parts = []
                for p0 in (2 * pp, 2 * pp + 2):
                    rhs = jnp.concatenate(
                        [abuf[slot, p0:p0 + 2, 2 * qp + par].reshape(256, NBF) for par in range(2)], axis=1)
                    parts.append(dot(left, rhs)[:8])
                at = qp * 128 + pp * 8
                t1[at:at + 16, :] = jnp.concatenate(parts, axis=0).astype(BF16)
        half = dot(t1[...], cv2[...]).astype(BF16)
        e_part = dot(w2[...], half)
        for j in range(OCC):
            for h in range(2):
                sendbuf[step, 2 * j + h] = e_part[8 * j:8 * j + 8, h * NBF:(h + 1) * NBF]
        recv[step, me] = sendbuf[step, me]
        for k in range(1, DEVS):
            to, where = peer(k)
            pltpu.make_async_remote_copy(
                src_ref=sendbuf.at[step, to], dst_ref=recv.at[step, me],
                send_sem=send_sem, recv_sem=recv_sem.at[step],
                device_id=where, device_id_type=MESH).start()

        @pl.when(step + SLOTS < STEPS)
        def _():
            fetch(step + SLOTS, slot).start(priority=1)

        return carry

    lax.fori_loop(0, STEPS, step_body, 0)

    def arrived(step, carry):
        view = recv.at[step, pl.ds(0, DEVS - 1)]
        pltpu.make_async_copy(view, view, recv_sem.at[step]).wait()
        return carry

    lax.fori_loop(0, STEPS, arrived, 0)
    sent = sendbuf.at[:, pl.ds(0, DEVS - 1)]
    pltpu.make_async_copy(sent, sent, send_sem).wait()


def finish(recv, cvx, out_ref):
    sums = []
    for r in range(2):
        part = recv[:, COLS * r] + recv[:, COLS * r + 1]
        part += recv[:, COLS * r + 2] + recv[:, COLS * r + 3]
        sums.append(part.reshape(STEPS * 8, NBF).T)
    half = jnp.concatenate(sums, axis=1)
    both = jnp.concatenate([half[:64], half[64:]], axis=1)
    high = both.astype(BF16)
    rest = both - high.astype(F32)
    mid = rest.astype(BF16)
    low = (rest - mid.astype(F32)).astype(BF16)
    right = cvx[...]
    total = dot(high, right) + dot(mid, right) + dot(low, right)
    for i in range(OCC):
        out_ref[i] = total[:HALF, i * NBF:i * NBF + VIRT]


def solution(mesh):
    def local_block(ao_blk, c_occ, c_virt):
        hbm = pl.BlockSpec(memory_space=pltpu.HBM)
        vmem = pl.BlockSpec(memory_space=pltpu.VMEM)
        recv, cvx = pl.pallas_call(
            kernel,
            out_shape=[
                jax.ShapeDtypeStruct((STEPS, DEVS, 8, NBF), F32),
                jax.ShapeDtypeStruct((512, 512), BF16),
            ],
            in_specs=[hbm] * 3,
            out_specs=[vmem] * 2,
            scratch_shapes=[
                pltpu.VMEM((SLOTS, ROWS_P, TILE_Q, NBF, NBF), BF16),
                pltpu.VMEM((OCC, NBF), BF16),
                pltpu.VMEM((VIRT, NBF), BF16),
                pltpu.VMEM((16, 256), BF16),
                pltpu.VMEM((256, 256), BF16),
                pltpu.VMEM((32, 256), BF16),
                pltpu.VMEM((256, 256), BF16),
                pltpu.VMEM((STEPS, DEVS, 8, NBF), F32),
                pltpu.SemaphoreType.DMA((SLOTS,)),
                pltpu.SemaphoreType.DMA((2,)),
                pltpu.SemaphoreType.DMA,
                pltpu.SemaphoreType.DMA((STEPS,)),
            ],
            compiler_params=pltpu.CompilerParams(
                collective_id=0, has_side_effects=True, vmem_limit_bytes=48 * 1024 * 1024),
        )(ao_blk, pltpu.with_memory_space_constraint(c_occ.T, pltpu.HBM),
          pltpu.with_memory_space_constraint(c_virt.T, pltpu.HBM))
        out = pl.pallas_call(
            finish,
            out_shape=jax.ShapeDtypeStruct((OCC, HALF, VIRT), F32),
            in_specs=[vmem] * 2,
            out_specs=vmem,
            compiler_params=pltpu.CompilerParams(vmem_limit_bytes=8 * 1024 * 1024),
        )(recv, cvx)
        return jnp.swapaxes(out, 1, 2)

    return jax.shard_map(
        local_block, mesh=mesh,
        in_specs=(P(("frag", "dev"), "dev2", None, None), P("frag", None), P("frag", None)),
        out_specs=P("frag", None, ("dev2", "dev")),
        check_vma=False)
```

```python
import functools

import jax
import jax.numpy as jnp
from jax import lax
from jax.experimental import pallas as pl
from jax.experimental.pallas import tpu as pltpu
from jax.sharding import PartitionSpec as P

MESH = pl.DeviceIdType.MESH
F32 = jnp.float32
BF16 = jnp.bfloat16

ROWS_P = 32
ROWS_Q = 64
NBF = 128
OCC = 4
VIRT = 112
HALF = VIRT // 2
TILE_Q = 4
STEPS = ROWS_Q // TILE_Q
SLOTS = 8
DEVS = 8
COLS = 4
PIECES = ((14, 0, 16), (14, 16, 16), (15, 0, 8), (15, 8, 8), (15, 16, 8), (15, 24, 8))
LAST = STEPS - 1
LOOPED = STEPS - 2


def iota(shape, dim):
    return lax.broadcasted_iota(jnp.int32, shape, dim)


def one_hot(cond):
    return jnp.where(cond, 1.0, 0.0).astype(BF16)


def dot(a, b):
    return jnp.dot(a, b, preferred_element_type=F32)


def dot_nt(a, b):
    return lax.dot_general(a, b, (((1,), (1,)), ((), ())), preferred_element_type=F32)


def dot_tn(a, b):
    return lax.dot_general(a, b, (((0,), (0,)), ((), ())), preferred_element_type=F32)


def split(x):
    high = x.astype(BF16)
    rest = x - high.astype(F32)
    mid = rest.astype(BF16)
    return high, mid, (rest - mid.astype(F32)).astype(BF16)


def kernel(*refs):
    pl.run_scoped(
        functools.partial(body, *refs),
        pltpu.SemaphoreType.DMA((SLOTS,)),
        pltpu.SemaphoreType.DMA((len(PIECES),)),
        pltpu.SemaphoreType.DMA((2,)),
    )


def body(a_hbm, co_hbm, cv_hbm, recv, base, cvd, abuf, co_ref, cv_ref, lhs1, cv2, w2, w2a, w2b, cvx, t1, sendbuf,
         send_sem, recv_sem, a_sem, l_sem, c_sem):
    row, col = lax.axis_index("dev2"), lax.axis_index("dev")
    me = row * COLS + col

    def fetch(step, slot):
        return pltpu.make_async_copy(a_hbm.at[:, pl.ds(step * TILE_Q, TILE_Q)], abuf.at[slot], a_sem.at[slot])

    def fetch_piece(n):
        step, first, count = PIECES[n]
        part = pl.ds(first, count)
        return pltpu.make_async_copy(
            a_hbm.at[part, pl.ds(step * TILE_Q, TILE_Q)], abuf.at[step % SLOTS, part], l_sem.at[n])

    co_copy = pltpu.make_async_copy(co_hbm, co_ref, c_sem.at[0])
    cv_copy = pltpu.make_async_copy(cv_hbm, cv_ref, c_sem.at[1])
    co_copy.start()
    cv_copy.start()
    for s in range(SLOTS):
        fetch(s, s).start(priority=1)

    x, core = col // 2, lax.rem(col, 2)
    far_row, far_x = 1 - row, 1 - x
    peers = [(far_row, 2 * far_x), (far_row, 2 * far_x + 1), (far_row, 2 * x), (far_row, 2 * x + 1),
             (row, 2 * far_x), (row, 2 * far_x + 1), (row, 2 * x + 1 - core)]

    barrier = pltpu.get_barrier_semaphore()
    for r, c in peers:
        pl.semaphore_signal(barrier, inc=1, device_id={"dev2": r, "dev": c}, device_id_type=MESH)

    co_copy.wait()
    cv_copy.wait()
    co, cv = co_ref[...], cv_ref[...]

    co_t = dot(one_hot(iota((16, OCC), 0) % OCC == iota((16, OCC), 1)), co)
    r16 = iota((16, NBF), 0)
    lhs1[...] = jnp.concatenate(
        [jnp.where(r16 // OCC == k, co_t, 0.0) for k in range(2)], axis=1).astype(BF16)

    co_i = dot(one_hot(iota((32, OCC), 0) % OCC == iota((32, OCC), 1)), co).astype(BF16)

    def spread(groups):
        width = sum(2 * count * OCC for _, count in groups)
        r, c = iota((NBF, width), 0), iota((NBF, width), 1)
        c32, r32 = iota((32, width), 1), iota((32, width), 0)
        pick, qp, at = r < 0, c32 < 0, 0
        for first, count in groups:
            half = count * OCC
            pick |= (r == col * ROWS_P + first + (c - at) % half // OCC) & (c >= at) & (c < at + 2 * half)
            qp |= (r32 // OCC % 2 == (c32 - at) // half) & (c32 >= at) & (c32 < at + 2 * half)
            at += 2 * half
        placed = dot(co_i, one_hot(pick))
        return jnp.where(qp & (r32 // 8 == c32 % OCC), placed, 0.0).astype(BF16)

    w2[...] = spread([(0, ROWS_P)])
    w2a[...] = spread([(0, 16)])
    w2b[...] = spread([(16, 8), (24, 8)])

    b, c = iota((VIRT, 256), 0), iota((VIRT, 256), 1)
    halves = dot_tn(cv, one_hot((b == (c // NBF) * HALF + c % 64) & (c % 64 < HALF)))
    c = iota((NBF, 256), 1)
    for par in range(2):
        cv2[par * NBF:(par + 1) * NBF, :] = jnp.where((c // 64) % 2 == par, halves, 0.0).astype(BF16)

    wide = jnp.concatenate([cv, jnp.zeros((NBF - VIRT, NBF), BF16)], axis=0)
    r, q = iota((512, NBF), 0), iota((512, NBF), 1)
    rows = dot_nt(one_hot(q == ((r % 256) // OCC) * 2 + r // 256), wide)
    for i in range(OCC):
        cvx[:, i * NBF:(i + 1) * NBF] = jnp.where(r % OCC == i, rows, 0.0).astype(BF16)
    r, q = iota((256, NBF), 0), iota((256, NBF), 1)
    at = (r // 8) % 2 * ROWS_Q + LAST * TILE_Q + (r % 8) // OCC * 2 + r // NBF
    rows = dot_nt(one_hot((q == at) & (r % NBF < 48)), wide)
    for i in range(OCC):
        cvd[:, i * NBF:(i + 1) * NBF] = jnp.where(r % OCC == i, rows, 0.0).astype(BF16)

    pl.semaphore_wait(barrier, DEVS - 1)

    def contract_r(slot, blocks):
        left = lhs1[...]
        for qp, pb, at in blocks:
            parts = []
            for p0 in (pb, pb + 2):
                rhs = jnp.concatenate(
                    [abuf[slot, p0:p0 + 2, 2 * qp + par].reshape(256, NBF) for par in range(2)], axis=1)
                parts.append(dot(left, rhs)[:8])
            t1[at:at + 16, :] = jnp.concatenate(parts, axis=0).astype(BF16)

    def contract_s(t_one):
        return dot(t_one, cv2[...]).astype(BF16)

    def pack(step, e_part):
        for j in range(OCC):
            for h in range(2):
                sendbuf[step, 2 * j + h] = e_part[8 * j:8 * j + 8, h * NBF:(h + 1) * NBF]

    def send(step, sem):
        for r, c in peers:
            pltpu.make_async_remote_copy(
                src_ref=sendbuf.at[step, r * COLS + c], dst_ref=recv.at[step, me],
                send_sem=send_sem, recv_sem=recv_sem.at[sem],
                device_id={"dev2": r, "dev": c}, device_id_type=MESH).start()
        recv[step, me] = sendbuf[step, me]

    def blocks(first, count, at):
        return [(qp, first + pb, at + qp * count * OCC + pb * OCC) for qp in range(2) for pb in range(0, count, 4)]

    whole = blocks(0, ROWS_P, 0)
    upper = [b for b in whole if b[1] < 16]
    lower = [b for b in whole if b[1] >= 16]

    def refill(step, slot):
        @pl.when(step + SLOTS < LOOPED)
        def _():
            fetch(step + SLOTS, slot).start(priority=1)

        for n in range(len(PIECES)):
            @pl.when(step + SLOTS == PIECES[n][0])
            def _():
                fetch_piece(n).start(priority=1)

    def beside(step, slot, mine):
        half = contract_s(t1[...])
        contract_r(slot, mine[:4])
        e_part = dot(w2[...], half)
        contract_r(slot, mine[4:])
        pack(step - 1, e_part)
        send(step - 1, 0)

    def step_body(step, carry):
        slot = lax.rem(step, SLOTS)
        fetch(step, slot).wait()
        beside(step, slot, whole)
        refill(step, slot)
        return carry

    fetch(0, 0).wait()
    contract_r(0, whole)
    refill(0, 0)
    lax.fori_loop(1, LOOPED, step_body, 0)

    slot = LOOPED % SLOTS
    fetch_piece(0).wait()
    beside(LOOPED, slot, upper)
    fetch_piece(1).wait()
    contract_r(slot, lower)
    slot = LAST % SLOTS
    fetch_piece(2).wait()
    beside(LAST, slot, [b for b in blocks(0, 16, 0) if b[1] < 8])
    fetch_piece(3).wait()
    contract_r(slot, [b for b in blocks(0, 16, 0) if b[1] >= 8])
    fetch_piece(4).wait()
    half = contract_s(t1[:128, :])
    contract_r(slot, blocks(16, 8, 128))
    e_part = dot(w2a[...], half)
    fetch_piece(5).wait()
    contract_r(slot, blocks(24, 8, 192))
    half = jnp.concatenate([contract_s(t1[128:192, :]), contract_s(t1[192:, :])], axis=0)
    e_part += dot(w2b[...], half)
    pack(LAST, e_part)
    send(LAST, 1)

    def arrived(view, sem):
        pltpu.make_async_copy(view, view, recv_sem.at[sem]).wait()

    arrived(recv.at[pl.ds(0, LAST), pl.ds(0, DEVS - 1)], 0)
    sums = []
    for r in range(2):
        part = recv[:LAST, COLS * r] + recv[:LAST, COLS * r + 1]
        part += recv[:LAST, COLS * r + 2] + recv[:LAST, COLS * r + 3]
        part = jnp.concatenate([part.reshape(LAST * 8, NBF), jnp.zeros((8, NBF), F32)], axis=0)
        sums.append(part.T)
    half = jnp.concatenate(sums, axis=1)
    high, mid, low = split(jnp.concatenate([half[:64], half[64:]], axis=1))
    right = cvx[...]
    base[...] = dot(high, right) + dot(mid, right) + dot(low, right)

    arrived(recv.at[LAST, pl.ds(0, DEVS - 1)], 1)
    sent = sendbuf.at[:, pl.ds(0, DEVS - 1)]
    pltpu.make_async_copy(sent, sent, send_sem).wait()


def finish(recv, base, cvd, out_ref):
    sums = []
    for r in range(2):
        part = recv[STEPS - 1, COLS * r] + recv[STEPS - 1, COLS * r + 1]
        sums.append(part + (recv[STEPS - 1, COLS * r + 2] + recv[STEPS - 1, COLS * r + 3]))
    parts = [x.astype(F32) for x in split(jnp.concatenate(sums, axis=0))]
    turned = jnp.concatenate(parts + [jnp.zeros((NBF - 48, NBF), F32)], axis=0).T.astype(BF16)
    total = base[...] + dot(jnp.concatenate([turned[:64], turned[64:]], axis=1), cvd[...])
    for i in range(OCC):
        out_ref[i] = total[:HALF, i * NBF:i * NBF + VIRT]


def solution(mesh):
    def local_block(ao_blk, c_occ, c_virt):
        hbm = pl.BlockSpec(memory_space=pltpu.HBM)
        vmem = pl.BlockSpec(memory_space=pltpu.VMEM)
        recv, base, cvd = pl.pallas_call(
            kernel,
            out_shape=[
                jax.ShapeDtypeStruct((STEPS, DEVS, 8, NBF), F32),
                jax.ShapeDtypeStruct((64, 512), F32),
                jax.ShapeDtypeStruct((256, 512), BF16),
            ],
            in_specs=[hbm] * 3,
            out_specs=[vmem] * 3,
            scratch_shapes=[
                pltpu.VMEM((SLOTS, ROWS_P, TILE_Q, NBF, NBF), BF16),
                pltpu.VMEM((OCC, NBF), BF16),
                pltpu.VMEM((VIRT, NBF), BF16),
                pltpu.VMEM((16, 256), BF16),
                pltpu.VMEM((256, 256), BF16),
                pltpu.VMEM((32, 256), BF16),
                pltpu.VMEM((32, NBF), BF16),
                pltpu.VMEM((32, NBF), BF16),
                pltpu.VMEM((512, 512), BF16),
                pltpu.VMEM((256, 256), BF16),
                pltpu.VMEM((STEPS, DEVS, 8, NBF), F32),
                pltpu.SemaphoreType.DMA,
                pltpu.SemaphoreType.DMA((2,)),
            ],
            compiler_params=pltpu.CompilerParams(
                collective_id=0, has_side_effects=True, vmem_limit_bytes=48 * 1024 * 1024),
        )(ao_blk, pltpu.with_memory_space_constraint(c_occ.T, pltpu.HBM),
          pltpu.with_memory_space_constraint(c_virt.T, pltpu.HBM))
        out = pl.pallas_call(
            finish,
            out_shape=jax.ShapeDtypeStruct((OCC, HALF, VIRT), F32),
            in_specs=[vmem] * 3,
            out_specs=vmem,
            compiler_params=pltpu.CompilerParams(vmem_limit_bytes=8 * 1024 * 1024),
        )(recv, base, cvd)
        return jnp.swapaxes(out, 1, 2)

    return jax.shard_map(
        local_block, mesh=mesh,
        in_specs=(P(("frag", "dev"), "dev2", None, None), P("frag", None), P("frag", None)),
        out_specs=P("frag", None, ("dev2", "dev")),
        check_vma=False)
```

```python
import functools

import jax
import jax.numpy as jnp
from jax import lax
from jax.experimental import pallas as pl
from jax.experimental.pallas import tpu as pltpu
from jax.sharding import PartitionSpec as P

MESH = pl.DeviceIdType.MESH
F32 = jnp.float32
BF16 = jnp.bfloat16

ROWS_P = 32
ROWS_Q = 64
NBF = 128
OCC = 4
VIRT = 112
HALF = VIRT // 2
TILE_Q = 4
STEPS = ROWS_Q // TILE_Q
SLOTS = 6
GIVEN = 2
EVERY = 6
DEVS = 8
COLS = 4
PIECES = ((14, 0, 16), (14, 16, 16), (15, 0, 8), (15, 8, 8), (15, 16, 8), (15, 24, 8))
LAST = STEPS - 1
LOOPED = STEPS - 2


def iota(shape, dim):
    return lax.broadcasted_iota(jnp.int32, shape, dim)


def one_hot(cond):
    return jnp.where(cond, 1.0, 0.0).astype(BF16)


def dot(a, b):
    return jnp.dot(a, b, preferred_element_type=F32)


def dot_nt(a, b):
    return lax.dot_general(a, b, (((1,), (1,)), ((), ())), preferred_element_type=F32)


def dot_tn(a, b):
    return lax.dot_general(a, b, (((0,), (0,)), ((), ())), preferred_element_type=F32)


def split(x):
    high = x.astype(BF16)
    rest = x - high.astype(F32)
    mid = rest.astype(BF16)
    return high, mid, (rest - mid.astype(F32)).astype(BF16)


def kernel(*refs):
    pl.run_scoped(
        functools.partial(body, *refs),
        pltpu.SemaphoreType.DMA((SLOTS,)),
        pltpu.SemaphoreType.DMA((len(PIECES),)),
        pltpu.SemaphoreType.DMA((2,)),
    )


def body(a_hbm, co_hbm, cv_hbm, recv, base, cvd, abuf, co_ref, cv_ref, lhs1, cv2, w2, w2a, w2b, cvx, t1, sendbuf,
         send_sem, recv_sem, give_sem, take_sem, a_sem, l_sem, c_sem):
    row, col = lax.axis_index("dev2"), lax.axis_index("dev")
    me = row * COLS + col

    def slot_of(tile):
        return lax.rem(tile - GIVEN, SLOTS)

    def fetch(tile, slot):
        return pltpu.make_async_copy(a_hbm.at[:, pl.ds(tile * TILE_Q, TILE_Q)], abuf.at[slot], a_sem.at[slot])

    def fetch_piece(n):
        tile, first, count = PIECES[n]
        part = pl.ds(first, count)
        return pltpu.make_async_copy(
            a_hbm.at[part, pl.ds(tile * TILE_Q, TILE_Q)], abuf.at[(tile - GIVEN) % SLOTS, part], l_sem.at[n])

    co_copy = pltpu.make_async_copy(co_hbm, co_ref, c_sem.at[0])
    cv_copy = pltpu.make_async_copy(cv_hbm, cv_ref, c_sem.at[1])
    co_copy.start()
    cv_copy.start()
    for s in range(SLOTS):
        fetch(GIVEN + s, s).start(priority=1)

    x, core = col // 2, lax.rem(col, 2)
    far_row, far_x = 1 - row, 1 - x
    peers = [(far_row, 2 * far_x), (far_row, 2 * far_x + 1), (far_row, 2 * x), (far_row, 2 * x + 1),
             (row, 2 * far_x), (row, 2 * far_x + 1), (row, 2 * x + 1 - core)]

    barrier = pltpu.get_barrier_semaphore()
    for r, c in peers:
        pl.semaphore_signal(barrier, inc=1, device_id={"dev2": r, "dev": c}, device_id_type=MESH)
    pl.semaphore_wait(barrier, DEVS - 1)

    other = 2 * x + 1 - core
    gifts = []
    for k in range(GIVEN):
        gifts.append(pltpu.make_async_remote_copy(
            src_ref=a_hbm.at[:, pl.ds(k * TILE_Q, TILE_Q)], dst_ref=abuf.at[SLOTS + k],
            send_sem=give_sem.at[k], recv_sem=take_sem.at[k],
            device_id={"dev2": row, "dev": other}, device_id_type=MESH))
        gifts[k].start()

    co_copy.wait()
    cv_copy.wait()
    co, cv = co_ref[...], cv_ref[...]

    co_t = dot(one_hot(iota((16, OCC), 0) % OCC == iota((16, OCC), 1)), co)
    r16 = iota((16, NBF), 0)
    lhs1[...] = jnp.concatenate(
        [jnp.where(r16 // OCC == k, co_t, 0.0) for k in range(2)], axis=1).astype(BF16)

    co_i = dot(one_hot(iota((32, OCC), 0) % OCC == iota((32, OCC), 1)), co).astype(BF16)

    def spread(dev, groups):
        width = sum(2 * count * OCC for _, count in groups)
        r, c = iota((NBF, width), 0), iota((NBF, width), 1)
        c32, r32 = iota((32, width), 1), iota((32, width), 0)
        pick, qp, at = r < 0, c32 < 0, 0
        for first, count in groups:
            half = count * OCC
            pick |= (r == dev * ROWS_P + first + (c - at) % half // OCC) & (c >= at) & (c < at + 2 * half)
            qp |= (r32 // OCC % 2 == (c32 - at) // half) & (c32 >= at) & (c32 < at + 2 * half)
            at += 2 * half
        placed = dot(co_i, one_hot(pick))
        return jnp.where(qp & (r32 // 8 == c32 % OCC), placed, 0.0).astype(BF16)

    w2[0] = spread(col, [(0, ROWS_P)])
    w2[1] = spread(other, [(0, ROWS_P)])
    w2a[...] = spread(col, [(0, 16)])
    w2b[...] = spread(col, [(16, 8), (24, 8)])

    b, c = iota((VIRT, 256), 0), iota((VIRT, 256), 1)
    halves = dot_tn(cv, one_hot((b == (c // NBF) * HALF + c % 64) & (c % 64 < HALF)))
    c = iota((NBF, 256), 1)
    for par in range(2):
        cv2[par * NBF:(par + 1) * NBF, :] = jnp.where((c // 64) % 2 == par, halves, 0.0).astype(BF16)

    wide = jnp.concatenate([cv, jnp.zeros((NBF - VIRT, NBF), BF16)], axis=0)
    r, q = iota((512, NBF), 0), iota((512, NBF), 1)
    rows = dot_nt(one_hot(q == ((r % 256) // OCC) * 2 + r // 256), wide)
    for i in range(OCC):
        cvx[:, i * NBF:(i + 1) * NBF] = jnp.where(r % OCC == i, rows, 0.0).astype(BF16)
    r, q = iota((256, NBF), 0), iota((256, NBF), 1)
    at = (r // 8) % 2 * ROWS_Q + LAST * TILE_Q + (r % 8) // OCC * 2 + r // NBF
    rows = dot_nt(one_hot((q == at) & (r % NBF < 48)), wide)
    for i in range(OCC):
        cvd[:, i * NBF:(i + 1) * NBF] = jnp.where(r % OCC == i, rows, 0.0).astype(BF16)

    def contract_r(slot, blocks):
        left = lhs1[...]
        for qp, pb, at in blocks:
            parts = []
            for p0 in (pb, pb + 2):
                rhs = jnp.concatenate(
                    [abuf[slot, p0:p0 + 2, 2 * qp + par].reshape(256, NBF) for par in range(2)], axis=1)
                parts.append(dot(left, rhs)[:8])
            t1[at:at + 16, :] = jnp.concatenate(parts, axis=0).astype(BF16)

    def contract_s(t_one):
        return dot(t_one, cv2[...]).astype(BF16)

    def pack(step, e_part):
        for j in range(OCC):
            for h in range(2):
                sendbuf[step, 2 * j + h] = e_part[8 * j:8 * j + 8, h * NBF:(h + 1) * NBF]

    def send(step, sem):
        for r, c in peers:
            pltpu.make_async_remote_copy(
                src_ref=sendbuf.at[step, r * COLS + c], dst_ref=recv.at[step, me],
                send_sem=send_sem, recv_sem=recv_sem.at[sem],
                device_id={"dev2": r, "dev": c}, device_id_type=MESH).start()
        recv[step, me] = sendbuf[step, me]

    def blocks(first, count, at):
        return [(qp, first + pb, at + qp * count * OCC + pb * OCC) for qp in range(2) for pb in range(0, count, 4)]

    whole = blocks(0, ROWS_P, 0)
    upper = [b for b in whole if b[1] < 16]
    lower = [b for b in whole if b[1] >= 16]

    def refill(tile):
        @pl.when(tile + SLOTS < LOOPED)
        def _():
            fetch(tile + SLOTS, slot_of(tile)).start(priority=1)

        for step in range(LOOPED, STEPS):
            @pl.when(tile + SLOTS == step)
            def _():
                for n in range(len(PIECES)):
                    if PIECES[n][0] == step:
                        fetch_piece(n).start(priority=1)

    def beside(slot, mine, before, weights):
        half = contract_s(t1[...])
        contract_r(slot, mine[:4])
        e_part = dot(weights, half)
        contract_r(slot, mine[4:])
        pack(before, e_part)
        send(before, 0)

    def taken(n):
        return (n - 1) // EVERY

    def own(n):
        return GIVEN + n - taken(n)

    def step_body(n, carry):
        theirs, before_theirs = lax.rem(n, EVERY) == 0, (lax.rem(n, EVERY) == 1) & (n > 1)
        slot = jnp.where(theirs, SLOTS + taken(n), slot_of(own(n)))
        before = jnp.where(before_theirs, taken(n) - 1, own(n) - 1)

        for k in range(GIVEN):
            @pl.when(n == (k + 1) * EVERY)
            def _():
                gifts[k].wait_recv()

        @pl.when(jnp.logical_not(theirs))
        def _():
            fetch(own(n), slot_of(own(n))).wait()

        beside(slot, whole, before, w2[jnp.where(before_theirs, 1, 0)])

        @pl.when(jnp.logical_not(theirs))
        def _():
            refill(own(n))

        return carry

    fetch(GIVEN, 0).wait()
    contract_r(0, whole)
    refill(GIVEN)
    lax.fori_loop(1, LOOPED, step_body, 0)

    slot = (LOOPED - GIVEN) % SLOTS
    fetch_piece(0).wait()
    beside(slot, upper, LOOPED - 1, w2[0])
    fetch_piece(1).wait()
    contract_r(slot, lower)
    slot = (LAST - GIVEN) % SLOTS
    fetch_piece(2).wait()
    beside(slot, [b for b in blocks(0, 16, 0) if b[1] < 8], LOOPED, w2[0])
    fetch_piece(3).wait()
    contract_r(slot, [b for b in blocks(0, 16, 0) if b[1] >= 8])
    fetch_piece(4).wait()
    half = contract_s(t1[:128, :])
    contract_r(slot, blocks(16, 8, 128))
    e_part = dot(w2a[...], half)
    fetch_piece(5).wait()
    contract_r(slot, blocks(24, 8, 192))
    half = jnp.concatenate([contract_s(t1[128:192, :]), contract_s(t1[192:, :])], axis=0)
    e_part += dot(w2b[...], half)
    pack(LAST, e_part)
    send(LAST, 1)

    def arrived(view, sem):
        pltpu.make_async_copy(view, view, recv_sem.at[sem]).wait()

    arrived(recv.at[pl.ds(0, LAST), pl.ds(0, DEVS - 1)], 0)
    sums = []
    for r in range(2):
        part = recv[:LAST, COLS * r] + recv[:LAST, COLS * r + 1]
        part += recv[:LAST, COLS * r + 2] + recv[:LAST, COLS * r + 3]
        part = jnp.concatenate([part.reshape(LAST * 8, NBF), jnp.zeros((8, NBF), F32)], axis=0)
        sums.append(part.T)
    half = jnp.concatenate(sums, axis=1)
    high, mid, low = split(jnp.concatenate([half[:64], half[64:]], axis=1))
    right = cvx[...]
    base[...] = dot(high, right) + dot(mid, right) + dot(low, right)

    arrived(recv.at[LAST, pl.ds(0, DEVS - 1)], 1)
    sent = sendbuf.at[:, pl.ds(0, DEVS - 1)]
    pltpu.make_async_copy(sent, sent, send_sem).wait()
    for gift in gifts:
        gift.wait_send()


def finish(recv, base, cvd, out_ref):
    sums = []
    for r in range(2):
        part = recv[STEPS - 1, COLS * r] + recv[STEPS - 1, COLS * r + 1]
        sums.append(part + (recv[STEPS - 1, COLS * r + 2] + recv[STEPS - 1, COLS * r + 3]))
    parts = [x.astype(F32) for x in split(jnp.concatenate(sums, axis=0))]
    turned = jnp.concatenate(parts + [jnp.zeros((NBF - 48, NBF), F32)], axis=0).T.astype(BF16)
    total = base[...] + dot(jnp.concatenate([turned[:64], turned[64:]], axis=1), cvd[...])
    for i in range(OCC):
        out_ref[i] = total[:HALF, i * NBF:i * NBF + VIRT]


def solution(mesh):
    def local_block(ao_blk, c_occ, c_virt):
        hbm = pl.BlockSpec(memory_space=pltpu.HBM)
        vmem = pl.BlockSpec(memory_space=pltpu.VMEM)
        recv, base, cvd = pl.pallas_call(
            kernel,
            out_shape=[
                jax.ShapeDtypeStruct((STEPS, DEVS, 8, NBF), F32),
                jax.ShapeDtypeStruct((64, 512), F32),
                jax.ShapeDtypeStruct((256, 512), BF16),
            ],
            in_specs=[hbm] * 3,
            out_specs=[vmem] * 3,
            scratch_shapes=[
                pltpu.VMEM((SLOTS + GIVEN, ROWS_P, TILE_Q, NBF, NBF), BF16),
                pltpu.VMEM((OCC, NBF), BF16),
                pltpu.VMEM((VIRT, NBF), BF16),
                pltpu.VMEM((16, 256), BF16),
                pltpu.VMEM((256, 256), BF16),
                pltpu.VMEM((2, 32, 256), BF16),
                pltpu.VMEM((32, NBF), BF16),
                pltpu.VMEM((32, NBF), BF16),
                pltpu.VMEM((512, 512), BF16),
                pltpu.VMEM((256, 256), BF16),
                pltpu.VMEM((STEPS, DEVS, 8, NBF), F32),
                pltpu.SemaphoreType.DMA,
                pltpu.SemaphoreType.DMA((2,)),
                pltpu.SemaphoreType.DMA((GIVEN,)),
                pltpu.SemaphoreType.DMA((GIVEN,)),
            ],
            compiler_params=pltpu.CompilerParams(
                collective_id=0, has_side_effects=True, vmem_limit_bytes=48 * 1024 * 1024),
        )(ao_blk, pltpu.with_memory_space_constraint(c_occ.T, pltpu.HBM),
          pltpu.with_memory_space_constraint(c_virt.T, pltpu.HBM))
        out = pl.pallas_call(
            finish,
            out_shape=jax.ShapeDtypeStruct((OCC, HALF, VIRT), F32),
            in_specs=[vmem] * 3,
            out_specs=vmem,
            compiler_params=pltpu.CompilerParams(vmem_limit_bytes=8 * 1024 * 1024),
        )(recv, base, cvd)
        return jnp.swapaxes(out, 1, 2)

    return jax.shard_map(
        local_block, mesh=mesh,
        in_specs=(P(("frag", "dev"), "dev2", None, None), P("frag", None), P("frag", None)),
        out_specs=P("frag", None, ("dev2", "dev")),
        check_vma=False)
```

```python
import functools

import jax
import jax.numpy as jnp
from jax import lax
from jax.experimental import pallas as pl
from jax.experimental.pallas import tpu as pltpu
from jax.sharding import PartitionSpec as P

MESH = pl.DeviceIdType.MESH
F32 = jnp.float32
BF16 = jnp.bfloat16

ROWS_P = 32
ROWS_Q = 64
NBF = 128
OCC = 4
VIRT = 112
HALF = VIRT // 2
TILE_Q = 4
STEPS = ROWS_Q // TILE_Q
SLOTS = 6
GIVEN = 2
TURNS = (5, 11)
DEVS = 8
COLS = 4
PIECES = ((14, 0, 16), (14, 16, 16), (15, 0, 8), (15, 8, 8), (15, 16, 8), (15, 24, 8))
LAST = STEPS - 1
LOOPED = STEPS - 2


def iota(shape, dim):
    return lax.broadcasted_iota(jnp.int32, shape, dim)


def one_hot(cond):
    return jnp.where(cond, 1.0, 0.0).astype(BF16)


def dot(a, b):
    return jnp.dot(a, b, preferred_element_type=F32)


def dot_nt(a, b):
    return lax.dot_general(a, b, (((1,), (1,)), ((), ())), preferred_element_type=F32)


def dot_tn(a, b):
    return lax.dot_general(a, b, (((0,), (0,)), ((), ())), preferred_element_type=F32)


def split(x):
    high = x.astype(BF16)
    rest = x - high.astype(F32)
    mid = rest.astype(BF16)
    return high, mid, (rest - mid.astype(F32)).astype(BF16)


def kernel(*refs):
    pl.run_scoped(
        functools.partial(body, *refs),
        pltpu.SemaphoreType.DMA((SLOTS,)),
        pltpu.SemaphoreType.DMA((len(PIECES),)),
        pltpu.SemaphoreType.DMA((2,)),
    )


def body(a_hbm, co_hbm, cv_hbm, recv, base, cvd, abuf, co_ref, cv_ref, lhs1, cv2, w2, w2a, w2b, w2x, cvx, t1, t1x, sendbuf,
         send_sem, recv_sem, give_sem, take_sem, a_sem, l_sem, c_sem):
    row, col = lax.axis_index("dev2"), lax.axis_index("dev")
    me = row * COLS + col

    def slot_of(tile):
        return lax.rem(tile - GIVEN, SLOTS)

    def fetch(tile, slot):
        return pltpu.make_async_copy(a_hbm.at[:, pl.ds(tile * TILE_Q, TILE_Q)], abuf.at[slot], a_sem.at[slot])

    def fetch_piece(n):
        tile, first, count = PIECES[n]
        part = pl.ds(first, count)
        return pltpu.make_async_copy(
            a_hbm.at[part, pl.ds(tile * TILE_Q, TILE_Q)], abuf.at[(tile - GIVEN) % SLOTS, part], l_sem.at[n])

    co_copy = pltpu.make_async_copy(co_hbm, co_ref, c_sem.at[0])
    cv_copy = pltpu.make_async_copy(cv_hbm, cv_ref, c_sem.at[1])
    co_copy.start()
    cv_copy.start()
    for s in range(SLOTS):
        fetch(GIVEN + s, s).start(priority=1)

    x, core = col // 2, lax.rem(col, 2)
    far_row, far_x = 1 - row, 1 - x
    peers = [(far_row, 2 * far_x), (far_row, 2 * far_x + 1), (far_row, 2 * x), (far_row, 2 * x + 1),
             (row, 2 * far_x), (row, 2 * far_x + 1), (row, 2 * x + 1 - core)]

    barrier = pltpu.get_barrier_semaphore()
    for r, c in peers:
        pl.semaphore_signal(barrier, inc=1, device_id={"dev2": r, "dev": c}, device_id_type=MESH)
    pl.semaphore_wait(barrier, DEVS - 1)

    other = 2 * x + 1 - core
    given = [(0, ROWS_P, k) for k in range(GIVEN)] + [(16, 16, LOOPED)]
    gifts = []
    for k, (first, count, tile) in enumerate(given):
        gifts.append(pltpu.make_async_remote_copy(
            src_ref=a_hbm.at[pl.ds(first, count), pl.ds(tile * TILE_Q, TILE_Q)],
            dst_ref=abuf.at[SLOTS + k, pl.ds(first, count)],
            send_sem=give_sem.at[k], recv_sem=take_sem.at[k],
            device_id={"dev2": row, "dev": other}, device_id_type=MESH))
    for k in range(GIVEN):
        gifts[k].start()

    @pl.when(core == 0)
    def _():
        gifts[GIVEN].start()

    co_copy.wait()
    cv_copy.wait()
    co, cv = co_ref[...], cv_ref[...]

    co_t = dot(one_hot(iota((16, OCC), 0) % OCC == iota((16, OCC), 1)), co)
    r16 = iota((16, NBF), 0)
    lhs1[...] = jnp.concatenate(
        [jnp.where(r16 // OCC == k, co_t, 0.0) for k in range(2)], axis=1).astype(BF16)

    co_i = dot(one_hot(iota((32, OCC), 0) % OCC == iota((32, OCC), 1)), co).astype(BF16)

    def spread(dev, groups):
        width = sum(2 * count * OCC for _, count in groups)
        r, c = iota((NBF, width), 0), iota((NBF, width), 1)
        c32, r32 = iota((32, width), 1), iota((32, width), 0)
        pick, qp, at = r < 0, c32 < 0, 0
        for first, count in groups:
            half = count * OCC
            pick |= (r == dev * ROWS_P + first + (c - at) % half // OCC) & (c >= at) & (c < at + 2 * half)
            qp |= (r32 // OCC % 2 == (c32 - at) // half) & (c32 >= at) & (c32 < at + 2 * half)
            at += 2 * half
        placed = dot(co_i, one_hot(pick))
        return jnp.where(qp & (r32 // 8 == c32 % OCC), placed, 0.0).astype(BF16)

    w2[0] = spread(col, [(0, ROWS_P)])
    w2[1] = spread(other, [(0, ROWS_P)])
    w2a[...] = spread(col, [(0, 16)])
    w2b[...] = spread(col, [(16, 8), (24, 8)])
    w2x[...] = spread(other, [(16, 16)])

    b, c = iota((VIRT, 256), 0), iota((VIRT, 256), 1)
    halves = dot_tn(cv, one_hot((b == (c // NBF) * HALF + c % 64) & (c % 64 < HALF)))
    c = iota((NBF, 256), 1)
    for par in range(2):
        cv2[par * NBF:(par + 1) * NBF, :] = jnp.where((c // 64) % 2 == par, halves, 0.0).astype(BF16)

    wide = jnp.concatenate([cv, jnp.zeros((NBF - VIRT, NBF), BF16)], axis=0)
    r, q = iota((512, NBF), 0), iota((512, NBF), 1)
    rows = dot_nt(one_hot(q == ((r % 256) // OCC) * 2 + r // 256), wide)
    for i in range(OCC):
        cvx[:, i * NBF:(i + 1) * NBF] = jnp.where(r % OCC == i, rows, 0.0).astype(BF16)
    r, q = iota((256, NBF), 0), iota((256, NBF), 1)
    at = (r // 8) % 2 * ROWS_Q + LAST * TILE_Q + (r % 8) // OCC * 2 + r // NBF
    rows = dot_nt(one_hot((q == at) & (r % NBF < 48)), wide)
    for i in range(OCC):
        cvd[:, i * NBF:(i + 1) * NBF] = jnp.where(r % OCC == i, rows, 0.0).astype(BF16)

    def contract_r(slot, blocks, ref=t1):
        left = lhs1[...]
        for qp, pb, at in blocks:
            parts = []
            for p0 in (pb, pb + 2):
                rhs = jnp.concatenate(
                    [abuf[slot, p0:p0 + 2, 2 * qp + par].reshape(256, NBF) for par in range(2)], axis=1)
                parts.append(dot(left, rhs)[:8])
            ref[at:at + 16, :] = jnp.concatenate(parts, axis=0).astype(BF16)

    def contract_s(t_one):
        rows = t_one.shape[0]
        if rows < NBF:
            return dot(t_one, cv2[...]).astype(BF16)
        parts = [dot(t_one[k:k + rows // 2], cv2[...]).astype(BF16) for k in (0, rows // 2)]
        return jnp.concatenate(parts, axis=0)

    def pack(step, e_part):
        for j in range(OCC):
            for h in range(2):
                sendbuf[step, 2 * j + h] = e_part[8 * j:8 * j + 8, h * NBF:(h + 1) * NBF]

    def send(step, sem):
        for r, c in peers:
            pltpu.make_async_remote_copy(
                src_ref=sendbuf.at[step, r * COLS + c], dst_ref=recv.at[step, me],
                send_sem=send_sem, recv_sem=recv_sem.at[sem],
                device_id={"dev2": r, "dev": c}, device_id_type=MESH).start()
        recv[step, me] = sendbuf[step, me]

    def blocks(first, count, at):
        return [(qp, first + pb, at + qp * count * OCC + pb * OCC) for qp in range(2) for pb in range(0, count, 4)]

    whole = blocks(0, ROWS_P, 0)
    upper = [b for b in whole if b[1] < 16]
    lower = [b for b in whole if b[1] >= 16]

    def refill(tile):
        @pl.when(tile + SLOTS < LOOPED)
        def _():
            fetch(tile + SLOTS, slot_of(tile)).start(priority=1)

        for step in range(LOOPED, STEPS):
            @pl.when(tile + SLOTS == step)
            def _():
                for n in range(len(PIECES)):
                    if PIECES[n][0] == step and n != 1:
                        fetch_piece(n).start(priority=1)

        @pl.when((tile + SLOTS == LOOPED) & (core == 1))
        def _():
            fetch_piece(1).start(priority=1)

    def beside(slot, mine, before, weights, more=False):
        half = contract_s(t1[...])
        if more:
            extra = contract_s(t1x[...])
        contract_r(slot, mine[:4])
        e_part = dot(weights, half)
        if more:
            e_part += dot(w2x[...], extra)
        contract_r(slot, mine[4:])
        pack(before, e_part)
        send(before, 0)

    def taken(n):
        return sum(jnp.where(n > turn, 1, 0) for turn in TURNS)

    def own(n):
        return GIVEN + n - taken(n)

    def step_body(n, carry):
        theirs = (n == TURNS[0]) | (n == TURNS[1])
        before_theirs = (n == TURNS[0] + 1) | (n == TURNS[1] + 1)
        slot = jnp.where(theirs, SLOTS + taken(n), slot_of(own(n)))
        before = jnp.where(before_theirs, taken(n) - 1, own(n) - 1)

        for k in range(GIVEN):
            @pl.when(n == TURNS[k])
            def _():
                gifts[k].wait_recv()

        @pl.when(jnp.logical_not(theirs))
        def _():
            fetch(own(n), slot_of(own(n))).wait()

        beside(slot, whole, before, w2[jnp.where(before_theirs, 1, 0)])

        @pl.when(jnp.logical_not(theirs))
        def _():
            refill(own(n))

        return carry

    fetch(GIVEN, 0).wait()
    contract_r(0, whole)
    refill(GIVEN)
    lax.fori_loop(1, LOOPED, step_body, 0)

    slot = (LOOPED - GIVEN) % SLOTS
    fetch_piece(0).wait()
    beside(slot, upper, LOOPED - 1, w2[0])
    first = [b for b in blocks(0, 16, 0) if b[1] < 8]
    last_slot = (LAST - GIVEN) % SLOTS

    @pl.when(core == 0)
    def _():
        for qp in range(2):
            t1[qp * 128 + 64:(qp + 1) * 128, :] = jnp.zeros((64, 256), BF16)
        fetch_piece(2).wait()
        beside(last_slot, first, LOOPED, w2[0])

    @pl.when(core == 1)
    def _():
        fetch_piece(1).wait()
        contract_r(slot, lower)
        gifts[GIVEN].wait_recv()
        contract_r(SLOTS + GIVEN, blocks(16, 16, 0), t1x)
        fetch_piece(2).wait()
        beside(last_slot, first, LOOPED, w2[0], more=True)

    slot = last_slot
    fetch_piece(3).wait()
    contract_r(slot, [b for b in blocks(0, 16, 0) if b[1] >= 8])
    fetch_piece(4).wait()
    half = contract_s(t1[:128, :])
    contract_r(slot, blocks(16, 8, 128))
    e_part = dot(w2a[...], half)
    fetch_piece(5).wait()
    contract_r(slot, blocks(24, 8, 192))
    half = jnp.concatenate([contract_s(t1[128:192, :]), contract_s(t1[192:, :])], axis=0)
    e_part += dot(w2b[...], half)
    pack(LAST, e_part)
    send(LAST, 1)

    def arrived(view, sem):
        pltpu.make_async_copy(view, view, recv_sem.at[sem]).wait()

    arrived(recv.at[pl.ds(0, LAST), pl.ds(0, DEVS - 1)], 0)
    sums = []
    for r in range(2):
        part = recv[:LAST, COLS * r] + recv[:LAST, COLS * r + 1]
        part += recv[:LAST, COLS * r + 2] + recv[:LAST, COLS * r + 3]
        part = jnp.concatenate([part.reshape(LAST * 8, NBF), jnp.zeros((8, NBF), F32)], axis=0)
        sums.append(part.T)
    half = jnp.concatenate(sums, axis=1)
    high, mid, low = split(jnp.concatenate([half[:64], half[64:]], axis=1))
    right = cvx[...]
    base[...] = dot(high, right) + dot(mid, right) + dot(low, right)

    arrived(recv.at[LAST, pl.ds(0, DEVS - 1)], 1)
    sent = sendbuf.at[:, pl.ds(0, DEVS - 1)]
    pltpu.make_async_copy(sent, sent, send_sem).wait()
    for k in range(GIVEN):
        gifts[k].wait_send()

    @pl.when(core == 0)
    def _():
        gifts[GIVEN].wait_send()


def finish(recv, base, cvd, out_ref):
    sums = []
    for r in range(2):
        part = recv[STEPS - 1, COLS * r] + recv[STEPS - 1, COLS * r + 1]
        sums.append(part + (recv[STEPS - 1, COLS * r + 2] + recv[STEPS - 1, COLS * r + 3]))
    parts = [x.astype(F32) for x in split(jnp.concatenate(sums, axis=0))]
    turned = jnp.concatenate(parts + [jnp.zeros((NBF - 48, NBF), F32)], axis=0).T.astype(BF16)
    total = base[...] + dot(jnp.concatenate([turned[:64], turned[64:]], axis=1), cvd[...])
    for i in range(OCC):
        out_ref[i] = total[:HALF, i * NBF:i * NBF + VIRT]


def solution(mesh):
    def local_block(ao_blk, c_occ, c_virt):
        hbm = pl.BlockSpec(memory_space=pltpu.HBM)
        vmem = pl.BlockSpec(memory_space=pltpu.VMEM)
        recv, base, cvd = pl.pallas_call(
            kernel,
            out_shape=[
                jax.ShapeDtypeStruct((STEPS, DEVS, 8, NBF), F32),
                jax.ShapeDtypeStruct((64, 512), F32),
                jax.ShapeDtypeStruct((256, 512), BF16),
            ],
            in_specs=[hbm] * 3,
            out_specs=[vmem] * 3,
            scratch_shapes=[
                pltpu.VMEM((SLOTS + GIVEN + 1, ROWS_P, TILE_Q, NBF, NBF), BF16),
                pltpu.VMEM((OCC, NBF), BF16),
                pltpu.VMEM((VIRT, NBF), BF16),
                pltpu.VMEM((16, 256), BF16),
                pltpu.VMEM((256, 256), BF16),
                pltpu.VMEM((2, 32, 256), BF16),
                pltpu.VMEM((32, NBF), BF16),
                pltpu.VMEM((32, NBF), BF16),
                pltpu.VMEM((32, NBF), BF16),
                pltpu.VMEM((512, 512), BF16),
                pltpu.VMEM((256, 256), BF16),
                pltpu.VMEM((NBF, 256), BF16),
                pltpu.VMEM((STEPS, DEVS, 8, NBF), F32),
                pltpu.SemaphoreType.DMA,
                pltpu.SemaphoreType.DMA((2,)),
                pltpu.SemaphoreType.DMA((GIVEN + 1,)),
                pltpu.SemaphoreType.DMA((GIVEN + 1,)),
            ],
            compiler_params=pltpu.CompilerParams(
                collective_id=0, has_side_effects=True, vmem_limit_bytes=48 * 1024 * 1024),
        )(ao_blk, pltpu.with_memory_space_constraint(c_occ.T, pltpu.HBM),
          pltpu.with_memory_space_constraint(c_virt.T, pltpu.HBM))
        out = pl.pallas_call(
            finish,
            out_shape=jax.ShapeDtypeStruct((OCC, HALF, VIRT), F32),
            in_specs=[vmem] * 3,
            out_specs=vmem,
            compiler_params=pltpu.CompilerParams(vmem_limit_bytes=8 * 1024 * 1024),
        )(recv, base, cvd)
        return jnp.swapaxes(out, 1, 2)

    return jax.shard_map(
        local_block, mesh=mesh,
        in_specs=(P(("frag", "dev"), "dev2", None, None), P("frag", None), P("frag", None)),
        out_specs=P("frag", None, ("dev2", "dev")),
        check_vma=False)
```

```python
import functools

import jax
import jax.numpy as jnp
from jax import lax
from jax.experimental import pallas as pl
from jax.experimental.pallas import tpu as pltpu
from jax.sharding import PartitionSpec as P

MESH = pl.DeviceIdType.MESH
F32 = jnp.float32
BF16 = jnp.bfloat16

ROWS_P = 32
ROWS_Q = 64
NBF = 128
OCC = 4
VIRT = 112
HALF = VIRT // 2
TILE_Q = 4
STEPS = ROWS_Q // TILE_Q
SLOTS = 5
OWN = 24
GIFT = ROWS_P - OWN
DEVS = 8
COLS = 4
PIECES = ((13, 0, 16), (13, 16, 16), (14, 0, 8), (14, 8, 8), (14, 16, 16), (15, 0, 8), (15, 8, 8), (15, 16, 8), (15, 24, 8))
SHARED = 14
LAST = STEPS - 1
LOOPED = STEPS - 3
GIVEN = 8


def iota(shape, dim):
    return lax.broadcasted_iota(jnp.int32, shape, dim)


def one_hot(cond):
    return jnp.where(cond, 1.0, 0.0).astype(BF16)


def dot(a, b):
    return jnp.dot(a, b, preferred_element_type=F32)


def dot_nt(a, b):
    return lax.dot_general(a, b, (((1,), (1,)), ((), ())), preferred_element_type=F32)


def dot_tn(a, b):
    return lax.dot_general(a, b, (((0,), (0,)), ((), ())), preferred_element_type=F32)


def split(x):
    high = x.astype(BF16)
    rest = x - high.astype(F32)
    mid = rest.astype(BF16)
    return high, mid, (rest - mid.astype(F32)).astype(BF16)


def kernel(*refs):
    pl.run_scoped(
        functools.partial(body, *refs),
        pltpu.SemaphoreType.DMA((SLOTS,)),
        pltpu.SemaphoreType.DMA((LOOPED,)),
        pltpu.SemaphoreType.DMA((len(PIECES),)),
        pltpu.SemaphoreType.DMA((2,)),
        pltpu.SemaphoreType.DMA,
        pltpu.SemaphoreType.DMA((2,)),
        pltpu.SemaphoreType.DMA((2,)),
        pltpu.SemaphoreType.DMA((GIVEN + 1,)),
    )


def body(a_hbm, co_hbm, cv_hbm, recv, base, cvd, abuf, land, ends, xbuf, co_ref, cv_ref, lhs1, cv2, w2, w2a, w2b, w2x, cvx, t1, t1x, sendbuf,
         a_sem, land_sem, l_sem, c_sem, send_sem, recv_sem, give_sem, take_sem):
    row, col = lax.axis_index("dev2"), lax.axis_index("dev")
    me = row * COLS + col

    def fetch(tile):
        slot = lax.rem(tile, SLOTS)
        return pltpu.make_async_copy(
            a_hbm.at[pl.ds(0, OWN), pl.ds(tile * TILE_Q, TILE_Q)], abuf.at[slot], a_sem.at[slot])

    def fetch_rest(tile):
        return pltpu.make_async_copy(
            a_hbm.at[pl.ds(OWN, GIFT), pl.ds(tile * TILE_Q, TILE_Q)], land.at[tile], land_sem.at[tile])

    def fetch_piece(n):
        tile, first, count = PIECES[n]
        part = pl.ds(first, count)
        return pltpu.make_async_copy(
            a_hbm.at[part, pl.ds(tile * TILE_Q, TILE_Q)], ends.at[tile - LOOPED, part], l_sem.at[n])

    co_copy = pltpu.make_async_copy(co_hbm, co_ref, c_sem.at[0])
    cv_copy = pltpu.make_async_copy(cv_hbm, cv_ref, c_sem.at[1])
    co_copy.start()
    cv_copy.start()
    for tile in range(SLOTS):
        fetch(tile).start(priority=1)
        if tile % 3 == 0:
            fetch_rest(tile).start(priority=1)

    x, core = col // 2, lax.rem(col, 2)
    far_row, far_x = 1 - row, 1 - x
    giver, taker = (row + x == 2) & (core == 0), (row + x == 2) & (core == 1)
    plain = row + x < 2
    peers = [(far_row, 2 * far_x), (far_row, 2 * far_x + 1), (far_row, 2 * x), (far_row, 2 * x + 1),
             (row, 2 * far_x), (row, 2 * far_x + 1), (row, 2 * x + 1 - core)]

    barrier = pltpu.get_barrier_semaphore()
    for r, c in peers:
        pl.semaphore_signal(barrier, inc=1, device_id={"dev2": r, "dev": c}, device_id_type=MESH)
    pl.semaphore_wait(barrier, DEVS - 1)

    other = 2 * x + 1 - core
    gifts = []
    for tile in [t for t in range(LOOPED) if t % 3] + [SHARED]:
        late = tile == SHARED
        gifts.append(pltpu.make_async_remote_copy(
            src_ref=a_hbm.at[pl.ds(16, 16) if late else pl.ds(OWN, GIFT), pl.ds(tile * TILE_Q, TILE_Q)],
            dst_ref=xbuf if late else land.at[tile],
            send_sem=give_sem.at[1 if late else 0], recv_sem=take_sem.at[len(gifts)],
            device_id={"dev2": row, "dev": other}, device_id_type=MESH))
    for k in range(GIVEN):
        gifts[k].start()

    @pl.when(giver)
    def _():
        gifts[GIVEN].start()

    co_copy.wait()
    cv_copy.wait()
    co, cv = co_ref[...], cv_ref[...]

    co_t = dot(one_hot(iota((16, OCC), 0) % OCC == iota((16, OCC), 1)), co)
    r16 = iota((16, NBF), 0)
    lhs1[...] = jnp.concatenate(
        [jnp.where(r16 // OCC == k, co_t, 0.0) for k in range(2)], axis=1).astype(BF16)

    co_i = dot(one_hot(iota((32, OCC), 0) % OCC == iota((32, OCC), 1)), co).astype(BF16)

    def spread(dev, groups):
        width = sum(2 * count * OCC for _, count in groups)
        r, c = iota((NBF, width), 0), iota((NBF, width), 1)
        c32, r32 = iota((32, width), 1), iota((32, width), 0)
        pick, qp, at = r < 0, c32 < 0, 0
        for first, count in groups:
            half = count * OCC
            pick |= (r == dev * ROWS_P + first + (c - at) % half // OCC) & (c >= at) & (c < at + 2 * half)
            qp |= (r32 // OCC % 2 == (c32 - at) // half) & (c32 >= at) & (c32 < at + 2 * half)
            at += 2 * half
        placed = dot(co_i, one_hot(pick))
        return jnp.where(qp & (r32 // 8 == c32 % OCC), placed, 0.0).astype(BF16)

    r, c = iota((NBF, 256), 0), iota((NBF, 256), 1)
    p = c % NBF // OCC
    for k in range(2):
        source = jnp.where((p < OWN) | (k == 0), col, other)
        placed = dot(co_i, one_hot(r == source * ROWS_P + p))
        c32, r32 = iota((32, 256), 1), iota((32, 256), 0)
        keep = (r32 // OCC % 2 == c32 // NBF) & (r32 // 8 == c32 % OCC)
        w2[k] = jnp.where(keep, placed, 0.0).astype(BF16)
    w2a[...] = spread(col, [(0, 16)])
    w2b[...] = spread(col, [(16, 8), (24, 8)])
    w2x[...] = spread(other, [(16, 16)])

    b, c = iota((VIRT, 256), 0), iota((VIRT, 256), 1)
    halves = dot_tn(cv, one_hot((b == (c // NBF) * HALF + c % 64) & (c % 64 < HALF)))
    c = iota((NBF, 256), 1)
    for par in range(2):
        cv2[par * NBF:(par + 1) * NBF, :] = jnp.where((c // 64) % 2 == par, halves, 0.0).astype(BF16)

    wide = jnp.concatenate([cv, jnp.zeros((NBF - VIRT, NBF), BF16)], axis=0)
    r, q = iota((512, NBF), 0), iota((512, NBF), 1)
    rows = dot_nt(one_hot(q == ((r % 256) // OCC) * 2 + r // 256), wide)
    for i in range(OCC):
        cvx[:, i * NBF:(i + 1) * NBF] = jnp.where(r % OCC == i, rows, 0.0).astype(BF16)
    r, q = iota((256, NBF), 0), iota((256, NBF), 1)
    at = (r // 8) % 2 * ROWS_Q + LAST * TILE_Q + (r % 8) // OCC * 2 + r // NBF
    rows = dot_nt(one_hot((q == at) & (r % NBF < 48)), wide)
    for i in range(OCC):
        cvd[:, i * NBF:(i + 1) * NBF] = jnp.where(r % OCC == i, rows, 0.0).astype(BF16)

    def contract_r(rows_of, blocks, ref=t1):
        left = lhs1[...]
        for qp, pb, at in blocks:
            parts = []
            for p0 in (pb, pb + 2):
                rhs = jnp.concatenate([rows_of(p0, 2 * qp + par).reshape(256, NBF) for par in range(2)], axis=1)
                parts.append(dot(left, rhs)[:8])
            ref[at:at + 16, :] = jnp.concatenate(parts, axis=0).astype(BF16)

    def looped(tile, slot):
        return lambda p0, q: abuf[slot, p0:p0 + 2, q] if p0 < OWN else land[tile, p0 - OWN:p0 - OWN + 2, q]

    def ending(tile):
        return lambda p0, q: ends[tile - LOOPED, p0:p0 + 2, q]

    def contract_s(t_one):
        rows = t_one.shape[0]
        if rows < NBF:
            return dot(t_one, cv2[...]).astype(BF16)
        parts = [dot(t_one[k:k + rows // 2], cv2[...]).astype(BF16) for k in (0, rows // 2)]
        return jnp.concatenate(parts, axis=0)

    def pack(step, e_part):
        for j in range(OCC):
            for h in range(2):
                sendbuf[step, 2 * j + h] = e_part[8 * j:8 * j + 8, h * NBF:(h + 1) * NBF]

    def send(step, sem):
        for r, c in peers:
            pltpu.make_async_remote_copy(
                src_ref=sendbuf.at[step, r * COLS + c], dst_ref=recv.at[step, me],
                send_sem=send_sem, recv_sem=recv_sem.at[sem],
                device_id={"dev2": r, "dev": c}, device_id_type=MESH).start()
        recv[step, me] = sendbuf[step, me]

    def blocks(first, count, at):
        return [(qp, first + pb, at + qp * count * OCC + pb * OCC) for qp in range(2) for pb in range(0, count, 4)]

    whole = blocks(0, ROWS_P, 0)
    upper = [b for b in whole if b[1] < 16]
    lower = [b for b in whole if b[1] >= 16]

    def refill(tile):
        new = tile + SLOTS

        @pl.when(new < LOOPED)
        def _():
            fetch(new).start(priority=1)

        @pl.when((new < LOOPED) & (lax.rem(new, 3) == 0))
        def _():
            fetch_rest(new).start(priority=1)

        for step in range(LOOPED, STEPS):
            @pl.when(new == step)
            def _():
                for n in range(len(PIECES)):
                    if PIECES[n][0] == step and PIECES[n] != (SHARED, 16, 16):
                        fetch_piece(n).start(priority=1)

        @pl.when((new == SHARED) & jnp.logical_not(giver))
        def _():
            fetch_piece(4).start(priority=1)

    def beside(rows_of, mine, before, weights, more=False):
        half = contract_s(t1[...])
        if more:
            extra = contract_s(t1x[...])
        contract_r(rows_of, mine[:4])
        e_part = dot(weights, half)
        if more:
            e_part += dot(w2x[...], extra)
        contract_r(rows_of, mine[4:])
        pack(before, e_part)
        send(before, 0)

    def step_body(tile, carry):
        fetch(tile).wait()

        @pl.when(lax.rem(tile, 3) == 0)
        def _():
            fetch_rest(tile).wait()

        @pl.when(lax.rem(tile, 3) != 0)
        def _():
            view = land.at[tile]
            pltpu.make_async_copy(view, view, take_sem.at[tile - tile // 3 - 1]).wait()

        mixed = jnp.where(lax.rem(tile - 1, 3) == 0, 0, 1)
        beside(looped(tile, lax.rem(tile, SLOTS)), whole, tile - 1, w2[mixed])
        refill(tile)
        return carry

    fetch(0).wait()
    fetch_rest(0).wait()
    contract_r(looped(0, 0), whole)
    refill(0)
    lax.fori_loop(1, LOOPED, step_body, 0)

    fetch_piece(0).wait()
    beside(ending(LOOPED), upper, LOOPED - 1, w2[0])
    fetch_piece(1).wait()
    contract_r(ending(LOOPED), lower)
    first = [b for b in blocks(0, 16, 0) if b[1] < 8]
    second = [b for b in blocks(0, 16, 0) if b[1] >= 8]

    @pl.when(giver)
    def _():
        fetch_piece(2).wait()
        beside(ending(SHARED), first, SHARED - 1, w2[0])
        fetch_piece(3).wait()
        contract_r(ending(SHARED), second)
        fetch_piece(5).wait()
        half = contract_s(t1[:128, :])
        contract_r(ending(LAST), first)
        pack(SHARED, dot(w2a[...], half))
        send(SHARED, 0)
        fetch_piece(6).wait()
        contract_r(ending(LAST), second)

    @pl.when(plain)
    def _():
        fetch_piece(2).wait()
        fetch_piece(3).wait()
        beside(ending(SHARED), upper, SHARED - 1, w2[0])
        fetch_piece(4).wait()
        contract_r(ending(SHARED), lower)
        fetch_piece(5).wait()
        fetch_piece(6).wait()
        beside(ending(LAST), first + second, SHARED, w2[0])

    @pl.when(taker)
    def _():
        fetch_piece(2).wait()
        fetch_piece(3).wait()
        beside(ending(SHARED), upper, SHARED - 1, w2[0])
        gifts[GIVEN].wait_recv()
        fetch_piece(4).wait()
        contract_r(ending(SHARED), lower)
        contract_r(lambda p0, q: xbuf[p0 - 16:p0 - 14, q], blocks(16, 16, 0), t1x)
        fetch_piece(5).wait()
        fetch_piece(6).wait()
        beside(ending(LAST), first + second, SHARED, w2[0], more=True)

    fetch_piece(7).wait()
    half = contract_s(t1[:128, :])
    contract_r(ending(LAST), blocks(16, 8, 128))
    e_part = dot(w2a[...], half)
    fetch_piece(8).wait()
    contract_r(ending(LAST), blocks(24, 8, 192))
    half = jnp.concatenate([contract_s(t1[128:192, :]), contract_s(t1[192:, :])], axis=0)
    e_part += dot(w2b[...], half)
    pack(LAST, e_part)
    send(LAST, 1)

    def arrived(view, sem):
        pltpu.make_async_copy(view, view, recv_sem.at[sem]).wait()

    arrived(recv.at[pl.ds(0, LAST), pl.ds(0, DEVS - 1)], 0)
    sums = []
    for r in range(2):
        part = recv[:LAST, COLS * r] + recv[:LAST, COLS * r + 1]
        part += recv[:LAST, COLS * r + 2] + recv[:LAST, COLS * r + 3]
        part = jnp.concatenate([part.reshape(LAST * 8, NBF), jnp.zeros((8, NBF), F32)], axis=0)
        sums.append(part.T)
    half = jnp.concatenate(sums, axis=1)
    high, mid, low = split(jnp.concatenate([half[:64], half[64:]], axis=1))
    right = cvx[...]
    base[...] = dot(high, right) + dot(mid, right) + dot(low, right)

    arrived(recv.at[LAST, pl.ds(0, DEVS - 1)], 1)
    sent = sendbuf.at[:, pl.ds(0, DEVS - 1)]
    pltpu.make_async_copy(sent, sent, send_sem).wait()
    view = land.at[pl.ds(0, GIVEN)]
    pltpu.make_async_copy(view, view, give_sem.at[0]).wait()

    @pl.when(giver)
    def _():
        gifts[GIVEN].wait_send()


def finish(recv, base, cvd, out_ref):
    sums = []
    for r in range(2):
        part = recv[STEPS - 1, COLS * r] + recv[STEPS - 1, COLS * r + 1]
        sums.append(part + (recv[STEPS - 1, COLS * r + 2] + recv[STEPS - 1, COLS * r + 3]))
    parts = [x.astype(F32) for x in split(jnp.concatenate(sums, axis=0))]
    turned = jnp.concatenate(parts + [jnp.zeros((NBF - 48, NBF), F32)], axis=0).T.astype(BF16)
    total = base[...] + dot(jnp.concatenate([turned[:64], turned[64:]], axis=1), cvd[...])
    for i in range(OCC):
        out_ref[i] = total[:HALF, i * NBF:i * NBF + VIRT]


def solution(mesh):
    def local_block(ao_blk, c_occ, c_virt):
        hbm = pl.BlockSpec(memory_space=pltpu.HBM)
        vmem = pl.BlockSpec(memory_space=pltpu.VMEM)
        recv, base, cvd = pl.pallas_call(
            kernel,
            out_shape=[
                jax.ShapeDtypeStruct((STEPS, DEVS, 8, NBF), F32),
                jax.ShapeDtypeStruct((64, 512), F32),
                jax.ShapeDtypeStruct((256, 512), BF16),
            ],
            in_specs=[hbm] * 3,
            out_specs=[vmem] * 3,
            scratch_shapes=[
                pltpu.VMEM((SLOTS, OWN, TILE_Q, NBF, NBF), BF16),
                pltpu.VMEM((LOOPED, GIFT, TILE_Q, NBF, NBF), BF16),
                pltpu.VMEM((STEPS - LOOPED, ROWS_P, TILE_Q, NBF, NBF), BF16),
                pltpu.VMEM((16, TILE_Q, NBF, NBF), BF16),
                pltpu.VMEM((OCC, NBF), BF16),
                pltpu.VMEM((VIRT, NBF), BF16),
                pltpu.VMEM((16, 256), BF16),
                pltpu.VMEM((256, 256), BF16),
                pltpu.VMEM((2, 32, 256), BF16),
                pltpu.VMEM((32, NBF), BF16),
                pltpu.VMEM((32, NBF), BF16),
                pltpu.VMEM((32, NBF), BF16),
                pltpu.VMEM((512, 512), BF16),
                pltpu.VMEM((256, 256), BF16),
                pltpu.VMEM((NBF, 256), BF16),
                pltpu.VMEM((STEPS, DEVS, 8, NBF), F32),
            ],
            compiler_params=pltpu.CompilerParams(
                collective_id=0, has_side_effects=True, vmem_limit_bytes=48 * 1024 * 1024),
        )(ao_blk, pltpu.with_memory_space_constraint(c_occ.T, pltpu.HBM),
          pltpu.with_memory_space_constraint(c_virt.T, pltpu.HBM))
        out = pl.pallas_call(
            finish,
            out_shape=jax.ShapeDtypeStruct((OCC, HALF, VIRT), F32),
            in_specs=[vmem] * 3,
            out_specs=vmem,
            compiler_params=pltpu.CompilerParams(vmem_limit_bytes=8 * 1024 * 1024),
        )(recv, base, cvd)
        return jnp.swapaxes(out, 1, 2)

    return jax.shard_map(
        local_block, mesh=mesh,
        in_specs=(P(("frag", "dev"), "dev2", None, None), P("frag", None), P("frag", None)),
        out_specs=P("frag", None, ("dev2", "dev")),
        check_vma=False)
```

```python
import functools

import jax
import jax.numpy as jnp
from jax import lax
from jax.experimental import pallas as pl
from jax.experimental.pallas import tpu as pltpu
from jax.sharding import PartitionSpec as P

MESH = pl.DeviceIdType.MESH
F32 = jnp.float32
BF16 = jnp.bfloat16

ROWS_P = 32
ROWS_Q = 64
NBF = 128
OCC = 4
VIRT = 112
HALF = VIRT // 2
TILE_Q = 4
STEPS = ROWS_Q // TILE_Q
SLOTS = 5
OWN = 24
GIFT = ROWS_P - OWN
DEVS = 8
COLS = 4
PIECES = ((13, 0, 16), (13, 16, 8), (13, 24, 8), (14, 0, 16), (14, 16, 16), (15, 0, 8), (15, 8, 8), (15, 16, 8), (15, 24, 8))
SIDE = 13
LAST = STEPS - 1
LOOPED = STEPS - 3
GIFTED = (2, 3, 5, 6, 8, 9, 11, 12)
GIVEN = len(GIFTED)


def iota(shape, dim):
    return lax.broadcasted_iota(jnp.int32, shape, dim)


def one_hot(cond):
    return jnp.where(cond, 1.0, 0.0).astype(BF16)


def dot(a, b):
    return jnp.dot(a, b, preferred_element_type=F32)


def dot_nt(a, b):
    return lax.dot_general(a, b, (((1,), (1,)), ((), ())), preferred_element_type=F32)


def dot_tn(a, b):
    return lax.dot_general(a, b, (((0,), (0,)), ((), ())), preferred_element_type=F32)


def split(x):
    high = x.astype(BF16)
    rest = x - high.astype(F32)
    mid = rest.astype(BF16)
    return high, mid, (rest - mid.astype(F32)).astype(BF16)


def kernel(*refs):
    pl.run_scoped(
        functools.partial(body, *refs),
        pltpu.SemaphoreType.DMA((SLOTS,)),
        pltpu.SemaphoreType.DMA((LOOPED,)),
        pltpu.SemaphoreType.DMA((len(PIECES),)),
        pltpu.SemaphoreType.DMA((2,)),
        pltpu.SemaphoreType.DMA,
        pltpu.SemaphoreType.DMA((3,)),
        pltpu.SemaphoreType.DMA((6,)),
        pltpu.SemaphoreType.DMA((GIVEN + 4,)),
    )


def body(a_hbm, co_hbm, cv_hbm, recv, base, cvd, abuf, land, ends, xbuf, co_ref, cv_ref, lhs1, cv2, w2, w2a, w2b, w2x, w2h, w2g, cvx, t1, t1x, t1h, hbuf, sendx, recvx, sendbuf,
         a_sem, land_sem, l_sem, c_sem, send_sem, recv_sem, give_sem, take_sem):
    row, col = lax.axis_index("dev2"), lax.axis_index("dev")
    me = row * COLS + col

    def fetch(tile):
        slot = lax.rem(tile, SLOTS)
        return pltpu.make_async_copy(
            a_hbm.at[pl.ds(0, OWN), pl.ds(tile * TILE_Q, TILE_Q)], abuf.at[slot], a_sem.at[slot])

    def fetch_rest(tile):
        return pltpu.make_async_copy(
            a_hbm.at[pl.ds(OWN, GIFT), pl.ds(tile * TILE_Q, TILE_Q)], land.at[tile], land_sem.at[tile])

    def fetch_piece(n):
        tile, first, count = PIECES[n]
        part = pl.ds(first, count)
        return pltpu.make_async_copy(
            a_hbm.at[part, pl.ds(tile * TILE_Q, TILE_Q)], ends.at[tile - LOOPED, part], l_sem.at[n])

    co_copy = pltpu.make_async_copy(co_hbm, co_ref, c_sem.at[0])
    cv_copy = pltpu.make_async_copy(cv_hbm, cv_ref, c_sem.at[1])
    co_copy.start()
    cv_copy.start()
    for tile in range(SLOTS):
        fetch(tile).start(priority=1)
        if tile not in GIFTED:
            fetch_rest(tile).start(priority=1)

    x, core = col // 2, lax.rem(col, 2)
    far_row, far_x = 1 - row, 1 - x
    giver, taker = (row + x == 2) & (core == 0), (row + x == 2) & (core == 1)
    last_chip = row + x == 2
    helper = ((row == 1) & (col == 1)) | ((row == 0) & (col == 3))
    plain = (row + x < 2) & jnp.logical_not(helper)
    peers = [(far_row, 2 * far_x), (far_row, 2 * far_x + 1), (far_row, 2 * x), (far_row, 2 * x + 1),
             (row, 2 * far_x), (row, 2 * far_x + 1), (row, 2 * x + 1 - core)]

    barrier = pltpu.get_barrier_semaphore()
    for r, c in peers:
        pl.semaphore_signal(barrier, inc=1, device_id={"dev2": r, "dev": c}, device_id_type=MESH)
    pl.semaphore_wait(barrier, DEVS - 1)

    other = 2 * x + 1 - core
    gifts = []
    for tile in GIFTED:
        gifts.append(pltpu.make_async_remote_copy(
            src_ref=a_hbm.at[pl.ds(OWN, GIFT), pl.ds(tile * TILE_Q, TILE_Q)], dst_ref=land.at[tile],
            send_sem=give_sem.at[0], recv_sem=take_sem.at[len(gifts)],
            device_id={"dev2": row, "dev": other}, device_id_type=MESH))
    for k in range(2):
        gifts.append(pltpu.make_async_remote_copy(
            src_ref=a_hbm.at[pl.ds(16 + 8 * k, 8), pl.ds(LAST * TILE_Q, TILE_Q)], dst_ref=xbuf.at[pl.ds(8 * k, 8)],
            send_sem=give_sem.at[1 + k], recv_sem=take_sem.at[GIVEN + k],
            device_id={"dev2": row, "dev": other}, device_id_type=MESH))
    for k in range(GIVEN):
        gifts[k].start()

    @pl.when(giver)
    def _():
        gifts[GIVEN].start()
        gifts[GIVEN + 1].start()

    sides = [
        pltpu.make_async_remote_copy(
            src_ref=a_hbm.at[pl.ds(first, 4), pl.ds(SIDE * TILE_Q, TILE_Q)], dst_ref=hbuf.at[pl.ds(core * 4, 4)],
            send_sem=give_sem.at[3 + n], recv_sem=take_sem.at[GIVEN + 2 + core],
            device_id={"dev2": r, "dev": c}, device_id_type=MESH)
        for n, (first, r, c) in enumerate([(28, 1, 1), (24, 0, 3)])]

    @pl.when(last_chip)
    def _():
        for side in sides:
            side.start()

    co_copy.wait()
    cv_copy.wait()
    co, cv = co_ref[...], cv_ref[...]

    co_t = dot(one_hot(iota((16, OCC), 0) % OCC == iota((16, OCC), 1)), co)
    r16 = iota((16, NBF), 0)
    lhs1[...] = jnp.concatenate(
        [jnp.where(r16 // OCC == k, co_t, 0.0) for k in range(2)], axis=1).astype(BF16)

    co_i = dot(one_hot(iota((32, OCC), 0) % OCC == iota((32, OCC), 1)), co).astype(BF16)

    def spread(groups):
        width = sum(2 * count * OCC for _, _, count in groups)
        r, c = iota((NBF, width), 0), iota((NBF, width), 1)
        c32, r32 = iota((32, width), 1), iota((32, width), 0)
        pick, qp, at = r < 0, c32 < 0, 0
        for dev, first, count in groups:
            half = count * OCC
            pick |= (r == dev * ROWS_P + first + (c - at) % half // OCC) & (c >= at) & (c < at + 2 * half)
            qp |= (r32 // OCC % 2 == (c32 - at) // half) & (c32 >= at) & (c32 < at + 2 * half)
            at += 2 * half
        placed = dot(co_i, one_hot(pick))
        return jnp.where(qp & (r32 // 8 == c32 % OCC), placed, 0.0).astype(BF16)

    r, c = iota((NBF, 256), 0), iota((NBF, 256), 1)
    p = c % NBF // OCC
    for k in range(2):
        source = jnp.where((p < OWN) | (k == 0), col, other)
        placed = dot(co_i, one_hot(r == source * ROWS_P + p))
        c32, r32 = iota((32, 256), 1), iota((32, 256), 0)
        keep = (r32 // OCC % 2 == c32 // NBF) & (r32 // 8 == c32 % OCC)
        w2[k] = jnp.where(keep, placed, 0.0).astype(BF16)
    w2a[...] = spread([(col, 0, 16)])
    w2b[...] = spread([(col, 16, 8), (col, 24, 8)])
    w2x[...] = spread([(other, 16, 8), (other, 24, 8)])
    w2g[...] = spread([(col, 0, 8), (col, 8, 8)])
    w2h[...] = spread([(2, 24 + 4 * row, 4), (3, 24 + 4 * row, 4)])

    b, c = iota((VIRT, 256), 0), iota((VIRT, 256), 1)
    halves = dot_tn(cv, one_hot((b == (c // NBF) * HALF + c % 64) & (c % 64 < HALF)))
    c = iota((NBF, 256), 1)
    for par in range(2):
        cv2[par * NBF:(par + 1) * NBF, :] = jnp.where((c // 64) % 2 == par, halves, 0.0).astype(BF16)

    wide = jnp.concatenate([cv, jnp.zeros((NBF - VIRT, NBF), BF16)], axis=0)
    r, q = iota((512, NBF), 0), iota((512, NBF), 1)
    rows = dot_nt(one_hot(q == ((r % 256) // OCC) * 2 + r // 256), wide)
    for i in range(OCC):
        cvx[:, i * NBF:(i + 1) * NBF] = jnp.where(r % OCC == i, rows, 0.0).astype(BF16)
    r, q = iota((256, NBF), 0), iota((256, NBF), 1)
    at = (r // 8) % 2 * ROWS_Q + LAST * TILE_Q + (r % 8) // OCC * 2 + r // NBF
    rows = dot_nt(one_hot((q == at) & (r % NBF < 48)), wide)
    for i in range(OCC):
        cvd[:, i * NBF:(i + 1) * NBF] = jnp.where(r % OCC == i, rows, 0.0).astype(BF16)

    def contract_r(rows_of, blocks, ref=t1):
        left = lhs1[...]
        for qp, pb, at in blocks:
            parts = []
            for p0 in (pb, pb + 2):
                rhs = jnp.concatenate([rows_of(p0, 2 * qp + par).reshape(256, NBF) for par in range(2)], axis=1)
                parts.append(dot(left, rhs)[:8])
            ref[at:at + 16, :] = jnp.concatenate(parts, axis=0).astype(BF16)

    def looped(tile, slot):
        return lambda p0, q: abuf[slot, p0:p0 + 2, q] if p0 < OWN else land[tile, p0 - OWN:p0 - OWN + 2, q]

    def ending(tile):
        return lambda p0, q: ends[tile - LOOPED, p0:p0 + 2, q]

    def contract_s(t_one):
        rows = t_one.shape[0]
        if rows < NBF:
            return dot(t_one, cv2[...]).astype(BF16)
        parts = [dot(t_one[k:k + rows // 2], cv2[...]).astype(BF16) for k in (0, rows // 2)]
        return jnp.concatenate(parts, axis=0)

    def pack(step, e_part):
        for j in range(OCC):
            for h in range(2):
                sendbuf[step, 2 * j + h] = e_part[8 * j:8 * j + 8, h * NBF:(h + 1) * NBF]

    def send(step, sem):
        for r, c in peers:
            pltpu.make_async_remote_copy(
                src_ref=sendbuf.at[step, r * COLS + c], dst_ref=recv.at[step, me],
                send_sem=send_sem, recv_sem=recv_sem.at[sem],
                device_id={"dev2": r, "dev": c}, device_id_type=MESH).start()
        recv[step, me] = sendbuf[step, me]

    def send_last():
        for to in range(DEVS):
            @pl.when(me != to)
            def _():
                pltpu.make_async_remote_copy(
                    src_ref=sendbuf.at[LAST, to], dst_ref=recv.at[LAST, me],
                    send_sem=send_sem, recv_sem=recv_sem.at[1],
                    device_id={"dev2": to // COLS, "dev": to % COLS}, device_id_type=MESH).start()
        recv[LAST, me] = sendbuf[LAST, me]

    def blocks(first, count, at):
        return [(qp, first + pb, at + qp * count * OCC + pb * OCC) for qp in range(2) for pb in range(0, count, 4)]

    whole = blocks(0, ROWS_P, 0)
    upper = [b for b in whole if b[1] < 16]
    lower = [b for b in whole if b[1] >= 16]

    def refill(tile):
        new = tile + SLOTS

        @pl.when(new < LOOPED)
        def _():
            fetch(new).start(priority=1)

        @pl.when((new < LOOPED) & (lax.rem(new, 3) == 1))
        def _():
            fetch_rest(new).start(priority=1)

        for step in range(LOOPED, STEPS):
            @pl.when(new == step)
            def _():
                for n in range(len(PIECES)):
                    if PIECES[n][0] == step and n not in (2, 7, 8):
                        fetch_piece(n).start(priority=1)

        @pl.when((new == SIDE) & jnp.logical_not(last_chip))
        def _():
            fetch_piece(2).start(priority=1)

        @pl.when((new == LAST) & jnp.logical_not(giver))
        def _():
            fetch_piece(7).start(priority=1)
            fetch_piece(8).start(priority=1)

    def beside(rows_of, mine, before, weights):
        half = contract_s(t1[...])
        contract_r(rows_of, mine[:4])
        e_part = dot(weights, half)
        contract_r(rows_of, mine[4:])
        pack(before, e_part)
        send(before, 0)

    def step_body(tile, carry):
        fetch(tile).wait()

        @pl.when(lax.rem(tile, 3) == 1)
        def _():
            fetch_rest(tile).wait()

        @pl.when(lax.rem(tile, 3) != 1)
        def _():
            view = land.at[tile]
            pltpu.make_async_copy(view, view, take_sem.at[tile - (tile + 1) // 3 - 1]).wait()

        mixed = jnp.where((lax.rem(tile, 3) == 2) | (tile == 1), 0, 1)
        beside(looped(tile, lax.rem(tile, SLOTS)), whole, tile - 1, w2[mixed])
        refill(tile)
        return carry

    fetch(0).wait()
    fetch_rest(0).wait()
    contract_r(looped(0, 0), whole)
    refill(0)
    lax.fori_loop(1, LOOPED, step_body, 0)

    fetch_piece(0).wait()
    beside(ending(LOOPED), upper, LOOPED - 1, w2[1])

    first = blocks(0, 16, 0)

    def gift_rows(p0, q):
        return xbuf[p0 - 16:p0 - 14, q]

    def most_of_side():
        contract_r(ending(SIDE), [b for b in lower if b[1] < 24])
        for qp in range(2):
            t1[qp * 128 + 96:(qp + 1) * 128, :] = jnp.zeros((32, 256), BF16)

    def both_halves(before):
        beside(ending(before + 1), upper, before, w2[0])
        fetch_piece(4).wait()
        contract_r(ending(before + 1), lower)

    def start_last():
        fetch_piece(5).wait()
        fetch_piece(6).wait()
        beside(ending(LAST), first, LAST - 1, w2[0])

    def finish_last(parts, weights, e_part=None):
        half = jnp.concatenate([contract_s(t1[k:k + 64, :]) for k in parts], axis=0)
        e_last = dot(weights, half)
        pack(LAST, e_last if e_part is None else e_part + e_last)
        send_last()

    @pl.when(giver)
    def _():
        fetch_piece(1).wait()
        most_of_side()
        fetch_piece(3).wait()
        both_halves(SIDE)
        fetch_piece(5).wait()
        beside(ending(LAST), blocks(0, 8, 0), LAST - 1, w2[0])
        fetch_piece(6).wait()
        contract_r(ending(LAST), blocks(8, 8, 64))
        finish_last((0, 64), w2g[...])

    @pl.when(taker)
    def _():
        fetch_piece(1).wait()
        gifts[GIVEN].wait_recv()
        most_of_side()
        contract_r(gift_rows, blocks(16, 8, 0), t1x)
        fetch_piece(3).wait()
        both_halves(SIDE)
        start_last()
        fetch_piece(7).wait()
        gifts[GIVEN + 1].wait_recv()
        half = contract_s(t1[:128, :])
        contract_r(ending(LAST), blocks(16, 8, 128))
        e_part = dot(w2a[...], half)
        contract_r(gift_rows, blocks(24, 8, 64), t1x)
        fetch_piece(8).wait()
        contract_r(ending(LAST), blocks(24, 8, 192))
        e_part += dot(w2x[...], contract_s(t1x[...]))
        finish_last((128, 192), w2b[...], e_part)

    @pl.when(plain)
    def _():
        fetch_piece(1).wait()
        fetch_piece(2).wait()
        contract_r(ending(SIDE), lower)
        fetch_piece(3).wait()
        both_halves(SIDE)

    @pl.when(helper)
    def _():
        fetch_piece(1).wait()
        fetch_piece(2).wait()
        for k in range(2):
            view = hbuf.at[pl.ds(4 * k, 4)]
            pltpu.make_async_copy(view, view, take_sem.at[GIVEN + 2 + k]).wait()
        contract_r(ending(SIDE), lower)
        contract_r(lambda p0, q: hbuf[p0:p0 + 2, q], [(qp, 4 * k, 32 * k + 16 * qp) for k in range(2) for qp in range(2)], t1h)
        fetch_piece(3).wait()
        half = contract_s(t1[...])
        extra = contract_s(t1h[...])
        contract_r(ending(SIDE + 1), upper[:4])
        e_part = dot(w2[0], half)
        e_side = dot(w2h[...], extra)
        contract_r(ending(SIDE + 1), upper[4:])
        pack(SIDE, e_part + jnp.where(row == 1, e_side, 0.0))
        for j in range(OCC):
            for h in range(2):
                sendx[2 * j + h] = e_side[8 * j:8 * j + 8, h * NBF:(h + 1) * NBF]
        send(SIDE, 0)

        @pl.when(row == 0)
        def _():
            for r, c in peers:
                pltpu.make_async_remote_copy(
                    src_ref=sendx.at[r * COLS + c], dst_ref=recvx, send_sem=give_sem.at[5], recv_sem=recv_sem.at[2],
                    device_id={"dev2": r, "dev": c}, device_id_type=MESH).start()
            recvx[...] = sendx[me]

        fetch_piece(4).wait()
        contract_r(ending(SIDE + 1), lower)

    @pl.when(jnp.logical_not(last_chip))
    def _():
        start_last()
        fetch_piece(7).wait()
        half = contract_s(t1[:128, :])
        contract_r(ending(LAST), blocks(16, 8, 128))
        e_part = dot(w2a[...], half)
        fetch_piece(8).wait()
        contract_r(ending(LAST), blocks(24, 8, 192))
        finish_last((128, 192), w2b[...], e_part)

    def arrived(view, sem):
        pltpu.make_async_copy(view, view, recv_sem.at[sem]).wait()

    arrived(recv.at[pl.ds(0, LAST), pl.ds(0, DEVS - 1)], 0)

    @pl.when(me != 3)
    def _():
        arrived(recvx, 2)

    recv[SIDE, COLS] = recv[SIDE, COLS] + recvx[...]
    sums = []
    for r in range(2):
        part = recv[:LAST, COLS * r] + recv[:LAST, COLS * r + 1]
        part += recv[:LAST, COLS * r + 2] + recv[:LAST, COLS * r + 3]
        part = jnp.concatenate([part.reshape(LAST * 8, NBF), jnp.zeros((8, NBF), F32)], axis=0)
        sums.append(part.T)
    half = jnp.concatenate(sums, axis=1)
    high, mid, low = split(jnp.concatenate([half[:64], half[64:]], axis=1))
    right = cvx[...]
    base[...] = dot(high, right) + dot(mid, right) + dot(low, right)

    arrived(recv.at[LAST, pl.ds(0, DEVS - 1)], 1)
    sent = sendbuf.at[:, pl.ds(0, DEVS - 1)]
    pltpu.make_async_copy(sent, sent, send_sem).wait()
    view = land.at[pl.ds(0, GIVEN)]
    pltpu.make_async_copy(view, view, give_sem.at[0]).wait()

    @pl.when(giver)
    def _():
        gifts[GIVEN].wait_send()
        gifts[GIVEN + 1].wait_send()

    @pl.when(last_chip)
    def _():
        for side in sides:
            side.wait_send()

    @pl.when(me == 3)
    def _():
        view = sendx.at[pl.ds(0, DEVS - 1)]
        pltpu.make_async_copy(view, view, give_sem.at[5]).wait()


def finish(recv, base, cvd, out_ref):
    sums = []
    for r in range(2):
        part = recv[STEPS - 1, COLS * r] + recv[STEPS - 1, COLS * r + 1]
        sums.append(part + (recv[STEPS - 1, COLS * r + 2] + recv[STEPS - 1, COLS * r + 3]))
    parts = [x.astype(F32) for x in split(jnp.concatenate(sums, axis=0))]
    turned = jnp.concatenate(parts + [jnp.zeros((NBF - 48, NBF), F32)], axis=0).T.astype(BF16)
    total = base[...] + dot(jnp.concatenate([turned[:64], turned[64:]], axis=1), cvd[...])
    for i in range(OCC):
        out_ref[i] = total[:HALF, i * NBF:i * NBF + VIRT]


def solution(mesh):
    def local_block(ao_blk, c_occ, c_virt):
        hbm = pl.BlockSpec(memory_space=pltpu.HBM)
        vmem = pl.BlockSpec(memory_space=pltpu.VMEM)
        recv, base, cvd = pl.pallas_call(
            kernel,
            out_shape=[
                jax.ShapeDtypeStruct((STEPS, DEVS, 8, NBF), F32),
                jax.ShapeDtypeStruct((64, 512), F32),
                jax.ShapeDtypeStruct((256, 512), BF16),
            ],
            in_specs=[hbm] * 3,
            out_specs=[vmem] * 3,
            scratch_shapes=[
                pltpu.VMEM((SLOTS, OWN, TILE_Q, NBF, NBF), BF16),
                pltpu.VMEM((LOOPED, GIFT, TILE_Q, NBF, NBF), BF16),
                pltpu.VMEM((STEPS - LOOPED, ROWS_P, TILE_Q, NBF, NBF), BF16),
                pltpu.VMEM((16, TILE_Q, NBF, NBF), BF16),
                pltpu.VMEM((OCC, NBF), BF16),
                pltpu.VMEM((VIRT, NBF), BF16),
                pltpu.VMEM((16, 256), BF16),
                pltpu.VMEM((256, 256), BF16),
                pltpu.VMEM((2, 32, 256), BF16),
                pltpu.VMEM((32, NBF), BF16),
                pltpu.VMEM((32, NBF), BF16),
                pltpu.VMEM((32, NBF), BF16),
                pltpu.VMEM((32, 64), BF16),
                pltpu.VMEM((32, NBF), BF16),
                pltpu.VMEM((512, 512), BF16),
                pltpu.VMEM((256, 256), BF16),
                pltpu.VMEM((NBF, 256), BF16),
                pltpu.VMEM((64, 256), BF16),
                pltpu.VMEM((8, TILE_Q, NBF, NBF), BF16),
                pltpu.VMEM((DEVS, 8, NBF), F32),
                pltpu.VMEM((8, NBF), F32),
                pltpu.VMEM((STEPS, DEVS, 8, NBF), F32),
            ],
            compiler_params=pltpu.CompilerParams(
                collective_id=0, has_side_effects=True, vmem_limit_bytes=48 * 1024 * 1024),
        )(ao_blk, pltpu.with_memory_space_constraint(c_occ.T, pltpu.HBM),
          pltpu.with_memory_space_constraint(c_virt.T, pltpu.HBM))
        out = pl.pallas_call(
            finish,
            out_shape=jax.ShapeDtypeStruct((OCC, HALF, VIRT), F32),
            in_specs=[vmem] * 3,
            out_specs=vmem,
            compiler_params=pltpu.CompilerParams(vmem_limit_bytes=8 * 1024 * 1024),
        )(recv, base, cvd)
        return jnp.swapaxes(out, 1, 2)

    return jax.shard_map(
        local_block, mesh=mesh,
        in_specs=(P(("frag", "dev"), "dev2", None, None), P("frag", None), P("frag", None)),
        out_specs=P("frag", None, ("dev2", "dev")),
        check_vma=False)
```

```python
import functools

import jax
import jax.numpy as jnp
from jax import lax
from jax.experimental import pallas as pl
from jax.experimental.pallas import tpu as pltpu
from jax.sharding import PartitionSpec as P

MESH = pl.DeviceIdType.MESH
F32 = jnp.float32
BF16 = jnp.bfloat16

ROWS_P = 32
ROWS_Q = 64
NBF = 128
OCC = 4
VIRT = 112
HALF = VIRT // 2
TILE_Q = 4
STEPS = ROWS_Q // TILE_Q
SLOTS = 5
OWN = 24
GIFT = ROWS_P - OWN
DEVS = 8
COLS = 4
PIECES = ((13, 0, 16), (13, 16, 8), (13, 24, 8), (14, 0, 16), (14, 16, 16), (15, 0, 8), (15, 8, 8), (15, 16, 8), (15, 24, 8))
SIDE = 13
LAST = STEPS - 1
LOOPED = STEPS - 3
GIFTED = (2, 3, 5, 6, 8, 9, 11, 12)
GIVEN = len(GIFTED)


def iota(shape, dim):
    return lax.broadcasted_iota(jnp.int32, shape, dim)


def one_hot(cond):
    return jnp.where(cond, 1.0, 0.0).astype(BF16)


def dot(a, b):
    return jnp.dot(a, b, preferred_element_type=F32)


def dot_nt(a, b):
    return lax.dot_general(a, b, (((1,), (1,)), ((), ())), preferred_element_type=F32)


def dot_tn(a, b):
    return lax.dot_general(a, b, (((0,), (0,)), ((), ())), preferred_element_type=F32)


def split(x):
    high = x.astype(BF16)
    rest = x - high.astype(F32)
    mid = rest.astype(BF16)
    return high, mid, (rest - mid.astype(F32)).astype(BF16)


def kernel(*refs):
    pl.run_scoped(
        functools.partial(body, *refs),
        pltpu.SemaphoreType.DMA((SLOTS,)),
        pltpu.SemaphoreType.DMA((LOOPED,)),
        pltpu.SemaphoreType.DMA((len(PIECES),)),
        pltpu.SemaphoreType.DMA((2,)),
        pltpu.SemaphoreType.DMA,
        pltpu.SemaphoreType.DMA((3,)),
        pltpu.SemaphoreType.DMA((6,)),
        pltpu.SemaphoreType.DMA((GIVEN + 4,)),
    )


def body(a_hbm, co_hbm, cv_hbm, recv, base, cvd, abuf, land, ends, xbuf, co_ref, cv_ref, lhs1, cv2, w2, w2a, w2b, w2t, w2h, w2g, cvx, t1, t1x, t1h, hbuf, sendx, recvx, sendbuf,
         a_sem, land_sem, l_sem, c_sem, send_sem, recv_sem, give_sem, take_sem):
    row, col = lax.axis_index("dev2"), lax.axis_index("dev")
    me = row * COLS + col

    def fetch(tile):
        slot = lax.rem(tile, SLOTS)
        return pltpu.make_async_copy(
            a_hbm.at[pl.ds(0, OWN), pl.ds(tile * TILE_Q, TILE_Q)], abuf.at[slot], a_sem.at[slot])

    def fetch_rest(tile):
        return pltpu.make_async_copy(
            a_hbm.at[pl.ds(OWN, GIFT), pl.ds(tile * TILE_Q, TILE_Q)], land.at[tile], land_sem.at[tile])

    def fetch_piece(n):
        tile, first, count = PIECES[n]
        part = pl.ds(first, count)
        return pltpu.make_async_copy(
            a_hbm.at[part, pl.ds(tile * TILE_Q, TILE_Q)], ends.at[tile - LOOPED, part], l_sem.at[n])

    co_copy = pltpu.make_async_copy(co_hbm, co_ref, c_sem.at[0])
    cv_copy = pltpu.make_async_copy(cv_hbm, cv_ref, c_sem.at[1])
    co_copy.start()
    cv_copy.start()
    for tile in range(SLOTS):
        fetch(tile).start(priority=1)
        if tile not in GIFTED:
            fetch_rest(tile).start(priority=1)

    x, core = col // 2, lax.rem(col, 2)
    far_row, far_x = 1 - row, 1 - x
    giver, taker = (row + x == 2) & (core == 0), (row + x == 2) & (core == 1)
    last_chip = row + x == 2
    helper = ((row == 1) & (col == 1)) | ((row == 0) & (col == 3))
    plain = (row + x < 2) & jnp.logical_not(helper)
    peers = [(far_row, 2 * far_x), (far_row, 2 * far_x + 1), (far_row, 2 * x), (far_row, 2 * x + 1),
             (row, 2 * far_x), (row, 2 * far_x + 1), (row, 2 * x + 1 - core)]

    barrier = pltpu.get_barrier_semaphore()
    for r, c in peers:
        pl.semaphore_signal(barrier, inc=1, device_id={"dev2": r, "dev": c}, device_id_type=MESH)
    pl.semaphore_wait(barrier, DEVS - 1)

    other = 2 * x + 1 - core
    gifts = []
    for tile in GIFTED:
        gifts.append(pltpu.make_async_remote_copy(
            src_ref=a_hbm.at[pl.ds(OWN, GIFT), pl.ds(tile * TILE_Q, TILE_Q)], dst_ref=land.at[tile],
            send_sem=give_sem.at[0], recv_sem=take_sem.at[len(gifts)],
            device_id={"dev2": row, "dev": other}, device_id_type=MESH))
    for k in range(2):
        gifts.append(pltpu.make_async_remote_copy(
            src_ref=a_hbm.at[pl.ds(16 + 8 * k, 8), pl.ds(LAST * TILE_Q, TILE_Q)], dst_ref=xbuf.at[pl.ds(8 * k, 8)],
            send_sem=give_sem.at[1 + k], recv_sem=take_sem.at[GIVEN + k],
            device_id={"dev2": row, "dev": other}, device_id_type=MESH))
    for k in range(GIVEN):
        gifts[k].start()

    @pl.when(giver)
    def _():
        gifts[GIVEN].start()
        gifts[GIVEN + 1].start()

    sides = [
        pltpu.make_async_remote_copy(
            src_ref=a_hbm.at[pl.ds(first, 4), pl.ds(SIDE * TILE_Q, TILE_Q)], dst_ref=hbuf.at[pl.ds(core * 4, 4)],
            send_sem=give_sem.at[3 + n], recv_sem=take_sem.at[GIVEN + 2 + core],
            device_id={"dev2": r, "dev": c}, device_id_type=MESH)
        for n, (first, r, c) in enumerate([(28, 1, 1), (24, 0, 3)])]

    @pl.when(last_chip)
    def _():
        for side in sides:
            side.start()

    co_copy.wait()
    cv_copy.wait()
    co, cv = co_ref[...], cv_ref[...]

    co_t = dot(one_hot(iota((16, OCC), 0) % OCC == iota((16, OCC), 1)), co)
    r16 = iota((16, NBF), 0)
    lhs1[...] = jnp.concatenate(
        [jnp.where(r16 // OCC == k, co_t, 0.0) for k in range(2)], axis=1).astype(BF16)

    co_i = dot(one_hot(iota((32, OCC), 0) % OCC == iota((32, OCC), 1)), co).astype(BF16)

    def spread(groups):
        width = sum(2 * count * OCC for _, _, count in groups)
        r, c = iota((NBF, width), 0), iota((NBF, width), 1)
        c32, r32 = iota((32, width), 1), iota((32, width), 0)
        pick, qp, at = r < 0, c32 < 0, 0
        for dev, first, count in groups:
            half = count * OCC
            pick |= (r == dev * ROWS_P + first + (c - at) % half // OCC) & (c >= at) & (c < at + 2 * half)
            qp |= (r32 // OCC % 2 == (c32 - at) // half) & (c32 >= at) & (c32 < at + 2 * half)
            at += 2 * half
        placed = dot(co_i, one_hot(pick))
        return jnp.where(qp & (r32 // 8 == c32 % OCC), placed, 0.0).astype(BF16)

    r, c = iota((NBF, 256), 0), iota((NBF, 256), 1)
    p = c % NBF // OCC
    for k in range(2):
        source = jnp.where((p < OWN) | (k == 0), col, other)
        placed = dot(co_i, one_hot(r == source * ROWS_P + p))
        c32, r32 = iota((32, 256), 1), iota((32, 256), 0)
        keep = (r32 // OCC % 2 == c32 // NBF) & (r32 // 8 == c32 % OCC)
        w2[k] = jnp.where(keep, placed, 0.0).astype(BF16)
    w2a[...] = spread([(col, 0, 16)])
    w2b[...] = spread([(col, 16, 8), (col, 24, 8)])
    w2t[...] = spread([(other, 16, 8), (other, 24, 8), (col, 16, 8), (col, 24, 8)])
    w2g[...] = spread([(col, 0, 8), (col, 8, 8)])
    w2h[...] = spread([(2, 24 + 4 * row, 4), (3, 24 + 4 * row, 4)])

    b, c = iota((VIRT, 256), 0), iota((VIRT, 256), 1)
    halves = dot_tn(cv, one_hot((b == (c // NBF) * HALF + c % 64) & (c % 64 < HALF)))
    c = iota((NBF, 256), 1)
    for par in range(2):
        cv2[par * NBF:(par + 1) * NBF, :] = jnp.where((c // 64) % 2 == par, halves, 0.0).astype(BF16)

    wide = jnp.concatenate([cv, jnp.zeros((NBF - VIRT, NBF), BF16)], axis=0)
    r, q = iota((512, NBF), 0), iota((512, NBF), 1)
    rows = dot_nt(one_hot(q == ((r % 256) // OCC) * 2 + r // 256), wide)
    for i in range(OCC):
        cvx[:, i * NBF:(i + 1) * NBF] = jnp.where(r % OCC == i, rows, 0.0).astype(BF16)
    r, q = iota((256, NBF), 0), iota((256, NBF), 1)
    at = (r // 8) % 2 * ROWS_Q + LAST * TILE_Q + (r % 8) // OCC * 2 + r // NBF
    rows = dot_nt(one_hot((q == at) & (r % NBF < 48)), wide)
    for i in range(OCC):
        cvd[:, i * NBF:(i + 1) * NBF] = jnp.where(r % OCC == i, rows, 0.0).astype(BF16)

    def contract_r(rows_of, blocks, ref=t1):
        left = lhs1[...]
        for qp, pb, at in blocks:
            parts = []
            for p0 in (pb, pb + 2):
                rhs = jnp.concatenate([rows_of(p0, 2 * qp + par).reshape(256, NBF) for par in range(2)], axis=1)
                parts.append(dot(left, rhs)[:8])
            ref[at:at + 16, :] = jnp.concatenate(parts, axis=0).astype(BF16)

    def looped(tile, slot):
        return lambda p0, q: abuf[slot, p0:p0 + 2, q] if p0 < OWN else land[tile, p0 - OWN:p0 - OWN + 2, q]

    def ending(tile):
        return lambda p0, q: ends[tile - LOOPED, p0:p0 + 2, q]

    def contract_s(t_one):
        rows = t_one.shape[0]
        if rows < NBF:
            return dot(t_one, cv2[...]).astype(BF16)
        parts = [dot(t_one[k:k + rows // 2], cv2[...]).astype(BF16) for k in (0, rows // 2)]
        return jnp.concatenate(parts, axis=0)

    def pack(step, e_part):
        for j in range(OCC):
            for h in range(2):
                sendbuf[step, 2 * j + h] = e_part[8 * j:8 * j + 8, h * NBF:(h + 1) * NBF]

    def send(step, sem):
        for r, c in peers:
            pltpu.make_async_remote_copy(
                src_ref=sendbuf.at[step, r * COLS + c], dst_ref=recv.at[step, me],
                send_sem=send_sem, recv_sem=recv_sem.at[sem],
                device_id={"dev2": r, "dev": c}, device_id_type=MESH).start()
        recv[step, me] = sendbuf[step, me]

    def send_last():
        for to in range(DEVS):
            @pl.when(me != to)
            def _():
                pltpu.make_async_remote_copy(
                    src_ref=sendbuf.at[LAST, to], dst_ref=recv.at[LAST, me],
                    send_sem=send_sem, recv_sem=recv_sem.at[1],
                    device_id={"dev2": to // COLS, "dev": to % COLS}, device_id_type=MESH).start()
        recv[LAST, me] = sendbuf[LAST, me]

    def blocks(first, count, at):
        return [(qp, first + pb, at + qp * count * OCC + pb * OCC) for qp in range(2) for pb in range(0, count, 4)]

    whole = blocks(0, ROWS_P, 0)
    upper = [b for b in whole if b[1] < 16]
    lower = [b for b in whole if b[1] >= 16]

    def refill(tile):
        new = tile + SLOTS

        @pl.when(new < LOOPED)
        def _():
            fetch(new).start(priority=1)

        @pl.when((new < LOOPED) & (lax.rem(new, 3) == 1))
        def _():
            fetch_rest(new).start(priority=1)

        for step in range(LOOPED, STEPS):
            @pl.when(new == step)
            def _():
                for n in range(len(PIECES)):
                    if PIECES[n][0] == step and n not in (2, 7, 8):
                        fetch_piece(n).start(priority=1)

        @pl.when((new == SIDE) & jnp.logical_not(last_chip))
        def _():
            fetch_piece(2).start(priority=1)

        @pl.when((new == LAST) & jnp.logical_not(giver))
        def _():
            fetch_piece(7).start(priority=1)
            fetch_piece(8).start(priority=1)

    def beside(rows_of, mine, before, weights):
        half = contract_s(t1[...])
        contract_r(rows_of, mine[:4])
        e_part = dot(weights, half)
        contract_r(rows_of, mine[4:])
        pack(before, e_part)
        send(before, 0)

    def step_body(tile, carry):
        fetch(tile).wait()

        @pl.when(lax.rem(tile, 3) == 1)
        def _():
            fetch_rest(tile).wait()

        @pl.when(lax.rem(tile, 3) != 1)
        def _():
            view = land.at[tile]
            pltpu.make_async_copy(view, view, take_sem.at[tile - (tile + 1) // 3 - 1]).wait()

        mixed = jnp.where((lax.rem(tile, 3) == 2) | (tile == 1), 0, 1)
        beside(looped(tile, lax.rem(tile, SLOTS)), whole, tile - 1, w2[mixed])
        refill(tile)
        return carry

    fetch(0).wait()
    fetch_rest(0).wait()
    contract_r(looped(0, 0), whole)
    refill(0)
    lax.fori_loop(1, LOOPED, step_body, 0)

    fetch_piece(0).wait()
    beside(ending(LOOPED), upper, LOOPED - 1, w2[1])

    first = blocks(0, 16, 0)

    def gift_rows(p0, q):
        return xbuf[p0 - 16:p0 - 14, q]

    def most_of_side():
        contract_r(ending(SIDE), [b for b in lower if b[1] < 24])
        for qp in range(2):
            t1[qp * 128 + 96:(qp + 1) * 128, :] = jnp.zeros((32, 256), BF16)

    def both_halves(before):
        beside(ending(before + 1), upper, before, w2[0])
        fetch_piece(4).wait()
        contract_r(ending(before + 1), lower)

    def start_last():
        fetch_piece(5).wait()
        fetch_piece(6).wait()
        beside(ending(LAST), first, LAST - 1, w2[0])

    def finish_last(parts, weights, e_part=None, early=()):
        half = jnp.concatenate([*early, *[contract_s(t1[k:k + 64, :]) for k in parts]], axis=0)
        e_last = dot(weights, half)
        pack(LAST, e_last if e_part is None else e_part + e_last)
        send_last()

    @pl.when(giver)
    def _():
        fetch_piece(1).wait()
        most_of_side()
        fetch_piece(3).wait()
        both_halves(SIDE)
        fetch_piece(5).wait()
        beside(ending(LAST), blocks(0, 8, 0), LAST - 1, w2[0])
        fetch_piece(6).wait()
        contract_r(ending(LAST), blocks(8, 8, 64))
        finish_last((0, 64), w2g[...])

    @pl.when(taker)
    def _():
        fetch_piece(1).wait()
        gifts[GIVEN].wait_recv()
        most_of_side()
        contract_r(gift_rows, blocks(16, 8, 0), t1x)
        fetch_piece(3).wait()
        both_halves(SIDE)
        start_last()
        fetch_piece(7).wait()
        gifts[GIVEN + 1].wait_recv()
        half = contract_s(t1[:128, :])
        contract_r(ending(LAST), blocks(16, 8, 128))
        e_part = dot(w2a[...], half)
        contract_r(gift_rows, blocks(24, 8, 64), t1x)
        fetch_piece(8).wait()
        contract_r(ending(LAST), blocks(24, 8, 192))
        early = contract_s(jnp.concatenate([t1x[...], t1[128:192, :]], axis=0))
        finish_last((192,), w2t[...], e_part, [early])

    @pl.when(plain)
    def _():
        fetch_piece(1).wait()
        fetch_piece(2).wait()
        contract_r(ending(SIDE), lower)
        fetch_piece(3).wait()
        both_halves(SIDE)

    @pl.when(helper)
    def _():
        fetch_piece(1).wait()
        fetch_piece(2).wait()
        for k in range(2):
            view = hbuf.at[pl.ds(4 * k, 4)]
            pltpu.make_async_copy(view, view, take_sem.at[GIVEN + 2 + k]).wait()
        contract_r(ending(SIDE), lower)
        contract_r(lambda p0, q: hbuf[p0:p0 + 2, q], [(qp, 4 * k, 32 * k + 16 * qp) for k in range(2) for qp in range(2)], t1h)
        fetch_piece(3).wait()
        half = contract_s(t1[...])
        extra = contract_s(t1h[...])
        contract_r(ending(SIDE + 1), upper[:4])
        e_part = dot(w2[0], half)
        e_side = dot(w2h[...], extra)
        contract_r(ending(SIDE + 1), upper[4:])
        pack(SIDE, e_part + jnp.where(row == 1, e_side, 0.0))
        for j in range(OCC):
            for h in range(2):
                sendx[2 * j + h] = e_side[8 * j:8 * j + 8, h * NBF:(h + 1) * NBF]
        send(SIDE, 0)

        @pl.when(row == 0)
        def _():
            for r, c in peers:
                pltpu.make_async_remote_copy(
                    src_ref=sendx.at[r * COLS + c], dst_ref=recvx, send_sem=give_sem.at[5], recv_sem=recv_sem.at[2],
                    device_id={"dev2": r, "dev": c}, device_id_type=MESH).start()
            recvx[...] = sendx[me]

        fetch_piece(4).wait()
        contract_r(ending(SIDE + 1), lower)

    @pl.when(jnp.logical_not(last_chip))
    def _():
        start_last()
        fetch_piece(7).wait()
        half = contract_s(t1[:128, :])
        contract_r(ending(LAST), blocks(16, 8, 128))
        e_part = dot(w2a[...], half)
        fetch_piece(8).wait()
        contract_r(ending(LAST), blocks(24, 8, 192))
        finish_last((128, 192), w2b[...], e_part)

    def arrived(view, sem):
        pltpu.make_async_copy(view, view, recv_sem.at[sem]).wait()

    arrived(recv.at[pl.ds(0, LAST), pl.ds(0, DEVS - 1)], 0)

    @pl.when(me != 3)
    def _():
        arrived(recvx, 2)

    recv[SIDE, COLS] = recv[SIDE, COLS] + recvx[...]
    sums = []
    for r in range(2):
        part = recv[:LAST, COLS * r] + recv[:LAST, COLS * r + 1]
        part += recv[:LAST, COLS * r + 2] + recv[:LAST, COLS * r + 3]
        part = jnp.concatenate([part.reshape(LAST * 8, NBF), jnp.zeros((8, NBF), F32)], axis=0)
        sums.append(part.T)
    half = jnp.concatenate(sums, axis=1)
    high, mid, low = split(jnp.concatenate([half[:64], half[64:]], axis=1))
    right = cvx[...]
    base[...] = dot(high, right) + dot(mid, right) + dot(low, right)

    arrived(recv.at[LAST, pl.ds(0, DEVS - 1)], 1)
    sent = sendbuf.at[:, pl.ds(0, DEVS - 1)]
    pltpu.make_async_copy(sent, sent, send_sem).wait()
    view = land.at[pl.ds(0, GIVEN)]
    pltpu.make_async_copy(view, view, give_sem.at[0]).wait()

    @pl.when(giver)
    def _():
        gifts[GIVEN].wait_send()
        gifts[GIVEN + 1].wait_send()

    @pl.when(last_chip)
    def _():
        for side in sides:
            side.wait_send()

    @pl.when(me == 3)
    def _():
        view = sendx.at[pl.ds(0, DEVS - 1)]
        pltpu.make_async_copy(view, view, give_sem.at[5]).wait()


def finish(recv, base, cvd, out_ref):
    sums = []
    for r in range(2):
        part = recv[STEPS - 1, COLS * r] + recv[STEPS - 1, COLS * r + 1]
        sums.append(part + (recv[STEPS - 1, COLS * r + 2] + recv[STEPS - 1, COLS * r + 3]))
    parts = [x.astype(F32) for x in split(jnp.concatenate(sums, axis=0))]
    turned = jnp.concatenate(parts + [jnp.zeros((NBF - 48, NBF), F32)], axis=0).T.astype(BF16)
    total = base[...] + dot(jnp.concatenate([turned[:64], turned[64:]], axis=1), cvd[...])
    for i in range(OCC):
        out_ref[i] = total[:HALF, i * NBF:i * NBF + VIRT]


def solution(mesh):
    def local_block(ao_blk, c_occ, c_virt):
        hbm = pl.BlockSpec(memory_space=pltpu.HBM)
        vmem = pl.BlockSpec(memory_space=pltpu.VMEM)
        recv, base, cvd = pl.pallas_call(
            kernel,
            out_shape=[
                jax.ShapeDtypeStruct((STEPS, DEVS, 8, NBF), F32),
                jax.ShapeDtypeStruct((64, 512), F32),
                jax.ShapeDtypeStruct((256, 512), BF16),
            ],
            in_specs=[hbm] * 3,
            out_specs=[vmem] * 3,
            scratch_shapes=[
                pltpu.VMEM((SLOTS, OWN, TILE_Q, NBF, NBF), BF16),
                pltpu.VMEM((LOOPED, GIFT, TILE_Q, NBF, NBF), BF16),
                pltpu.VMEM((STEPS - LOOPED, ROWS_P, TILE_Q, NBF, NBF), BF16),
                pltpu.VMEM((16, TILE_Q, NBF, NBF), BF16),
                pltpu.VMEM((OCC, NBF), BF16),
                pltpu.VMEM((VIRT, NBF), BF16),
                pltpu.VMEM((16, 256), BF16),
                pltpu.VMEM((256, 256), BF16),
                pltpu.VMEM((2, 32, 256), BF16),
                pltpu.VMEM((32, NBF), BF16),
                pltpu.VMEM((32, NBF), BF16),
                pltpu.VMEM((32, 256), BF16),
                pltpu.VMEM((32, 64), BF16),
                pltpu.VMEM((32, NBF), BF16),
                pltpu.VMEM((512, 512), BF16),
                pltpu.VMEM((256, 256), BF16),
                pltpu.VMEM((NBF, 256), BF16),
                pltpu.VMEM((64, 256), BF16),
                pltpu.VMEM((8, TILE_Q, NBF, NBF), BF16),
                pltpu.VMEM((DEVS, 8, NBF), F32),
                pltpu.VMEM((8, NBF), F32),
                pltpu.VMEM((STEPS, DEVS, 8, NBF), F32),
            ],
            compiler_params=pltpu.CompilerParams(
                collective_id=0, has_side_effects=True, vmem_limit_bytes=48 * 1024 * 1024),
        )(ao_blk, pltpu.with_memory_space_constraint(c_occ.T, pltpu.HBM),
          pltpu.with_memory_space_constraint(c_virt.T, pltpu.HBM))
        out = pl.pallas_call(
            finish,
            out_shape=jax.ShapeDtypeStruct((OCC, HALF, VIRT), F32),
            in_specs=[vmem] * 3,
            out_specs=vmem,
            compiler_params=pltpu.CompilerParams(vmem_limit_bytes=8 * 1024 * 1024),
        )(recv, base, cvd)
        return jnp.swapaxes(out, 1, 2)

    return jax.shard_map(
        local_block, mesh=mesh,
        in_specs=(P(("frag", "dev"), "dev2", None, None), P("frag", None), P("frag", None)),
        out_specs=P("frag", None, ("dev2", "dev")),
        check_vma=False)
```

```python
import functools

import jax
import jax.numpy as jnp
from jax import lax
from jax.experimental import pallas as pl
from jax.experimental.pallas import tpu as pltpu
from jax.sharding import PartitionSpec as P

MESH = pl.DeviceIdType.MESH
F32 = jnp.float32
BF16 = jnp.bfloat16

ROWS_P = 32
ROWS_Q = 64
NBF = 128
OCC = 4
VIRT = 112
HALF = VIRT // 2
TILE_Q = 4
STEPS = ROWS_Q // TILE_Q
SLOTS = 5
OWN = 24
GIFT = ROWS_P - OWN
DEVS = 8
QUEUE = 1
COLS = 4
PIECES = ((13, 0, 16), (13, 16, 8), (13, 24, 8), (14, 0, 16), (14, 16, 16), (15, 0, 8), (15, 8, 8), (15, 16, 8), (15, 24, 8))
SIDE = 13
LAST = STEPS - 1
LOOPED = STEPS - 3
GIFTED = (2, 3, 5, 6, 8, 9, 11, 12)
GIVEN = len(GIFTED)


def iota(shape, dim):
    return lax.broadcasted_iota(jnp.int32, shape, dim)


def both(shape):
    return iota(shape, 0), iota(shape, 1)


def one_hot(cond):
    return jnp.where(cond, 1.0, 0.0).astype(BF16)


def dot(a, b):
    return jnp.dot(a, b, preferred_element_type=F32)


def dot_nt(a, b):
    return lax.dot_general(a, b, (((1,), (1,)), ((), ())), preferred_element_type=F32)


def dot_tn(a, b):
    return lax.dot_general(a, b, (((0,), (0,)), ((), ())), preferred_element_type=F32)


def split(x):
    high = x.astype(BF16)
    rest = x - high.astype(F32)
    mid = rest.astype(BF16)
    return high, mid, (rest - mid.astype(F32)).astype(BF16)


def kernel(*refs):
    pl.run_scoped(
        functools.partial(body, *refs),
        pltpu.SemaphoreType.DMA((SLOTS,)),
        pltpu.SemaphoreType.DMA((LOOPED,)),
        pltpu.SemaphoreType.DMA((len(PIECES),)),
        pltpu.SemaphoreType.DMA((2,)),
        pltpu.SemaphoreType.DMA,
        pltpu.SemaphoreType.DMA((3,)),
        pltpu.SemaphoreType.DMA((6,)),
        pltpu.SemaphoreType.DMA((GIVEN + 4,)),
    )


def body(a_hbm, co_hbm, cv_hbm, recv, base, cvd, abuf, land, ends, xbuf, co_ref, cv_ref, lhs1, cv2, w2, w2a, w2b, w2t, w2h, w2g, cvx, t1, t1x, t1h, hbuf, sendx, recvx, sendbuf,
         a_sem, land_sem, l_sem, c_sem, send_sem, recv_sem, give_sem, take_sem):
    row, col = lax.axis_index("dev2"), lax.axis_index("dev")
    me = row * COLS + col

    def fetch(tile):
        slot = lax.rem(tile, SLOTS)
        return pltpu.make_async_copy(
            a_hbm.at[pl.ds(0, OWN), pl.ds(tile * TILE_Q, TILE_Q)], abuf.at[slot], a_sem.at[slot])

    def fetch_rest(tile):
        return pltpu.make_async_copy(
            a_hbm.at[pl.ds(OWN, GIFT), pl.ds(tile * TILE_Q, TILE_Q)], land.at[tile], land_sem.at[tile])

    def fetch_piece(n):
        tile, first, count = PIECES[n]
        part = pl.ds(first, count)
        return pltpu.make_async_copy(
            a_hbm.at[part, pl.ds(tile * TILE_Q, TILE_Q)], ends.at[tile - LOOPED, part], l_sem.at[n])

    co_copy = pltpu.make_async_copy(co_hbm, co_ref, c_sem.at[0])
    cv_copy = pltpu.make_async_copy(cv_hbm, cv_ref, c_sem.at[1])
    co_copy.start()
    cv_copy.start()
    for tile in range(SLOTS):
        fetch(tile).start(priority=QUEUE)
        if tile not in GIFTED:
            fetch_rest(tile).start(priority=QUEUE)

    x, core = col // 2, lax.rem(col, 2)
    far_row, far_x = 1 - row, 1 - x
    giver, taker = (row + x == 2) & (core == 0), (row + x == 2) & (core == 1)
    last_chip = row + x == 2
    helper = ((row == 1) & (col == 1)) | ((row == 0) & (col == 3))
    plain = (row + x < 2) & jnp.logical_not(helper)
    peers = [(far_row, 2 * far_x), (far_row, 2 * far_x + 1), (far_row, 2 * x), (far_row, 2 * x + 1),
             (row, 2 * far_x), (row, 2 * far_x + 1), (row, 2 * x + 1 - core)]

    barrier = pltpu.get_barrier_semaphore()
    for r, c in peers:
        pl.semaphore_signal(barrier, device_id={"dev2": r, "dev": c}, device_id_type=MESH)
    pl.semaphore_wait(barrier, DEVS - 1)

    other = 2 * x + 1 - core
    gifts = []
    for tile in GIFTED:
        gifts.append(pltpu.make_async_remote_copy(
            src_ref=a_hbm.at[pl.ds(OWN, GIFT), pl.ds(tile * TILE_Q, TILE_Q)], dst_ref=land.at[tile],
            send_sem=give_sem.at[0], recv_sem=take_sem.at[len(gifts)],
            device_id={"dev2": row, "dev": other}, device_id_type=MESH))
    for k in range(2):
        gifts.append(pltpu.make_async_remote_copy(
            src_ref=a_hbm.at[pl.ds(16 + 8 * k, 8), pl.ds(LAST * TILE_Q, TILE_Q)], dst_ref=xbuf.at[pl.ds(8 * k, 8)],
            send_sem=give_sem.at[1 + k], recv_sem=take_sem.at[GIVEN + k],
            device_id={"dev2": row, "dev": other}, device_id_type=MESH))
    for k in range(GIVEN):
        gifts[k].start()

    @pl.when(giver)
    def _():
        gifts[GIVEN].start()
        gifts[GIVEN + 1].start()

    sides = [
        pltpu.make_async_remote_copy(
            src_ref=a_hbm.at[pl.ds(first, 4), pl.ds(SIDE * TILE_Q, TILE_Q)], dst_ref=hbuf.at[pl.ds(core * 4, 4)],
            send_sem=give_sem.at[3 + n], recv_sem=take_sem.at[GIVEN + 2 + core],
            device_id={"dev2": r, "dev": c}, device_id_type=MESH)
        for n, (first, r, c) in enumerate([(28, 1, 1), (24, 0, 3)])]

    @pl.when(last_chip)
    def _():
        for side in sides:
            side.start()

    co_copy.wait()
    cv_copy.wait()
    co, cv = co_ref[...], cv_ref[...]

    co_t = dot(one_hot(iota((16, OCC), 0) % OCC == iota((16, OCC), 1)), co)
    r16 = iota((16, NBF), 0)
    lhs1[...] = jnp.concatenate(
        [jnp.where(r16 // OCC == k, co_t, 0.0) for k in range(2)], axis=1).astype(BF16)

    co_i = dot(one_hot(iota((32, OCC), 0) % OCC == iota((32, OCC), 1)), co).astype(BF16)

    def spread(groups):
        width = sum(2 * count * OCC for _, _, count in groups)
        r, c = both((NBF, width))
        c32, r32 = iota((32, width), 1), iota((32, width), 0)
        pick, qp, at = r < 0, c32 < 0, 0
        for dev, first, count in groups:
            half = count * OCC
            pick |= (r == dev * ROWS_P + first + (c - at) % half // OCC) & (c >= at) & (c < at + 2 * half)
            qp |= (r32 // OCC % 2 == (c32 - at) // half) & (c32 >= at) & (c32 < at + 2 * half)
            at += 2 * half
        placed = dot(co_i, one_hot(pick))
        return jnp.where(qp & (r32 // 8 == c32 % OCC), placed, 0.0).astype(BF16)

    r, c = both((NBF, 256))
    p = c % NBF // OCC
    for k in range(2):
        source = jnp.where((p < OWN) | (k == 0), col, other)
        placed = dot(co_i, one_hot(r == source * ROWS_P + p))
        c32, r32 = iota((32, 256), 1), iota((32, 256), 0)
        keep = (r32 // OCC % 2 == c32 // NBF) & (r32 // 8 == c32 % OCC)
        w2[k] = jnp.where(keep, placed, 0.0).astype(BF16)
    w2a[...] = spread([(col, 0, 16)])
    w2b[...] = spread([(col, 16, 8), (col, 24, 8)])
    w2t[...] = spread([(other, 16, 8), (other, 24, 8), (col, 16, 8), (col, 24, 8)])
    w2g[...] = spread([(col, 0, 8), (col, 8, 8)])
    w2h[...] = spread([(2, 24 + 4 * row, 4), (3, 24 + 4 * row, 4)])

    b, c = both((VIRT, 256))
    halves = dot_tn(cv, one_hot((b == (c // NBF) * HALF + c % 64) & (c % 64 < HALF)))
    c = iota((NBF, 256), 1)
    for par in range(2):
        cv2[par * NBF:(par + 1) * NBF, :] = jnp.where((c // 64) % 2 == par, halves, 0.0).astype(BF16)

    wide = jnp.concatenate([cv, jnp.zeros((NBF - VIRT, NBF), BF16)])
    r, q = both((512, NBF))
    rows = dot_nt(one_hot(q == ((r % 256) // OCC) * 2 + r // 256), wide)
    for i in range(OCC):
        cvx[:, i * NBF:(i + 1) * NBF] = jnp.where(r % OCC == i, rows, 0.0).astype(BF16)
    r, q = both((256, NBF))
    at = (r // 8) % 2 * ROWS_Q + LAST * TILE_Q + (r % 8) // OCC * 2 + r // NBF
    rows = dot_nt(one_hot((q == at) & (r % NBF < 48)), wide)
    for i in range(OCC):
        cvd[:, i * NBF:(i + 1) * NBF] = jnp.where(r % OCC == i, rows, 0.0).astype(BF16)

    def contract_r(rows_of, blocks, ref=t1):
        left = lhs1[...]
        for qp, pb, at in blocks:
            parts = []
            for p0 in (pb, pb + 2):
                rhs = jnp.concatenate([rows_of(p0, 2 * qp + par).reshape(256, NBF) for par in range(2)], axis=1)
                parts.append(dot(left, rhs)[:8])
            ref[at:at + 16, :] = jnp.concatenate(parts).astype(BF16)

    def looped(tile, slot):
        return lambda p0, q: abuf[slot, p0:p0 + 2, q] if p0 < OWN else land[tile, p0 - OWN:p0 - OWN + 2, q]

    def ending(tile):
        return lambda p0, q: ends[tile - LOOPED, p0:p0 + 2, q]

    def contract_s(t_one):
        rows = t_one.shape[0]
        if rows < NBF:
            return dot(t_one, cv2[...]).astype(BF16)
        parts = [dot(t_one[k:k + rows // 2], cv2[...]).astype(BF16) for k in (0, rows // 2)]
        return jnp.concatenate(parts)

    def pack(step, e_part):
        for j in range(OCC):
            for h in range(2):
                sendbuf[step, 2 * j + h] = e_part[8 * j:8 * j + 8, h * NBF:(h + 1) * NBF]

    def send(step, sem):
        for r, c in peers:
            pltpu.make_async_remote_copy(
                src_ref=sendbuf.at[step, r * COLS + c], dst_ref=recv.at[step, me],
                send_sem=send_sem, recv_sem=recv_sem.at[sem],
                device_id={"dev2": r, "dev": c}, device_id_type=MESH).start()
        recv[step, me] = sendbuf[step, me]

    def send_last():
        for to in range(DEVS):
            @pl.when(me != to)
            def _():
                pltpu.make_async_remote_copy(
                    src_ref=sendbuf.at[LAST, to], dst_ref=recv.at[LAST, me],
                    send_sem=send_sem, recv_sem=recv_sem.at[1],
                    device_id={"dev2": to // COLS, "dev": to % COLS}, device_id_type=MESH).start()
        recv[LAST, me] = sendbuf[LAST, me]

    def blocks(first, count, at):
        return [(qp, first + pb, at + qp * count * OCC + pb * OCC) for qp in range(2) for pb in range(0, count, 4)]

    whole = blocks(0, ROWS_P, 0)
    upper = [b for b in whole if b[1] < 16]
    lower = [b for b in whole if b[1] >= 16]

    def refill(tile):
        new = tile + SLOTS

        @pl.when(new < LOOPED)
        def _():
            fetch(new).start(priority=QUEUE)

        @pl.when((new < LOOPED) & (lax.rem(new, 3) == 1))
        def _():
            fetch_rest(new).start(priority=QUEUE)

        for step in range(LOOPED, STEPS):
            @pl.when(new == step)
            def _():
                for n in range(len(PIECES)):
                    if PIECES[n][0] == step and n not in (2, 7, 8):
                        fetch_piece(n).start(priority=QUEUE)

        @pl.when((new == SIDE) & jnp.logical_not(last_chip))
        def _():
            fetch_piece(2).start(priority=QUEUE)

        @pl.when((new == LAST) & jnp.logical_not(giver))
        def _():
            fetch_piece(7).start(priority=QUEUE)
            fetch_piece(8).start(priority=QUEUE)

    def beside(rows_of, mine, before, weights):
        half = contract_s(t1[...])
        contract_r(rows_of, mine[:4])
        e_part = dot(weights, half)
        contract_r(rows_of, mine[4:])
        pack(before, e_part)
        send(before, 0)

    def step_body(tile, carry):
        fetch(tile).wait()

        @pl.when(lax.rem(tile, 3) == 1)
        def _():
            fetch_rest(tile).wait()

        @pl.when(lax.rem(tile, 3) != 1)
        def _():
            view = land.at[tile]
            pltpu.make_async_copy(view, view, take_sem.at[tile - (tile + 1) // 3 - 1]).wait()

        mixed = jnp.where((lax.rem(tile, 3) == 2) | (tile == 1), 0, 1)
        beside(looped(tile, lax.rem(tile, SLOTS)), whole, tile - 1, w2[mixed])
        refill(tile)
        return carry

    fetch(0).wait()
    fetch_rest(0).wait()
    contract_r(looped(0, 0), whole)
    refill(0)
    lax.fori_loop(1, LOOPED, step_body, 0)

    fetch_piece(0).wait()
    beside(ending(LOOPED), upper, LOOPED - 1, w2[1])

    first = blocks(0, 16, 0)

    def gift_rows(p0, q):
        return xbuf[p0 - 16:p0 - 14, q]

    def most_of_side():
        contract_r(ending(SIDE), [b for b in lower if b[1] < 24])
        for qp in range(2):
            t1[qp * 128 + 96:(qp + 1) * 128, :] = jnp.zeros((32, 256), BF16)

    def both_halves(before):
        beside(ending(before + 1), upper, before, w2[0])
        fetch_piece(4).wait()
        contract_r(ending(before + 1), lower)

    def start_last():
        fetch_piece(5).wait()
        fetch_piece(6).wait()
        beside(ending(LAST), first, LAST - 1, w2[0])

    def finish_last(parts, weights, e_part=None, early=()):
        half = jnp.concatenate([*early, *[contract_s(t1[k:k + 64, :]) for k in parts]])
        e_last = dot(weights, half)
        pack(LAST, e_last if e_part is None else e_part + e_last)
        send_last()

    @pl.when(giver)
    def _():
        fetch_piece(1).wait()
        most_of_side()
        fetch_piece(3).wait()
        both_halves(SIDE)
        fetch_piece(5).wait()
        beside(ending(LAST), blocks(0, 8, 0), LAST - 1, w2[0])
        fetch_piece(6).wait()
        contract_r(ending(LAST), blocks(8, 8, 64))
        finish_last((0, 64), w2g[...])

    @pl.when(taker)
    def _():
        fetch_piece(1).wait()
        gifts[GIVEN].wait_recv()
        most_of_side()
        contract_r(gift_rows, blocks(16, 8, 0), t1x)
        fetch_piece(3).wait()
        both_halves(SIDE)
        start_last()
        fetch_piece(7).wait()
        gifts[GIVEN + 1].wait_recv()
        half = contract_s(t1[:128, :])
        contract_r(ending(LAST), blocks(16, 8, 128))
        e_part = dot(w2a[...], half)
        contract_r(gift_rows, blocks(24, 8, 64), t1x)
        fetch_piece(8).wait()
        contract_r(ending(LAST), blocks(24, 8, 192))
        early = contract_s(jnp.concatenate([t1x[...], t1[128:192, :]]))
        finish_last((192,), w2t[...], e_part, [early])

    @pl.when(plain)
    def _():
        fetch_piece(1).wait()
        fetch_piece(2).wait()
        contract_r(ending(SIDE), lower)
        fetch_piece(3).wait()
        both_halves(SIDE)

    @pl.when(helper)
    def _():
        fetch_piece(1).wait()
        fetch_piece(2).wait()
        for k in range(2):
            view = hbuf.at[pl.ds(4 * k, 4)]
            pltpu.make_async_copy(view, view, take_sem.at[GIVEN + 2 + k]).wait()
        contract_r(ending(SIDE), lower)
        contract_r(lambda p0, q: hbuf[p0:p0 + 2, q], [(qp, 4 * k, 32 * k + 16 * qp) for k in range(2) for qp in range(2)], t1h)
        fetch_piece(3).wait()
        half = contract_s(t1[...])
        extra = contract_s(t1h[...])
        contract_r(ending(SIDE + 1), upper[:4])
        e_part = dot(w2[0], half)
        e_side = dot(w2h[...], extra)
        contract_r(ending(SIDE + 1), upper[4:])
        pack(SIDE, e_part + jnp.where(row == 1, e_side, 0.0))
        for j in range(OCC):
            for h in range(2):
                sendx[2 * j + h] = e_side[8 * j:8 * j + 8, h * NBF:(h + 1) * NBF]
        send(SIDE, 0)

        @pl.when(row == 0)
        def _():
            for r, c in peers:
                pltpu.make_async_remote_copy(
                    src_ref=sendx.at[r * COLS + c], dst_ref=recvx, send_sem=give_sem.at[5], recv_sem=recv_sem.at[2],
                    device_id={"dev2": r, "dev": c}, device_id_type=MESH).start()
            recvx[...] = sendx[me]

        fetch_piece(4).wait()
        contract_r(ending(SIDE + 1), lower)

    @pl.when(jnp.logical_not(last_chip))
    def _():
        start_last()
        fetch_piece(7).wait()
        half = contract_s(t1[:128, :])
        contract_r(ending(LAST), blocks(16, 8, 128))
        e_part = dot(w2a[...], half)
        fetch_piece(8).wait()
        contract_r(ending(LAST), blocks(24, 8, 192))
        finish_last((128, 192), w2b[...], e_part)

    def arrived(view, sem):
        pltpu.make_async_copy(view, view, recv_sem.at[sem]).wait()

    arrived(recv.at[pl.ds(0, LAST), pl.ds(0, DEVS - 1)], 0)

    @pl.when(me != 3)
    def _():
        arrived(recvx, 2)

    recv[SIDE, COLS] = recv[SIDE, COLS] + recvx[...]
    sums = []
    for r in range(2):
        part = recv[:LAST, COLS * r] + recv[:LAST, COLS * r + 1]
        part += recv[:LAST, COLS * r + 2] + recv[:LAST, COLS * r + 3]
        part = jnp.concatenate([part.reshape(LAST * 8, NBF), jnp.zeros((8, NBF), F32)])
        sums.append(part.T)
    half = jnp.concatenate(sums, axis=1)
    high, mid, low = split(jnp.concatenate([half[:64], half[64:]], axis=1))
    right = cvx[...]
    base[...] = dot(high, right) + dot(mid, right) + dot(low, right)

    arrived(recv.at[LAST, pl.ds(0, DEVS - 1)], 1)
    sent = sendbuf.at[:, pl.ds(0, DEVS - 1)]
    pltpu.make_async_copy(sent, sent, send_sem).wait()
    view = land.at[pl.ds(0, GIVEN)]
    pltpu.make_async_copy(view, view, give_sem.at[0]).wait()

    @pl.when(giver)
    def _():
        gifts[GIVEN].wait_send()
        gifts[GIVEN + 1].wait_send()

    @pl.when(last_chip)
    def _():
        for side in sides:
            side.wait_send()

    @pl.when(me == 3)
    def _():
        view = sendx.at[pl.ds(0, DEVS - 1)]
        pltpu.make_async_copy(view, view, give_sem.at[5]).wait()


def finish(recv, base, cvd, out_ref):
    sums = []
    for r in range(2):
        part = recv[STEPS - 1, COLS * r] + recv[STEPS - 1, COLS * r + 1]
        sums.append(part + (recv[STEPS - 1, COLS * r + 2] + recv[STEPS - 1, COLS * r + 3]))
    parts = [x.astype(F32) for x in split(jnp.concatenate(sums))]
    turned = jnp.concatenate(parts + [jnp.zeros((NBF - 48, NBF), F32)]).T.astype(BF16)
    total = base[...] + dot(jnp.concatenate([turned[:64], turned[64:]], axis=1), cvd[...])
    for i in range(OCC):
        out_ref[i] = total[:HALF, i * NBF:i * NBF + VIRT]


def solution(mesh):
    def local_block(ao_blk, c_occ, c_virt):
        hbm = pl.BlockSpec(memory_space=pltpu.HBM)
        vmem = pl.BlockSpec(memory_space=pltpu.VMEM)
        recv, base, cvd = pl.pallas_call(
            kernel,
            out_shape=[
                jax.ShapeDtypeStruct((STEPS, DEVS, 8, NBF), F32),
                jax.ShapeDtypeStruct((64, 512), F32),
                jax.ShapeDtypeStruct((256, 512), BF16),
            ],
            in_specs=[hbm] * 3,
            out_specs=[vmem] * 3,
            scratch_shapes=[
                pltpu.VMEM((SLOTS, OWN, TILE_Q, NBF, NBF), BF16),
                pltpu.VMEM((LOOPED, GIFT, TILE_Q, NBF, NBF), BF16),
                pltpu.VMEM((STEPS - LOOPED, ROWS_P, TILE_Q, NBF, NBF), BF16),
                pltpu.VMEM((16, TILE_Q, NBF, NBF), BF16),
                pltpu.VMEM((OCC, NBF), BF16),
                pltpu.VMEM((VIRT, NBF), BF16),
                pltpu.VMEM((16, 256), BF16),
                pltpu.VMEM((256, 256), BF16),
                pltpu.VMEM((2, 32, 256), BF16),
                pltpu.VMEM((32, NBF), BF16),
                pltpu.VMEM((32, NBF), BF16),
                pltpu.VMEM((32, 256), BF16),
                pltpu.VMEM((32, 64), BF16),
                pltpu.VMEM((32, NBF), BF16),
                pltpu.VMEM((512, 512), BF16),
                pltpu.VMEM((256, 256), BF16),
                pltpu.VMEM((NBF, 256), BF16),
                pltpu.VMEM((64, 256), BF16),
                pltpu.VMEM((8, TILE_Q, NBF, NBF), BF16),
                pltpu.VMEM((DEVS, 8, NBF), F32),
                pltpu.VMEM((8, NBF), F32),
                pltpu.VMEM((STEPS, DEVS, 8, NBF), F32),
            ],
            compiler_params=pltpu.CompilerParams(
                collective_id=0, has_side_effects=True, vmem_limit_bytes=48 * 1024 * 1024),
        )(ao_blk, pltpu.with_memory_space_constraint(c_occ.T, pltpu.HBM),
          pltpu.with_memory_space_constraint(c_virt.T, pltpu.HBM))
        out = pl.pallas_call(
            finish,
            out_shape=jax.ShapeDtypeStruct((OCC, HALF, VIRT), F32),
            in_specs=[vmem] * 3,
            out_specs=vmem,
            compiler_params=pltpu.CompilerParams(vmem_limit_bytes=8 * 1024 * 1024),
        )(recv, base, cvd)
        return jnp.swapaxes(out, 1, 2)

    return jax.shard_map(
        local_block, mesh=mesh,
        in_specs=(P(("frag", "dev"), "dev2", None, None), P("frag", None), P("frag", None)),
        out_specs=P("frag", None, ("dev2", "dev")),
        check_vma=False)
```

```python
import functools

import jax
import jax.numpy as jnp
from jax import lax
from jax.experimental import pallas as pl
from jax.experimental.pallas import tpu as pltpu
from jax.sharding import PartitionSpec as P

MESH = pl.DeviceIdType.MESH
F32 = jnp.float32
BF16 = jnp.bfloat16

ROWS_P = 32
ROWS_Q = 64
NBF = 128
OCC = 4
VIRT = 112
HALF = VIRT // 2
TILE_Q = 4
STEPS = ROWS_Q // TILE_Q
SLOTS = 5
OWN = 24
GIFT = ROWS_P - OWN
DEVS = 8
QUEUE = 1
COLS = 4
PIECES = ((13, 0, 16), (13, 16, 8), (13, 24, 8), (14, 0, 16), (14, 16, 16), (15, 0, 8), (15, 8, 8), (15, 16, 8), (15, 24, 8))
SIDE = 13
LAST = STEPS - 1
EARLY = STEPS - 2
LOOPED = STEPS - 3
GIFTED = (2, 3, 5, 6, 8, 9, 11, 12)
GIVEN = len(GIFTED)


def iota(shape, dim):
    return lax.broadcasted_iota(jnp.int32, shape, dim)


def both(shape):
    return iota(shape, 0), iota(shape, 1)


def one_hot(cond):
    return jnp.where(cond, 1.0, 0.0).astype(BF16)


def dot(a, b):
    return jnp.dot(a, b, preferred_element_type=F32)


def dot_nt(a, b):
    return lax.dot_general(a, b, (((1,), (1,)), ((), ())), preferred_element_type=F32)


def dot_tn(a, b):
    return lax.dot_general(a, b, (((0,), (0,)), ((), ())), preferred_element_type=F32)


def split(x):
    high = x.astype(BF16)
    rest = x - high.astype(F32)
    mid = rest.astype(BF16)
    return high, mid, (rest - mid.astype(F32)).astype(BF16)


def kernel(*refs):
    pl.run_scoped(
        functools.partial(body, *refs),
        pltpu.SemaphoreType.DMA((SLOTS,)),
        pltpu.SemaphoreType.DMA((LOOPED,)),
        pltpu.SemaphoreType.DMA((len(PIECES),)),
        pltpu.SemaphoreType.DMA((2,)),
        pltpu.SemaphoreType.DMA,
        pltpu.SemaphoreType.DMA((3,)),
        pltpu.SemaphoreType.DMA((6,)),
        pltpu.SemaphoreType.DMA((GIVEN + 4,)),
    )


def body(a_hbm, co_hbm, cv_hbm, recv, base, cvd, abuf, land, ends, xbuf, co_ref, cv_ref, lhs1, cv2, w2, w2a, w2b, w2t, w2h, w2g, cvx, t1, t1x, t1h, hbuf, sendx, recvx, sendbuf,
         a_sem, land_sem, l_sem, c_sem, send_sem, recv_sem, give_sem, take_sem):
    row, col = lax.axis_index("dev2"), lax.axis_index("dev")
    me = row * COLS + col

    def fetch(tile):
        slot = lax.rem(tile, SLOTS)
        return pltpu.make_async_copy(
            a_hbm.at[pl.ds(0, OWN), pl.ds(tile * TILE_Q, TILE_Q)], abuf.at[slot], a_sem.at[slot])

    def fetch_rest(tile):
        return pltpu.make_async_copy(
            a_hbm.at[pl.ds(OWN, GIFT), pl.ds(tile * TILE_Q, TILE_Q)], land.at[tile], land_sem.at[tile])

    def fetch_piece(n):
        tile, first, count = PIECES[n]
        part = pl.ds(first, count)
        return pltpu.make_async_copy(
            a_hbm.at[part, pl.ds(tile * TILE_Q, TILE_Q)], ends.at[tile - LOOPED, part], l_sem.at[n])

    co_copy = pltpu.make_async_copy(co_hbm, co_ref, c_sem.at[0])
    cv_copy = pltpu.make_async_copy(cv_hbm, cv_ref, c_sem.at[1])
    co_copy.start()
    cv_copy.start()
    for tile in range(SLOTS):
        fetch(tile).start(priority=QUEUE)
        if tile not in GIFTED:
            fetch_rest(tile).start(priority=QUEUE)

    x, core = col // 2, lax.rem(col, 2)
    far_row, far_x = 1 - row, 1 - x
    giver, taker = (row + x == 2) & (core == 0), (row + x == 2) & (core == 1)
    last_chip = row + x == 2
    helper = ((row == 1) & (col == 1)) | ((row == 0) & (col == 3))
    plain = (row + x < 2) & jnp.logical_not(helper)
    peers = [(far_row, 2 * far_x), (far_row, 2 * far_x + 1), (far_row, 2 * x), (far_row, 2 * x + 1),
             (row, 2 * far_x), (row, 2 * far_x + 1), (row, 2 * x + 1 - core)]

    barrier = pltpu.get_barrier_semaphore()
    for r, c in peers:
        pl.semaphore_signal(barrier, device_id={"dev2": r, "dev": c}, device_id_type=MESH)
    pl.semaphore_wait(barrier, DEVS - 1)

    other = 2 * x + 1 - core
    gifts = []
    for tile in GIFTED:
        gifts.append(pltpu.make_async_remote_copy(
            src_ref=a_hbm.at[pl.ds(OWN, GIFT), pl.ds(tile * TILE_Q, TILE_Q)], dst_ref=land.at[tile],
            send_sem=give_sem.at[0], recv_sem=take_sem.at[len(gifts)],
            device_id={"dev2": row, "dev": other}, device_id_type=MESH))
    for k in range(2):
        gifts.append(pltpu.make_async_remote_copy(
            src_ref=a_hbm.at[pl.ds(16 + 8 * k, 8), pl.ds(LAST * TILE_Q, TILE_Q)], dst_ref=xbuf.at[pl.ds(8 * k, 8)],
            send_sem=give_sem.at[1 + k], recv_sem=take_sem.at[GIVEN + k],
            device_id={"dev2": row, "dev": other}, device_id_type=MESH))
    for k in range(GIVEN):
        gifts[k].start()

    @pl.when(giver)
    def _():
        gifts[GIVEN].start()
        gifts[GIVEN + 1].start()

    sides = [
        pltpu.make_async_remote_copy(
            src_ref=a_hbm.at[pl.ds(first, 4), pl.ds(SIDE * TILE_Q, TILE_Q)], dst_ref=hbuf.at[pl.ds(core * 4, 4)],
            send_sem=give_sem.at[3 + n], recv_sem=take_sem.at[GIVEN + 2 + core],
            device_id={"dev2": r, "dev": c}, device_id_type=MESH)
        for n, (first, r, c) in enumerate([(28, 1, 1), (24, 0, 3)])]

    @pl.when(last_chip)
    def _():
        for side in sides:
            side.start()

    co_copy.wait()
    cv_copy.wait()
    co, cv = co_ref[...], cv_ref[...]

    co_t = dot(one_hot(iota((16, OCC), 0) % OCC == iota((16, OCC), 1)), co)
    r16 = iota((16, NBF), 0)
    lhs1[...] = jnp.concatenate(
        [jnp.where(r16 // OCC == k, co_t, 0.0) for k in range(2)], axis=1).astype(BF16)

    co_i = dot(one_hot(iota((32, OCC), 0) % OCC == iota((32, OCC), 1)), co).astype(BF16)

    def spread(groups):
        width = sum(2 * count * OCC for _, _, count in groups)
        r, c = both((NBF, width))
        c32, r32 = iota((32, width), 1), iota((32, width), 0)
        pick, qp, at = r < 0, c32 < 0, 0
        for dev, first, count in groups:
            half = count * OCC
            pick |= (r == dev * ROWS_P + first + (c - at) % half // OCC) & (c >= at) & (c < at + 2 * half)
            qp |= (r32 // OCC % 2 == (c32 - at) // half) & (c32 >= at) & (c32 < at + 2 * half)
            at += 2 * half
        placed = dot(co_i, one_hot(pick))
        return jnp.where(qp & (r32 // 8 == c32 % OCC), placed, 0.0).astype(BF16)

    r, c = both((NBF, 256))
    p = c % NBF // OCC
    for k in range(2):
        source = jnp.where((p < OWN) | (k == 0), col, other)
        placed = dot(co_i, one_hot(r == source * ROWS_P + p))
        c32, r32 = iota((32, 256), 1), iota((32, 256), 0)
        keep = (r32 // OCC % 2 == c32 // NBF) & (r32 // 8 == c32 % OCC)
        w2[k] = jnp.where(keep, placed, 0.0).astype(BF16)
    w2a[...] = spread([(col, 0, 16)])
    w2b[...] = spread([(col, 16, 8), (col, 24, 8)])
    w2t[...] = spread([(other, 16, 8), (other, 24, 8), (col, 16, 8), (col, 24, 8)])
    w2g[...] = spread([(col, 0, 8), (col, 8, 8)])
    w2h[...] = spread([(2, 24 + 4 * row, 4), (3, 24 + 4 * row, 4)])

    b, c = both((VIRT, 256))
    halves = dot_tn(cv, one_hot((b == (c // NBF) * HALF + c % 64) & (c % 64 < HALF)))
    c = iota((NBF, 256), 1)
    for par in range(2):
        cv2[par * NBF:(par + 1) * NBF, :] = jnp.where((c // 64) % 2 == par, halves, 0.0).astype(BF16)

    wide = jnp.concatenate([cv, jnp.zeros((NBF - VIRT, NBF), BF16)])
    r, q = both((512, NBF))
    rows = dot_nt(one_hot(q == ((r % 256) // OCC) * 2 + r // 256), wide)
    for i in range(OCC):
        cvx[:, i * NBF:(i + 1) * NBF] = jnp.where(r % OCC == i, rows, 0.0).astype(BF16)
    r, q = both((256, NBF))
    at = (r // 16) % 2 * ROWS_Q + (EARLY + r // 8 % 2) * TILE_Q + (r % 8) // OCC * 2 + r // NBF
    rows = dot_nt(one_hot((q == at) & (r % NBF < 96)), wide)
    for i in range(OCC):
        cvd[:, i * NBF:(i + 1) * NBF] = jnp.where(r % OCC == i, rows, 0.0).astype(BF16)

    def contract_r(rows_of, blocks, ref=t1):
        left = lhs1[...]
        for qp, pb, at in blocks:
            parts = []
            for p0 in (pb, pb + 2):
                rhs = jnp.concatenate([rows_of(p0, 2 * qp + par).reshape(256, NBF) for par in range(2)], axis=1)
                parts.append(dot(left, rhs)[:8])
            ref[at:at + 16, :] = jnp.concatenate(parts).astype(BF16)

    def looped(tile, slot):
        return lambda p0, q: abuf[slot, p0:p0 + 2, q] if p0 < OWN else land[tile, p0 - OWN:p0 - OWN + 2, q]

    def ending(tile):
        return lambda p0, q: ends[tile - LOOPED, p0:p0 + 2, q]

    def contract_s(t_one):
        rows = t_one.shape[0]
        if rows < NBF:
            return dot(t_one, cv2[...]).astype(BF16)
        parts = [dot(t_one[k:k + rows // 2], cv2[...]).astype(BF16) for k in (0, rows // 2)]
        return jnp.concatenate(parts)

    def pack(step, e_part):
        for j in range(OCC):
            for h in range(2):
                sendbuf[step, 2 * j + h] = e_part[8 * j:8 * j + 8, h * NBF:(h + 1) * NBF]

    def send(step, sem):
        for r, c in peers:
            pltpu.make_async_remote_copy(
                src_ref=sendbuf.at[step, r * COLS + c], dst_ref=recv.at[step, me],
                send_sem=send_sem, recv_sem=recv_sem.at[sem],
                device_id={"dev2": r, "dev": c}, device_id_type=MESH).start()
        recv[step, me] = sendbuf[step, me]

    def send_last():
        for to in range(DEVS):
            @pl.when(me != to)
            def _():
                pltpu.make_async_remote_copy(
                    src_ref=sendbuf.at[LAST, to], dst_ref=recv.at[LAST, me],
                    send_sem=send_sem, recv_sem=recv_sem.at[1],
                    device_id={"dev2": to // COLS, "dev": to % COLS}, device_id_type=MESH).start()
        recv[LAST, me] = sendbuf[LAST, me]

    def blocks(first, count, at):
        return [(qp, first + pb, at + qp * count * OCC + pb * OCC) for qp in range(2) for pb in range(0, count, 4)]

    whole = blocks(0, ROWS_P, 0)
    upper = [b for b in whole if b[1] < 16]
    lower = [b for b in whole if b[1] >= 16]

    def refill(tile):
        new = tile + SLOTS

        @pl.when(new < LOOPED)
        def _():
            fetch(new).start(priority=QUEUE)

        @pl.when((new < LOOPED) & (lax.rem(new, 3) == 1))
        def _():
            fetch_rest(new).start(priority=QUEUE)

        for step in range(LOOPED, STEPS):
            @pl.when(new == step)
            def _():
                for n in range(len(PIECES)):
                    if PIECES[n][0] == step and n not in (2, 7, 8):
                        fetch_piece(n).start(priority=QUEUE)

        @pl.when((new == SIDE) & jnp.logical_not(last_chip))
        def _():
            fetch_piece(2).start(priority=QUEUE)

        @pl.when((new == LAST) & jnp.logical_not(giver))
        def _():
            fetch_piece(7).start(priority=QUEUE)
            fetch_piece(8).start(priority=QUEUE)

    def beside(rows_of, mine, before, weights):
        half = contract_s(t1[...])
        contract_r(rows_of, mine[:4])
        e_part = dot(weights, half)
        contract_r(rows_of, mine[4:])
        pack(before, e_part)
        send(before, int(isinstance(before, int) and before == EARLY))

    def step_body(tile, carry):
        fetch(tile).wait()

        @pl.when(lax.rem(tile, 3) == 1)
        def _():
            fetch_rest(tile).wait()

        @pl.when(lax.rem(tile, 3) != 1)
        def _():
            view = land.at[tile]
            pltpu.make_async_copy(view, view, take_sem.at[tile - (tile + 1) // 3 - 1]).wait()

        mixed = jnp.where((lax.rem(tile, 3) == 2) | (tile == 1), 0, 1)
        beside(looped(tile, lax.rem(tile, SLOTS)), whole, tile - 1, w2[mixed])
        refill(tile)
        return carry

    fetch(0).wait()
    fetch_rest(0).wait()
    contract_r(looped(0, 0), whole)
    refill(0)
    lax.fori_loop(1, LOOPED, step_body, 0)

    fetch_piece(0).wait()
    beside(ending(LOOPED), upper, LOOPED - 1, w2[1])

    first = blocks(0, 16, 0)

    def gift_rows(p0, q):
        return xbuf[p0 - 16:p0 - 14, q]

    def most_of_side():
        contract_r(ending(SIDE), [b for b in lower if b[1] < 24])
        for qp in range(2):
            t1[qp * 128 + 96:(qp + 1) * 128, :] = jnp.zeros((32, 256), BF16)

    def both_halves(before):
        beside(ending(before + 1), upper, before, w2[0])
        fetch_piece(4).wait()
        contract_r(ending(before + 1), lower)

    def start_last():
        fetch_piece(5).wait()
        fetch_piece(6).wait()
        beside(ending(LAST), first, LAST - 1, w2[0])

    def finish_last(parts, weights, e_part=None, early=()):
        half = jnp.concatenate([*early, *[contract_s(t1[k:k + 64, :]) for k in parts]])
        e_last = dot(weights, half)
        pack(LAST, e_last if e_part is None else e_part + e_last)
        send_last()

    @pl.when(giver)
    def _():
        fetch_piece(1).wait()
        most_of_side()
        fetch_piece(3).wait()
        both_halves(SIDE)
        fetch_piece(5).wait()
        beside(ending(LAST), blocks(0, 8, 0), LAST - 1, w2[0])
        fetch_piece(6).wait()
        contract_r(ending(LAST), blocks(8, 8, 64))
        finish_last((0, 64), w2g[...])

    @pl.when(taker)
    def _():
        fetch_piece(1).wait()
        gifts[GIVEN].wait_recv()
        most_of_side()
        contract_r(gift_rows, blocks(16, 8, 0), t1x)
        fetch_piece(3).wait()
        both_halves(SIDE)
        start_last()
        fetch_piece(7).wait()
        gifts[GIVEN + 1].wait_recv()
        half = contract_s(t1[:128, :])
        contract_r(ending(LAST), blocks(16, 8, 128))
        e_part = dot(w2a[...], half)
        contract_r(gift_rows, blocks(24, 8, 64), t1x)
        fetch_piece(8).wait()
        contract_r(ending(LAST), blocks(24, 8, 192))
        early = contract_s(jnp.concatenate([t1x[...], t1[128:192, :]]))
        finish_last((192,), w2t[...], e_part, [early])

    @pl.when(plain)
    def _():
        fetch_piece(1).wait()
        fetch_piece(2).wait()
        contract_r(ending(SIDE), lower)
        fetch_piece(3).wait()
        both_halves(SIDE)

    @pl.when(helper)
    def _():
        fetch_piece(1).wait()
        fetch_piece(2).wait()
        for k in range(2):
            view = hbuf.at[pl.ds(4 * k, 4)]
            pltpu.make_async_copy(view, view, take_sem.at[GIVEN + 2 + k]).wait()
        contract_r(ending(SIDE), lower)
        contract_r(lambda p0, q: hbuf[p0:p0 + 2, q], [(qp, 4 * k, 32 * k + 16 * qp) for k in range(2) for qp in range(2)], t1h)
        fetch_piece(3).wait()
        half = contract_s(t1[...])
        extra = contract_s(t1h[...])
        contract_r(ending(SIDE + 1), upper[:4])
        e_part = dot(w2[0], half)
        e_side = dot(w2h[...], extra)
        contract_r(ending(SIDE + 1), upper[4:])
        pack(SIDE, e_part + jnp.where(row == 1, e_side, 0.0))
        for j in range(OCC):
            for h in range(2):
                sendx[2 * j + h] = e_side[8 * j:8 * j + 8, h * NBF:(h + 1) * NBF]
        send(SIDE, 0)

        @pl.when(row == 0)
        def _():
            for r, c in peers:
                pltpu.make_async_remote_copy(
                    src_ref=sendx.at[r * COLS + c], dst_ref=recvx, send_sem=give_sem.at[5], recv_sem=recv_sem.at[2],
                    device_id={"dev2": r, "dev": c}, device_id_type=MESH).start()
            recvx[...] = sendx[me]

        fetch_piece(4).wait()
        contract_r(ending(SIDE + 1), lower)

    @pl.when(jnp.logical_not(last_chip))
    def _():
        start_last()
        fetch_piece(7).wait()
        half = contract_s(t1[:128, :])
        contract_r(ending(LAST), blocks(16, 8, 128))
        e_part = dot(w2a[...], half)
        fetch_piece(8).wait()
        contract_r(ending(LAST), blocks(24, 8, 192))
        finish_last((128, 192), w2b[...], e_part)

    def arrived(view, sem):
        pltpu.make_async_copy(view, view, recv_sem.at[sem]).wait()

    arrived(recv.at[pl.ds(0, EARLY), pl.ds(0, DEVS - 1)], 0)

    @pl.when(me != 3)
    def _():
        arrived(recvx, 2)

    recv[SIDE, COLS] = recv[SIDE, COLS] + recvx[...]
    sums = []
    for r in range(2):
        part = recv[:EARLY, COLS * r] + recv[:EARLY, COLS * r + 1]
        part += recv[:EARLY, COLS * r + 2] + recv[:EARLY, COLS * r + 3]
        part = jnp.concatenate([part.reshape(EARLY * 8, NBF), jnp.zeros((16, NBF), F32)])
        sums.append(part.T)
    half = jnp.concatenate(sums, axis=1)
    high, mid, low = split(jnp.concatenate([half[:64], half[64:]], axis=1))
    right = cvx[...]
    base[...] = dot(high, right) + dot(mid, right) + dot(low, right)

    arrived(recv.at[pl.ds(EARLY, 2), pl.ds(0, DEVS - 1)], 1)
    sent = sendbuf.at[:, pl.ds(0, DEVS - 1)]
    pltpu.make_async_copy(sent, sent, send_sem).wait()
    view = land.at[pl.ds(0, GIVEN)]
    pltpu.make_async_copy(view, view, give_sem.at[0]).wait()

    @pl.when(giver)
    def _():
        gifts[GIVEN].wait_send()
        gifts[GIVEN + 1].wait_send()

    @pl.when(last_chip)
    def _():
        for side in sides:
            side.wait_send()

    @pl.when(me == 3)
    def _():
        view = sendx.at[pl.ds(0, DEVS - 1)]
        pltpu.make_async_copy(view, view, give_sem.at[5]).wait()


def finish(recv, base, cvd, out_ref):
    sums = []
    for r in range(2):
        part = recv[EARLY:, COLS * r] + recv[EARLY:, COLS * r + 1]
        sums.append((part + (recv[EARLY:, COLS * r + 2] + recv[EARLY:, COLS * r + 3])).reshape(16, NBF))
    parts = [x.astype(F32) for x in split(jnp.concatenate(sums))]
    turned = jnp.concatenate(parts + [jnp.zeros((NBF - 96, NBF), F32)]).T.astype(BF16)
    total = base[...] + dot(jnp.concatenate([turned[:64], turned[64:]], axis=1), cvd[...])
    for i in range(OCC):
        out_ref[i] = total[:HALF, i * NBF:i * NBF + VIRT]


def solution(mesh):
    def local_block(ao_blk, c_occ, c_virt):
        hbm = pl.BlockSpec(memory_space=pltpu.HBM)
        vmem = pl.BlockSpec(memory_space=pltpu.VMEM)
        recv, base, cvd = pl.pallas_call(
            kernel,
            out_shape=[
                jax.ShapeDtypeStruct((STEPS, DEVS, 8, NBF), F32),
                jax.ShapeDtypeStruct((64, 512), F32),
                jax.ShapeDtypeStruct((256, 512), BF16),
            ],
            in_specs=[hbm] * 3,
            out_specs=[vmem] * 3,
            scratch_shapes=[
                pltpu.VMEM((SLOTS, OWN, TILE_Q, NBF, NBF), BF16),
                pltpu.VMEM((LOOPED, GIFT, TILE_Q, NBF, NBF), BF16),
                pltpu.VMEM((STEPS - LOOPED, ROWS_P, TILE_Q, NBF, NBF), BF16),
                pltpu.VMEM((16, TILE_Q, NBF, NBF), BF16),
                pltpu.VMEM((OCC, NBF), BF16),
                pltpu.VMEM((VIRT, NBF), BF16),
                pltpu.VMEM((16, 256), BF16),
                pltpu.VMEM((256, 256), BF16),
                pltpu.VMEM((2, 32, 256), BF16),
                pltpu.VMEM((32, NBF), BF16),
                pltpu.VMEM((32, NBF), BF16),
                pltpu.VMEM((32, 256), BF16),
                pltpu.VMEM((32, 64), BF16),
                pltpu.VMEM((32, NBF), BF16),
                pltpu.VMEM((512, 512), BF16),
                pltpu.VMEM((256, 256), BF16),
                pltpu.VMEM((NBF, 256), BF16),
                pltpu.VMEM((64, 256), BF16),
                pltpu.VMEM((8, TILE_Q, NBF, NBF), BF16),
                pltpu.VMEM((DEVS, 8, NBF), F32),
                pltpu.VMEM((8, NBF), F32),
                pltpu.VMEM((STEPS, DEVS, 8, NBF), F32),
            ],
            compiler_params=pltpu.CompilerParams(
                collective_id=0, has_side_effects=True, vmem_limit_bytes=48 * 1024 * 1024),
        )(ao_blk, pltpu.with_memory_space_constraint(c_occ.T, pltpu.HBM),
          pltpu.with_memory_space_constraint(c_virt.T, pltpu.HBM))
        out = pl.pallas_call(
            finish,
            out_shape=jax.ShapeDtypeStruct((OCC, HALF, VIRT), F32),
            in_specs=[vmem] * 3,
            out_specs=vmem,
            compiler_params=pltpu.CompilerParams(vmem_limit_bytes=8 * 1024 * 1024),
        )(recv, base, cvd)
        return jnp.swapaxes(out, 1, 2)

    return jax.shard_map(
        local_block, mesh=mesh,
        in_specs=(P(("frag", "dev"), "dev2", None, None), P("frag", None), P("frag", None)),
        out_specs=P("frag", None, ("dev2", "dev")),
        check_vma=False)
```

```python
import functools

import jax
import jax.numpy as jnp
from jax import lax
from jax.experimental import pallas as pl
from jax.experimental.pallas import tpu as pltpu
from jax.sharding import PartitionSpec as P

MESH = pl.DeviceIdType.MESH
F32 = jnp.float32
BF16 = jnp.bfloat16

ROWS_P = 32
ROWS_Q = 64
NBF = 128
OCC = 4
VIRT = 112
HALF = VIRT // 2
TILE_Q = 4
STEPS = ROWS_Q // TILE_Q
SLOTS = 5
OWN = 24
GIFT = ROWS_P - OWN
DEVS = 8
QUEUE = 1
COLS = 4
PIECES = ((13, 0, 16), (13, 16, 8), (13, 24, 8), (14, 0, 16), (14, 16, 16), (15, 0, 8), (15, 8, 8), (15, 16, 8), (15, 24, 8))
SIDE = 13
LAST = STEPS - 1
LOOPED = STEPS - 3
GIFTED = (2, 3, 5, 6, 8, 9, 11, 12)
GIVEN = len(GIFTED)


def iota(shape, dim):
    return lax.broadcasted_iota(jnp.int32, shape, dim)


def both(shape):
    return iota(shape, 0), iota(shape, 1)


def one_hot(cond):
    return jnp.where(cond, 1.0, 0.0).astype(BF16)


def dot(a, b):
    return jnp.dot(a, b, preferred_element_type=F32)


def dot_nt(a, b):
    return lax.dot_general(a, b, (((1,), (1,)), ((), ())), preferred_element_type=F32)


def dot_tn(a, b):
    return lax.dot_general(a, b, (((0,), (0,)), ((), ())), preferred_element_type=F32)


def split(x):
    high = x.astype(BF16)
    rest = x - high.astype(F32)
    mid = rest.astype(BF16)
    return high, mid, (rest - mid.astype(F32)).astype(BF16)


def kernel(*refs):
    pl.run_scoped(
        functools.partial(body, *refs),
        pltpu.SemaphoreType.DMA((SLOTS,)),
        pltpu.SemaphoreType.DMA((LOOPED,)),
        pltpu.SemaphoreType.DMA((len(PIECES),)),
        pltpu.SemaphoreType.DMA((2,)),
        pltpu.SemaphoreType.DMA,
        pltpu.SemaphoreType.DMA((3,)),
        pltpu.SemaphoreType.DMA((6,)),
        pltpu.SemaphoreType.DMA((GIVEN + 4,)),
    )


def body(a_hbm, co_hbm, cv_hbm, recv, base, cvd, abuf, land, ends, xbuf, co_ref, cv_ref, lhs1, cv2, w2, w2a, w2b, w2t, w2h, w2g, cvx, t1, t1x, t1h, hbuf, sendx, recvx, sendbuf,
         a_sem, land_sem, l_sem, c_sem, send_sem, recv_sem, give_sem, take_sem):
    row, col = lax.axis_index("dev2"), lax.axis_index("dev")
    me = row * COLS + col

    def fetch(tile):
        slot = lax.rem(tile, SLOTS)
        return pltpu.make_async_copy(
            a_hbm.at[pl.ds(0, OWN), pl.ds(tile * TILE_Q, TILE_Q)], abuf.at[slot], a_sem.at[slot])

    def fetch_rest(tile):
        return pltpu.make_async_copy(
            a_hbm.at[pl.ds(OWN, GIFT), pl.ds(tile * TILE_Q, TILE_Q)], land.at[tile], land_sem.at[tile])

    def fetch_piece(n):
        tile, first, count = PIECES[n]
        part = pl.ds(first, count)
        return pltpu.make_async_copy(
            a_hbm.at[part, pl.ds(tile * TILE_Q, TILE_Q)], ends.at[tile - LOOPED, part], l_sem.at[n])

    co_copy = pltpu.make_async_copy(co_hbm, co_ref, c_sem.at[0])
    cv_copy = pltpu.make_async_copy(cv_hbm, cv_ref, c_sem.at[1])
    co_copy.start()
    cv_copy.start()
    for tile in range(SLOTS):
        fetch(tile).start(priority=QUEUE)
        if tile not in GIFTED:
            fetch_rest(tile).start(priority=QUEUE)

    x, core = col // 2, lax.rem(col, 2)
    far_row, far_x = 1 - row, 1 - x
    giver, taker = (row + x == 2) & (core == 0), (row + x == 2) & (core == 1)
    last_chip = row + x == 2
    helper = ((row == 1) & (col == 1)) | ((row == 0) & (col == 3))
    plain = (row + x < 2) & jnp.logical_not(helper)
    peers = [(far_row, 2 * far_x), (far_row, 2 * far_x + 1), (far_row, 2 * x), (far_row, 2 * x + 1),
             (row, 2 * far_x), (row, 2 * far_x + 1), (row, 2 * x + 1 - core)]

    barrier = pltpu.get_barrier_semaphore()
    for r, c in peers:
        pl.semaphore_signal(barrier, device_id={"dev2": r, "dev": c}, device_id_type=MESH)
    pl.semaphore_wait(barrier, DEVS - 1)

    other = 2 * x + 1 - core
    gifts = []
    for tile in GIFTED:
        gifts.append(pltpu.make_async_remote_copy(
            src_ref=a_hbm.at[pl.ds(OWN, GIFT), pl.ds(tile * TILE_Q, TILE_Q)], dst_ref=land.at[tile],
            send_sem=give_sem.at[0], recv_sem=take_sem.at[len(gifts)],
            device_id={"dev2": row, "dev": other}, device_id_type=MESH))
    for k in range(2):
        gifts.append(pltpu.make_async_remote_copy(
            src_ref=a_hbm.at[pl.ds(16 + 8 * k, 8), pl.ds(LAST * TILE_Q, TILE_Q)], dst_ref=xbuf.at[pl.ds(8 * k, 8)],
            send_sem=give_sem.at[1 + k], recv_sem=take_sem.at[GIVEN + k],
            device_id={"dev2": row, "dev": other}, device_id_type=MESH))
    for k in range(GIVEN):
        gifts[k].start()

    @pl.when(giver)
    def _():
        gifts[GIVEN].start()
        gifts[GIVEN + 1].start()

    sides = [
        pltpu.make_async_remote_copy(
            src_ref=a_hbm.at[pl.ds(first, 4), pl.ds(SIDE * TILE_Q, TILE_Q)], dst_ref=hbuf.at[pl.ds(core * 4, 4)],
            send_sem=give_sem.at[3 + n], recv_sem=take_sem.at[GIVEN + 2 + core],
            device_id={"dev2": r, "dev": c}, device_id_type=MESH)
        for n, (first, r, c) in enumerate([(28, 1, 1), (24, 0, 3)])]

    @pl.when(last_chip)
    def _():
        for side in sides:
            side.start()

    co_copy.wait()
    cv_copy.wait()
    co, cv = co_ref[...], cv_ref[...]

    co_t = dot(one_hot(iota((16, OCC), 0) % OCC == iota((16, OCC), 1)), co)
    r16 = iota((16, NBF), 0)
    lhs1[...] = jnp.concatenate(
        [jnp.where(r16 // OCC == k, co_t, 0.0) for k in range(2)], axis=1).astype(BF16)

    co_i = dot(one_hot(iota((32, OCC), 0) % OCC == iota((32, OCC), 1)), co).astype(BF16)

    def spread(groups):
        width = sum(2 * count * OCC for _, _, count in groups)
        r, c = both((NBF, width))
        c32, r32 = iota((32, width), 1), iota((32, width), 0)
        pick, qp, at = r < 0, c32 < 0, 0
        for dev, first, count in groups:
            half = count * OCC
            pick |= (r == dev * ROWS_P + first + (c - at) % half // OCC) & (c >= at) & (c < at + 2 * half)
            qp |= (r32 // OCC % 2 == (c32 - at) // half) & (c32 >= at) & (c32 < at + 2 * half)
            at += 2 * half
        placed = dot(co_i, one_hot(pick))
        return jnp.where(qp & (r32 // 8 == c32 % OCC), placed, 0.0).astype(BF16)

    r, c = both((NBF, 256))
    p = c % NBF // OCC
    for k in range(2):
        source = jnp.where((p < OWN) | (k == 0), col, other)
        placed = dot(co_i, one_hot(r == source * ROWS_P + p))
        c32, r32 = iota((32, 256), 1), iota((32, 256), 0)
        keep = (r32 // OCC % 2 == c32 // NBF) & (r32 // 8 == c32 % OCC)
        w2[k] = jnp.where(keep, placed, 0.0).astype(BF16)
    w2a[...] = spread([(col, 0, 16)])
    w2b[...] = spread([(col, 16, 8), (col, 24, 8)])
    w2t[...] = spread([(other, 16, 8), (other, 24, 8), (col, 16, 8), (col, 24, 8)])
    w2g[...] = spread([(col, 0, 8), (col, 8, 8)])
    w2h[...] = spread([(2, 24 + 4 * row, 4), (3, 24 + 4 * row, 4)])

    b, c = both((VIRT, 256))
    halves = dot_tn(cv, one_hot((b == (c // NBF) * HALF + c % 64) & (c % 64 < HALF)))
    c = iota((NBF, 256), 1)
    for par in range(2):
        cv2[par * NBF:(par + 1) * NBF, :] = jnp.where((c // 64) % 2 == par, halves, 0.0).astype(BF16)

    wide = jnp.concatenate([cv, jnp.zeros((NBF - VIRT, NBF), BF16)])
    r, q = both((512, NBF))
    rows = dot_nt(one_hot(q == ((r % 256) // OCC) * 2 + r // 256), wide)
    for i in range(OCC):
        cvx[:, i * NBF:(i + 1) * NBF] = jnp.where(r % OCC == i, rows, 0.0).astype(BF16)
    r, q = both((256, NBF))
    at = (r // 8) % 2 * ROWS_Q + LAST * TILE_Q + (r % 8) // OCC * 2 + r // NBF
    rows = dot_nt(one_hot((q == at) & (r % NBF < 48)), wide)
    for i in range(OCC):
        cvd[:, i * NBF:(i + 1) * NBF] = jnp.where(r % OCC == i, rows, 0.0).astype(BF16)

    def contract_r(rows_of, blocks, ref=t1):
        left = lhs1[...]
        for qp, pb, at in blocks:
            parts = []
            for p0 in (pb, pb + 2):
                rhs = jnp.concatenate([rows_of(p0, 2 * qp + par).reshape(256, NBF) for par in range(2)], axis=1)
                parts.append(dot(left, rhs)[:8])
            ref[at:at + 16, :] = jnp.concatenate(parts).astype(BF16)

    def looped(tile, slot):
        return lambda p0, q: abuf[slot, p0:p0 + 2, q] if p0 < OWN else land[tile, p0 - OWN:p0 - OWN + 2, q]

    def ending(tile):
        return lambda p0, q: ends[tile - LOOPED, p0:p0 + 2, q]

    def contract_s(t_one):
        rows = t_one.shape[0]
        if rows < NBF:
            return dot(t_one, cv2[...]).astype(BF16)
        parts = [dot(t_one[k:k + rows // 2], cv2[...]).astype(BF16) for k in (0, rows // 2)]
        return jnp.concatenate(parts)

    def pack(step, e_part):
        for j in range(OCC):
            for h in range(2):
                sendbuf[step, 2 * j + h] = e_part[8 * j:8 * j + 8, h * NBF:(h + 1) * NBF]

    def send(step, sem):
        for r, c in peers:
            pltpu.make_async_remote_copy(
                src_ref=sendbuf.at[step, r * COLS + c], dst_ref=recv.at[step, me],
                send_sem=send_sem, recv_sem=recv_sem.at[sem],
                device_id={"dev2": r, "dev": c}, device_id_type=MESH).start()
        recv[step, me] = sendbuf[step, me]

    def send_last():
        for to in range(DEVS):
            @pl.when(me != to)
            def _():
                pltpu.make_async_remote_copy(
                    src_ref=sendbuf.at[LAST, to], dst_ref=recv.at[LAST, me],
                    send_sem=send_sem, recv_sem=recv_sem.at[1],
                    device_id={"dev2": to // COLS, "dev": to % COLS}, device_id_type=MESH).start()
        recv[LAST, me] = sendbuf[LAST, me]

    def blocks(first, count, at):
        return [(qp, first + pb, at + qp * count * OCC + pb * OCC) for qp in range(2) for pb in range(0, count, 4)]

    whole = blocks(0, ROWS_P, 0)
    upper = [b for b in whole if b[1] < 16]
    lower = [b for b in whole if b[1] >= 16]

    def refill(tile):
        new = tile + SLOTS

        @pl.when(new < LOOPED)
        def _():
            fetch(new).start(priority=QUEUE)

        @pl.when((new < LOOPED) & (lax.rem(new, 3) == 1))
        def _():
            fetch_rest(new).start(priority=QUEUE)

        for step in range(LOOPED, STEPS):
            @pl.when(new == step)
            def _():
                for n in range(len(PIECES)):
                    if PIECES[n][0] == step and n not in (2, 7, 8):
                        fetch_piece(n).start(priority=QUEUE)

        @pl.when((new == SIDE) & jnp.logical_not(last_chip))
        def _():
            fetch_piece(2).start(priority=QUEUE)

        @pl.when((new == LAST) & jnp.logical_not(giver))
        def _():
            fetch_piece(7).start(priority=QUEUE)
            fetch_piece(8).start(priority=QUEUE)

    def beside(rows_of, mine, before, weights):
        half = contract_s(t1[...])
        contract_r(rows_of, mine[:4])
        e_part = dot(weights, half)
        contract_r(rows_of, mine[4:])
        pack(before, e_part)
        send(before, 0)

    def step_body(tile, carry):
        fetch(tile).wait()

        @pl.when(lax.rem(tile, 3) == 1)
        def _():
            fetch_rest(tile).wait()

        @pl.when(lax.rem(tile, 3) != 1)
        def _():
            view = land.at[tile]
            pltpu.make_async_copy(view, view, take_sem.at[tile - (tile + 1) // 3 - 1]).wait()

        mixed = jnp.where((lax.rem(tile, 3) == 2) | (tile == 1), 0, 1)
        beside(looped(tile, lax.rem(tile, SLOTS)), whole, tile - 1, w2[mixed])
        refill(tile)
        return carry

    fetch(0).wait()
    fetch_rest(0).wait()
    contract_r(looped(0, 0), whole)
    refill(0)
    lax.fori_loop(1, LOOPED, step_body, 0)

    fetch_piece(0).wait()
    beside(ending(LOOPED), upper, LOOPED - 1, w2[1])

    first = blocks(0, 16, 0)

    def gift_rows(p0, q):
        return xbuf[p0 - 16:p0 - 14, q]

    def most_of_side():
        contract_r(ending(SIDE), [b for b in lower if b[1] < 24])
        for qp in range(2):
            t1[qp * 128 + 96:(qp + 1) * 128, :] = jnp.zeros((32, 256), BF16)

    def both_halves(before):
        beside(ending(before + 1), upper, before, w2[0])
        fetch_piece(4).wait()
        contract_r(ending(before + 1), lower)

    def start_last():
        fetch_piece(5).wait()
        fetch_piece(6).wait()
        beside(ending(LAST), first, LAST - 1, w2[0])

    def finish_last(parts, weights, e_part=None, early=()):
        half = jnp.concatenate([*early, *[contract_s(t1[k:k + 64, :]) for k in parts]])
        e_last = dot(weights, half)
        pack(LAST, e_last if e_part is None else e_part + e_last)
        send_last()

    @pl.when(giver)
    def _():
        fetch_piece(1).wait()
        most_of_side()
        fetch_piece(3).wait()
        both_halves(SIDE)
        fetch_piece(5).wait()
        beside(ending(LAST), blocks(0, 8, 0), LAST - 1, w2[0])
        fetch_piece(6).wait()
        contract_r(ending(LAST), blocks(8, 8, 64))
        finish_last((0, 64), w2g[...])

    @pl.when(taker)
    def _():
        fetch_piece(1).wait()
        gifts[GIVEN].wait_recv()
        most_of_side()
        contract_r(gift_rows, blocks(16, 8, 0), t1x)
        fetch_piece(3).wait()
        both_halves(SIDE)
        fetch_piece(5).wait()
        beside(ending(LAST), [b for b in first if b[1] < 8], LAST - 1, w2[0])
        fetch_piece(6).wait()
        gifts[GIVEN + 1].wait_recv()
        contract_r(ending(LAST), [b for b in first if b[1] >= 8])
        contract_r(gift_rows, blocks(24, 8, 64), t1x)
        fetch_piece(7).wait()
        half = contract_s(t1[:128, :])
        contract_r(ending(LAST), blocks(16, 8, 128))
        e_part = dot(w2a[...], half)
        fetch_piece(8).wait()
        contract_r(ending(LAST), blocks(24, 8, 192))
        early = contract_s(jnp.concatenate([t1x[...], t1[128:192, :]]))
        finish_last((192,), w2t[...], e_part, [early])

    @pl.when(plain)
    def _():
        fetch_piece(1).wait()
        fetch_piece(2).wait()
        contract_r(ending(SIDE), lower)
        fetch_piece(3).wait()
        both_halves(SIDE)

    @pl.when(helper)
    def _():
        fetch_piece(1).wait()
        fetch_piece(2).wait()
        for k in range(2):
            view = hbuf.at[pl.ds(4 * k, 4)]
            pltpu.make_async_copy(view, view, take_sem.at[GIVEN + 2 + k]).wait()
        contract_r(ending(SIDE), lower)
        contract_r(lambda p0, q: hbuf[p0:p0 + 2, q], [(qp, 4 * k, 32 * k + 16 * qp) for k in range(2) for qp in range(2)], t1h)
        fetch_piece(3).wait()
        half = contract_s(t1[...])
        extra = contract_s(t1h[...])
        contract_r(ending(SIDE + 1), upper[:4])
        e_part = dot(w2[0], half)
        e_side = dot(w2h[...], extra)
        contract_r(ending(SIDE + 1), upper[4:])
        pack(SIDE, e_part + jnp.where(row == 1, e_side, 0.0))
        for j in range(OCC):
            for h in range(2):
                sendx[2 * j + h] = e_side[8 * j:8 * j + 8, h * NBF:(h + 1) * NBF]
        send(SIDE, 0)

        @pl.when(row == 0)
        def _():
            for r, c in peers:
                pltpu.make_async_remote_copy(
                    src_ref=sendx.at[r * COLS + c], dst_ref=recvx, send_sem=give_sem.at[5], recv_sem=recv_sem.at[2],
                    device_id={"dev2": r, "dev": c}, device_id_type=MESH).start()
            recvx[...] = sendx[me]

        fetch_piece(4).wait()
        contract_r(ending(SIDE + 1), lower)

    @pl.when(jnp.logical_not(last_chip))
    def _():
        start_last()
        fetch_piece(7).wait()
        half = contract_s(t1[:128, :])
        contract_r(ending(LAST), blocks(16, 8, 128))
        e_part = dot(w2a[...], half)
        fetch_piece(8).wait()
        contract_r(ending(LAST), blocks(24, 8, 192))
        finish_last((128, 192), w2b[...], e_part)

    def arrived(view, sem):
        pltpu.make_async_copy(view, view, recv_sem.at[sem]).wait()

    arrived(recv.at[pl.ds(0, LAST), pl.ds(0, DEVS - 1)], 0)

    @pl.when(me != 3)
    def _():
        arrived(recvx, 2)

    recv[SIDE, COLS] = recv[SIDE, COLS] + recvx[...]
    sums = []
    for r in range(2):
        part = recv[:LAST, COLS * r] + recv[:LAST, COLS * r + 1]
        part += recv[:LAST, COLS * r + 2] + recv[:LAST, COLS * r + 3]
        part = jnp.concatenate([part.reshape(LAST * 8, NBF), jnp.zeros((8, NBF), F32)])
        sums.append(part.T)
    half = jnp.concatenate(sums, axis=1)
    high, mid, low = split(jnp.concatenate([half[:64], half[64:]], axis=1))
    right = cvx[...]
    base[...] = dot(high, right) + dot(mid, right) + dot(low, right)

    arrived(recv.at[LAST, pl.ds(0, DEVS - 1)], 1)
    sent = sendbuf.at[:, pl.ds(0, DEVS - 1)]
    pltpu.make_async_copy(sent, sent, send_sem).wait()
    view = land.at[pl.ds(0, GIVEN)]
    pltpu.make_async_copy(view, view, give_sem.at[0]).wait()

    @pl.when(giver)
    def _():
        gifts[GIVEN].wait_send()
        gifts[GIVEN + 1].wait_send()

    @pl.when(last_chip)
    def _():
        for side in sides:
            side.wait_send()

    @pl.when(me == 3)
    def _():
        view = sendx.at[pl.ds(0, DEVS - 1)]
        pltpu.make_async_copy(view, view, give_sem.at[5]).wait()


def finish(recv, base, cvd, out_ref):
    sums = []
    for r in range(2):
        part = recv[STEPS - 1, COLS * r] + recv[STEPS - 1, COLS * r + 1]
        sums.append(part + (recv[STEPS - 1, COLS * r + 2] + recv[STEPS - 1, COLS * r + 3]))
    parts = [x.astype(F32) for x in split(jnp.concatenate(sums))]
    turned = jnp.concatenate(parts + [jnp.zeros((NBF - 48, NBF), F32)]).T.astype(BF16)
    total = base[...] + dot(jnp.concatenate([turned[:64], turned[64:]], axis=1), cvd[...])
    for i in range(OCC):
        out_ref[i] = total[:HALF, i * NBF:i * NBF + VIRT]


def solution(mesh):
    def local_block(ao_blk, c_occ, c_virt):
        hbm = pl.BlockSpec(memory_space=pltpu.HBM)
        vmem = pl.BlockSpec(memory_space=pltpu.VMEM)
        recv, base, cvd = pl.pallas_call(
            kernel,
            out_shape=[
                jax.ShapeDtypeStruct((STEPS, DEVS, 8, NBF), F32),
                jax.ShapeDtypeStruct((64, 512), F32),
                jax.ShapeDtypeStruct((256, 512), BF16),
            ],
            in_specs=[hbm] * 3,
            out_specs=[vmem] * 3,
            scratch_shapes=[
                pltpu.VMEM((SLOTS, OWN, TILE_Q, NBF, NBF), BF16),
                pltpu.VMEM((LOOPED, GIFT, TILE_Q, NBF, NBF), BF16),
                pltpu.VMEM((STEPS - LOOPED, ROWS_P, TILE_Q, NBF, NBF), BF16),
                pltpu.VMEM((16, TILE_Q, NBF, NBF), BF16),
                pltpu.VMEM((OCC, NBF), BF16),
                pltpu.VMEM((VIRT, NBF), BF16),
                pltpu.VMEM((16, 256), BF16),
                pltpu.VMEM((256, 256), BF16),
                pltpu.VMEM((2, 32, 256), BF16),
                pltpu.VMEM((32, NBF), BF16),
                pltpu.VMEM((32, NBF), BF16),
                pltpu.VMEM((32, 256), BF16),
                pltpu.VMEM((32, 64), BF16),
                pltpu.VMEM((32, NBF), BF16),
                pltpu.VMEM((512, 512), BF16),
                pltpu.VMEM((256, 256), BF16),
                pltpu.VMEM((NBF, 256), BF16),
                pltpu.VMEM((64, 256), BF16),
                pltpu.VMEM((8, TILE_Q, NBF, NBF), BF16),
                pltpu.VMEM((DEVS, 8, NBF), F32),
                pltpu.VMEM((8, NBF), F32),
                pltpu.VMEM((STEPS, DEVS, 8, NBF), F32),
            ],
            compiler_params=pltpu.CompilerParams(
                collective_id=0, has_side_effects=True, vmem_limit_bytes=48 * 1024 * 1024),
        )(ao_blk, pltpu.with_memory_space_constraint(c_occ.T, pltpu.HBM),
          pltpu.with_memory_space_constraint(c_virt.T, pltpu.HBM))
        out = pl.pallas_call(
            finish,
            out_shape=jax.ShapeDtypeStruct((OCC, HALF, VIRT), F32),
            in_specs=[vmem] * 3,
            out_specs=vmem,
            compiler_params=pltpu.CompilerParams(vmem_limit_bytes=8 * 1024 * 1024),
        )(recv, base, cvd)
        return jnp.swapaxes(out, 1, 2)

    return jax.shard_map(
        local_block, mesh=mesh,
        in_specs=(P(("frag", "dev"), "dev2", None, None), P("frag", None), P("frag", None)),
        out_specs=P("frag", None, ("dev2", "dev")),
        check_vma=False)
```
